32 devices in a mesh: grp: 2 (over x), seq: 8 (over z, y), tp: 2 (over core).
Axes of the slice: x: 2, y: 2, z: 4, core: 2. Of those that a mesh axis runs over, the one named last changes fastest.
Arguments:
- visual_q: bfloat16 [4096, 1536], P(('grp', 'seq'), 'tp'), parts along dimension 0, may hold values from -8 to 8
- visual_key_input: bfloat16 [4096, 1536], P(('grp', 'seq'), 'tp'), parts along dimension 0, may hold values from -8 to 8
- visual_v: bfloat16 [4096, 1536], P(('grp', 'seq'), 'tp'), parts along dimension 0, may hold values from -6 to 6
- text_k: bfloat16 [512, 1536], P(('grp', 'seq'), 'tp'), parts along dimension 0, may hold values from -6 to 6
- text_v: bfloat16 [512, 1536], P(('grp', 'seq'), 'tp'), parts along dimension 0, may hold values from -6 to 6
- text_mask: int32 [512], P(('grp', 'seq')), parts along dimension 0, may hold values from 0 to 1, as said below
- slab_order: int32 [16], P(('grp', 'seq')), parts along dimension 0, may hold values from 0 to 7, each once
- q_gain: float32 [128], replicated, may hold values from 0.8 to 6
- key_norm_gain: float32 [128], replicated, may hold values from 0.8 to 6
- w_out: bfloat16 [1536, 3072], P('tp'), may hold values from -0.8984375 to 0.8984375
Outputs:
- attended: bfloat16 [4096, 3072], P(('grp', 'seq', 'tp')), parts along dimension 0
The draws below stay inside these ranges and needn't reach their ends.
There are 2 independent parts, one for each index of `grp`. The reference program is written for one: setup_inputs(seed, part) draws one part's arguments, and reference() takes and returns one part's arrays. A program takes and returns all parts, laid end to end along the dimension named above; an argument that names none is the same for every part. Nothing has to cross between parts.
Inputs may be any that keep to these rules, and one draw needn't show every extreme that they name: `text_mask`: the first entries are 1 and the rest 0, with at least 32 ones. `slab_order`: each slab number once.
All inputs are finite; a program needn't handle non-finite values.
Results may differ from the reference program's by a relative error of at most 0.013.
The reference program's roundings to bfloat16 on the way count: a program that leaves them out, or rounds other values in their place, can miss the bound.
Values may be sent and summed in bfloat16 or wider, within the bound.
A program may use at most 128 MiB of HBM per device.

```python
import jax
import jax.numpy as jnp
from jax import lax

HEADS = 12
HEAD = 128
D = 3072
TEXT = 256
SLAB_H = 2
WIDE = 32
TOK_DEV = 256
VIS = 2048
N_SEQ = 8
N_TP = 2


def shared_rows(key):
    return jnp.clip(jax.random.normal(jax.random.fold_in(key, 101), (VIS, HEADS * HEAD), jnp.float32), -8.0, 8.0)


def draw_visual_key_input(key, part):
    return shared_rows(key).astype(jnp.bfloat16)


def draw_visual_q(key, part):
    fresh = jnp.clip(jax.random.normal(jax.random.fold_in(key, 202), (VIS, HEADS * HEAD), jnp.float32), -8.0, 8.0)
    return fresh.astype(jnp.bfloat16)


def draw_gain(key):
    return jax.random.uniform(key, (HEAD,), jnp.float32, 0.8, 1.6)


def draw_q_gain(key, part):
    return draw_gain(jax.random.fold_in(key, 303))


def draw_key_norm_gain(key, part):
    return draw_gain(jax.random.fold_in(key, 404))


def draw_text_mask(key, part):
    length = jax.random.randint(jax.random.fold_in(key, 505), (), TEXT // 8, TEXT + 1)
    return (jnp.arange(TEXT) < length).astype(jnp.int32)


def levels(rng, dims, cuts, low, high):
    def one(dim, shards_of):
        steps = jax.random.uniform(jax.random.fold_in(jax.random.fold_in(rng, 6), dim), (shards_of,), jnp.float32, low / len(cuts), high / len(cuts))
        return jnp.repeat(jnp.exp(steps), dims[dim] // shards_of).reshape((-1,) + (1,) * (len(dims) - dim - 1))

    loudness = one(*cuts[0])
    for cut in cuts[1:]:
        loudness = loudness * one(*cut)
    return loudness


def bell_draw(stream_key, shape, scale, limit, split=(), kind=jnp.bfloat16):
    loudness = levels(stream_key, shape, split, -0.22, 0.18) if split else 1.0
    values = jax.random.normal(stream_key, shape, jnp.float32) * scale * loudness
    return jnp.minimum(jnp.maximum(values, -limit), limit).astype(kind)


def setup_inputs(seed: int = 0, part: int = 0) -> dict:
    key_of = jax.random.split(jax.random.key(seed), 11)
    part_splits = jax.random.split(jax.random.fold_in(key_of[10], part), 11)
    visual_q = draw_visual_q(jax.random.fold_in(jax.random.fold_in(key_of[10], part), 71), part)
    visual_key_input = draw_visual_key_input(jax.random.fold_in(jax.random.fold_in(key_of[10], part), 71), part)
    visual_v = bell_draw(part_splits[2], (VIS, HEADS * HEAD), 1.0, 6.0, ((0, 8), (1, 2)))
    text_k = bell_draw(part_splits[3], (TEXT, HEADS * HEAD), 1.0, 6.0, ((0, 8), (1, 2)))
    text_v = bell_draw(part_splits[4], (TEXT, HEADS * HEAD), 1.0, 6.0, ((0, 8), (1, 2)))
    text_mask = draw_text_mask(jax.random.fold_in(jax.random.fold_in(key_of[10], part), 71), part)
    slab_order = jax.random.permutation(part_splits[6], N_SEQ).astype(jnp.int32)
    q_gain = draw_q_gain(jax.random.fold_in(key_of[10], 71), part)
    key_norm_gain = draw_key_norm_gain(jax.random.fold_in(key_of[10], 71), part)
    w_out = bell_draw(key_of[9], (HEADS * HEAD, D), 0.15, 0.8984375, ((0, 2),))
    return {"visual_q": visual_q, "visual_key_input": visual_key_input, "visual_v": visual_v, "text_k": text_k, "text_v": text_v, "text_mask": text_mask, "slab_order": slab_order, "q_gain": q_gain, "key_norm_gain": key_norm_gain, "w_out": w_out}


PARTS = (32, 48, 48)

def apply_norm(x, gain):
    x32 = x.astype(jnp.float32).reshape(x.shape[0], -1, 128)
    scale = lax.rsqrt(lax.optimization_barrier(jnp.mean(x32 * x32, axis=-1, keepdims=True)) + 0.05)
    return x32 * scale * gain

def angles(frame, height, column):
    pieces = []
    for pos, size in zip((frame, height, column), PARTS):
        half = size // 2
        freq = 10000.0 ** (-jnp.arange(half, dtype=jnp.float32) / half)
        pieces.append(pos.astype(jnp.float32)[:, None] * freq[None, :])
    angle = jnp.concatenate(pieces, axis=-1)
    return (jnp.cos(angle), jnp.sin(angle))

def apply_rotation(x, cosine_table, sine_table):
    outs = []
    offset = 0
    column = 0
    for size in PARTS:
        half = size // 2
        first = x[..., offset:offset + half]
        second = x[..., offset + half:offset + size]
        cpart = cosine_table[:, None, column:column + half]
        spart = sine_table[:, None, column:column + half]
        outs.append(first * cpart - second * spart)
        outs.append(second * cpart + first * spart)
        offset += size
        column += half
    return jnp.concatenate(outs, axis=-1)

def reference(visual_q, visual_key_input, visual_v, text_k, text_v, text_mask, slab_order, q_gain, key_norm_gain, w_out):
    index = jnp.arange(VIS, dtype=jnp.int32)
    owner = index // TOK_DEV
    local = index % TOK_DEV
    frame = local // (SLAB_H * WIDE)
    height = slab_order[owner] * SLAB_H + local // WIDE % SLAB_H
    column = local % WIDE
    cosine_table, sine_table = angles(frame, height, column)
    queries = (apply_rotation(apply_norm(visual_q, q_gain), cosine_table, sine_table) / jnp.sqrt(jnp.float32(HEAD))).astype(jnp.bfloat16)
    visual_key_rows = apply_rotation(apply_norm(visual_key_input, key_norm_gain), cosine_table, sine_table).astype(jnp.bfloat16)
    textual_keys = apply_norm(text_k, key_norm_gain).astype(jnp.bfloat16)
    key_rows = jnp.concatenate([visual_key_rows, textual_keys], axis=0).astype(jnp.float32)
    values = jnp.concatenate([visual_v, text_v], axis=0).reshape(VIS + TEXT, HEADS, HEAD).astype(jnp.float32)
    valid = jnp.concatenate([jnp.ones((VIS,), jnp.int32), text_mask.astype(jnp.int32)]) == 1
    blocks = queries.reshape(VIS // 256, 256, HEADS, HEAD) if VIS % 256 == 0 else queries.reshape(1, VIS, HEADS, HEAD)

    def attend(block):
        scores = jnp.einsum('qhd,khd->qhk', block.astype(jnp.float32), key_rows)
        scores = jnp.where(valid[None, None, :], scores, -jnp.inf)
        top = lax.optimization_barrier(jnp.max(scores, axis=-1, keepdims=True))
        probs = jnp.exp(scores - top)
        total = lax.optimization_barrier(jnp.sum(probs, axis=-1))
        weights = probs.astype(jnp.bfloat16).astype(jnp.float32)
        mixed = jnp.einsum('qhk,khd->qhd', weights, values)
        return (mixed / total[..., None]).astype(jnp.bfloat16)
    heads_out = lax.map(attend, blocks).reshape(VIS, HEADS * HEAD)
    group = HEADS * HEAD // N_TP
    summed = jnp.zeros((VIS, D), jnp.float32)
    for member in range(N_TP):
        partial_value = jnp.dot(heads_out[:, member * group:(member + 1) * group], w_out[member * group:(member + 1) * group, :], preferred_element_type=jnp.float32).astype(jnp.bfloat16)
        partial_value = lax.optimization_barrier(partial_value)
        summed = summed + partial_value.astype(jnp.float32)
    return summed.astype(jnp.bfloat16)
```

```python
import functools

import jax
import jax.numpy as jnp
import numpy as np
from jax import lax
from jax.experimental import pallas as pl
from jax.experimental.pallas import tpu as pltpu
from jax.sharding import PartitionSpec as P

SLAB_H = 2
WIDE = 32
HEAD = 128
PARTS = (32, 48, 48)
NEGATIVE = -1e30
MESH = pl.DeviceIdType.MESH
F32 = jnp.float32
BF16 = jnp.bfloat16
LEAD_Y, LEAD_Z, LEAD_Q = 2, 2, 2
GROUP = 4
STATS = 16
HUB_SLOTS = 8


def lane_constants():
    lanes = np.zeros((8, HEAD), np.float32)
    perm = np.zeros((HEAD, HEAD), np.float32)
    offset = 0
    for index, size in enumerate(PARTS):
        half = size // 2
        f = np.float32(10000.0) ** (-np.arange(half, dtype=np.float32) / np.float32(half))
        lanes[0, offset : offset + half] = f
        lanes[0, offset + half : offset + size] = f
        lanes[1, offset : offset + size] = index
        lanes[2, offset : offset + half] = 1.0
        for j in range(half):
            perm[offset + half + j, offset + j] = -1.0
            perm[offset + j, offset + half + j] = 1.0
        offset += size
    return lanes, perm


def nt(a, b):
    return lax.dot_general(a, b, (((1,), (1,)), ((), ())), preferred_element_type=F32)


def tn(a, b):
    return lax.dot_general(a, b, (((0,), (0,)), ((), ())), preferred_element_type=F32)


def kernel(
    n, chunks,
    slab_ref, q_hbm, k_hbm, v_hbm, tk_hbm, tv_hbm, mask_ref, qg_ref, kg_ref, lanes_ref, perm_ref, w_ref,
    out_ref,
    kv, tb, qs, o_send, o_recv, o_own, lse_own, o_all, w, w_far, h_mine, h_send, h_recv, acc, tabs,
    q_ref, k_ref, v_ref, tk_ref, tv_ref,
    kv_ss, kv_rs, tb_ss, tb_rs, q_ss, q_rs, o_ss, o_rs, h_ss, h_rs, wf_ss, wf_rs, w_sem, in_sem,
):
    rows, width = q_ref.shape
    heads = width // HEAD
    trows = tk_ref.shape[0]
    keys = rows + trows
    a = n // GROUP
    g, s, t = lax.axis_index("grp"), lax.axis_index("seq"), lax.axis_index("tp")
    u, low = s // GROUP, s % GROUP
    zdev = (g, s + 2 - 4 * (low // 2), t)
    ydev = (g, s + 1 - 2 * (low % 2), t)
    tdev = (g, s, 1 - t)
    fwd = [(g, lax.rem(u + j, a) * GROUP + low, t) for j in range(a)]
    back = [(g, lax.rem(u + a - j, a) * GROUP + low, t) for j in range(a)]

    barrier = pltpu.get_barrier_semaphore()
    friends = [zdev, ydev, tdev] + fwd[1:]
    for dev in friends:
        pl.semaphore_signal(barrier, inc=1, device_id=dev, device_id_type=MESH)

    loads = [
        pltpu.make_async_copy(x, y, in_sem.at[i])
        for i, (x, y) in enumerate(
            ((k_hbm, k_ref), (tk_hbm, tk_ref), (v_hbm, v_ref), (tv_hbm, tv_ref), (q_hbm, q_ref))
        )
    ]
    for load in loads:
        load.start()
    w_copy = pltpu.make_async_copy(w_ref, w, w_sem)
    w_copy.start()

    def remote(src, dst, ss, rs, dev):
        return pltpu.make_async_remote_copy(
            src_ref=src, dst_ref=dst, send_sem=ss, recv_sem=rs, device_id=dev, device_id_type=MESH
        )

    def kv_z(h):
        return remote(kv.at[0, h], kv.at[1, h], kv_ss.at[0, h], kv_rs.at[0, h], zdev)

    def kv_y(h):
        return remote(kv.at[0, h], kv.at[2, h], kv_ss.at[1, h], kv_rs.at[1, h], ydev)

    def kv_relay(h):
        return remote(kv.at[1, h], kv.at[3, h], kv_ss.at[2, h], kv_rs.at[2, h], ydev)

    def q_move(j, h):
        return remote(qs.at[0, h], qs.at[j, h], q_ss.at[j - 1, h], q_rs.at[j - 1, h], fwd[j])

    def o_move(j, h):
        return remote(
            o_send.at[j - 1, h], o_recv.at[j - 1, h], o_ss.at[j - 1, h], o_rs.at[j - 1, h], back[j]
        )

    tb_z = remote(tb.at[0], tb.at[1], tb_ss.at[0], tb_rs.at[0], zdev)
    tb_y = remote(tb.at[0], tb.at[2], tb_ss.at[1], tb_rs.at[1], ydev)
    tb_relay = remote(tb.at[1], tb.at[3], tb_ss.at[2], tb_rs.at[2], ydev)

    freq, part, lead = lanes_ref[0:1, :], lanes_ref[1:2, :], lanes_ref[2:3, :]
    blocks = rows // WIDE
    block = lax.broadcasted_iota(jnp.int32, (blocks, HEAD), 0)
    slab = slab_ref[0] * SLAB_H
    place = jnp.where(part < 0.5, (block // SLAB_H).astype(F32), (slab + block % SLAB_H).astype(F32)) * freq
    across = lax.broadcasted_iota(jnp.int32, (WIDE, HEAD), 0).astype(F32) * freq
    trig = (jnp.cos(place), jnp.cos(across)), (jnp.sin(place), jnp.sin(across))

    def partner(x):
        wide = jnp.broadcast_to(x, (8, HEAD))
        near, far = PARTS[0] // 2, PARTS[1] // 2
        after = jnp.where(part < 0.5, pltpu.roll(wide, HEAD - near, 1), pltpu.roll(wide, HEAD - far, 1))
        before = jnp.where(part < 0.5, pltpu.roll(wide, near, 1), pltpu.roll(wide, far, 1))
        return jnp.where(lead > 0.5, after, before)[0:1]

    def h_move(h):
        return remote(h_send.at[h], h_recv.at[h], h_ss.at[h], h_rs.at[h], tdev)

    w_move = remote(w, w_far, wf_ss, wf_rs, tdev)

    scale_q = F32(1.0) / jnp.sqrt(F32(HEAD))
    kg = kg_ref[...]
    qg = qg_ref[...] * scale_q
    for which, (by_block, by_column) in enumerate(trig):
        for gain, index in ((qg, 0), (kg, 2)):
            gain = gain if which == 0 else partner(gain)
            for i in range(blocks):
                full = jnp.where(part < 1.5, by_block[i : i + 1], by_column)
                tabs[index + which, i * WIDE : (i + 1) * WIDE, :] = full * gain
    row = lax.broadcasted_iota(jnp.int32, (trows, trows), 0)
    col = lax.broadcasted_iota(jnp.int32, (trows, trows), 1)
    mark = jnp.where((row == col) & (mask_ref[...] != 1), F32(NEGATIVE), F32(0.0))
    tb[0] = jnp.broadcast_to(jnp.sum(mark, axis=1, keepdims=True), (trows, HEAD)).astype(BF16)

    def norm_scale(x32):
        return lax.rsqrt(jnp.mean(x32 * x32, axis=-1, keepdims=True) + 0.05)

    def rotated(x, which):
        x32 = x.astype(F32)
        turned = jnp.dot(x, perm_ref[...], preferred_element_type=F32)
        return ((x32 * tabs[which] + turned * tabs[which + 1]) * norm_scale(x32)).astype(BF16)

    def prepare(h):
        cols = pl.ds(pl.multiple_of(h * HEAD, HEAD), HEAD)
        kv[0, h, 0:rows, :] = rotated(k_ref[:, cols], 2)
        tk = tk_ref[:, cols].astype(F32)
        kv[0, h, rows:keys, :] = (tk * norm_scale(tk) * kg).astype(BF16)
        kv[0, h, keys : keys + rows, :] = v_ref[:, cols]
        kv[0, h, keys + rows : 2 * keys, :] = tv_ref[:, cols]
        qs[0, h] = rotated(q_ref[:, cols], 0)

    def send(h, ready):
        for lead, start in ((LEAD_Y, send_y), (LEAD_Z, send_z), (LEAD_Q, send_q)):
            if ready is None:

                @pl.when(h < lead)
                def _(start=start):
                    start(h)
            else:

                @pl.when(h + lead < heads)
                def _(start=start, lead=lead):
                    start(h + lead)

    def send_y(h):
        kv_y(h).start()

    def send_z(h):
        kv_z(h).start()

    def send_q(h):
        for j in range(1, a):
            q_move(j, h).start()

    for load in loads:
        load.wait()
    prepare(0)
    pl.semaphore_wait(barrier, len(friends))
    tb_z.start()
    tb_y.start()
    send(0, None)

    def first(h, c):
        prepare(h)
        send(h, None)
        return c

    lax.fori_loop(1, heads, first, 0)
    tb_z.wait_recv()
    tb_relay.start()
    kv_z(0).wait_recv()
    kv_relay(0).start()
    w_copy.wait()
    w_move.start()
    half = rows // 2

    def attend(j, h):
        queries = qs[j, h]
        scores = []
        top = None
        for slot in range(GROUP):
            sc = nt(kv[slot, h, 0:keys, :], queries)
            mark = tb[slot].astype(F32)
            mark = jnp.concatenate([mark] * (rows // HEAD), axis=1)
            sc = jnp.concatenate([sc[0:rows], sc[rows:keys] + mark], axis=0)
            peak = jnp.max(sc, axis=0, keepdims=True)
            top = peak if top is None else jnp.maximum(top, peak)
            scores.append(sc)
        total = None
        acc = None
        for slot in range(GROUP):
            p = jnp.exp(scores[slot] - top)
            part = jnp.sum(p, axis=0, keepdims=True)
            mixed = tn(kv[slot, h, keys : 2 * keys, :], p.astype(BF16))
            total = part if total is None else total + part
            acc = mixed if acc is None else acc + mixed
        return acc / total, top + jnp.log(total)

    def main(h, c):
        @pl.when(h + 1 < heads)
        def _():
            kv_z(h + 1).wait_recv()
            kv_relay(h + 1).start()

        send(h, True)

        kv_y(h).wait_recv()

        @pl.when(h == 0)
        def _():
            tb_y.wait_recv()
            tb_relay.wait_recv()

        for j in range(1, a):
            q_move(j, h).wait_recv()
        kv_relay(h).wait_recv()
        for j in range(1, a):
            o, lse = attend(j, h)
            high = lse.astype(BF16)
            rest = lse - high.astype(F32)
            mid = rest.astype(BF16)
            tail = (rest - mid.astype(F32)).astype(BF16)
            o_send[j - 1, h, HEAD : HEAD + 16, :] = jnp.concatenate(
                [high.astype(F32), mid.astype(F32), tail.astype(F32), jnp.zeros((13, rows), F32)], axis=0
            ).astype(BF16)
            o_send[j - 1, h, 0:HEAD, :] = o.astype(BF16)
            o_move(j, h).start()
        o, lse = attend(0, h)
        o_own[h] = o
        lse_own[h] = jnp.broadcast_to(lse, (8, rows))

        @pl.when(h > 0)
        def _():
            merge(h - 1)

        return c

    def merge(h):
        lses = [lse_own[h][0:1]]
        parts = [o_own[h]]
        for j in range(1, a):
            o_move(j, h).wait_recv()
            stats = o_recv[j - 1, h, HEAD : HEAD + 16, :].astype(F32)
            lses.append(stats[0:1] + stats[1:2] + stats[2:3])
            parts.append(o_recv[j - 1, h, 0:HEAD, :].astype(F32))
        top = functools.reduce(jnp.maximum, lses)
        shares = [jnp.exp(x - top) for x in lses]
        total = functools.reduce(jnp.add, shares)
        o = functools.reduce(jnp.add, [x * y for x, y in zip(parts, shares)]) / total
        o_all[...] = o.astype(BF16)
        h_send[h] = o_all[:, pl.ds(pl.multiple_of((1 - t) * half, half), half)].T
        h_move(h).start()
        cols = pl.ds(pl.multiple_of(h * HEAD, HEAD), HEAD)
        h_mine[:, cols] = o_all[:, pl.ds(pl.multiple_of(t * half, half), half)].T

    lax.fori_loop(0, heads, main, 0)

    step = w.shape[1] // chunks
    spans = [slice(i * step, (i + 1) * step) for i in range(chunks)]
    early = (heads - 1) * HEAD

    def dot(x, y):
        return jnp.dot(x, y, preferred_element_type=F32)

    for span in spans:
        acc[0, :, span] = dot(h_mine[:, :early], w[:early, span])
    w_move.wait_recv()
    for h in range(heads - 1):
        h_move(h).wait_recv()
    theirs = jnp.concatenate([h_recv[h] for h in range(heads - 1)], axis=1)
    for span in spans:
        acc[1, :, span] = dot(theirs, w_far[:early, span])
    merge(heads - 1)
    for span in spans:
        acc[0, :, span] += dot(h_mine[:, early:], w[early:, span])
    h_move(heads - 1).wait_recv()
    for span in spans:
        far = acc[1, :, span] + dot(h_recv[heads - 1], w_far[early:, span])
        near = acc[0, :, span]
        out_ref[:, span] = (near.astype(BF16).astype(F32) + far.astype(BF16).astype(F32)).astype(BF16)

    def drain(h, c):
        kv_z(h).wait_send()
        kv_y(h).wait_send()
        kv_relay(h).wait_send()
        h_move(h).wait_send()
        for j in range(1, a):
            q_move(j, h).wait_send()
            o_move(j, h).wait_send()
        return c

    lax.fori_loop(0, heads, drain, 0)
    tb_z.wait_send()
    tb_y.wait_send()
    tb_relay.wait_send()
    w_move.wait_send()


def hub_kernel(
    chunks,
    slab_ref, q_hbm, k_hbm, v_hbm, tk_hbm, tv_hbm, mask_ref, qg_ref, kg_ref, lanes_ref, perm_ref, w_ref,
    out_ref,
    mine, held, tb, q_mine, q_held, o_send, o_recv, scores_a, scores_b, o_all, w, w_far, h_mine, h_send, h_recv,
    acc, tabs, q_ref, k_ref, v_ref, tk_ref, tv_ref,
    kv_ss, kv_rs, tb_ss, tb_rs, q_ss, q_rs, o_ss, o_rs, h_ss, h_rs, wf_ss, wf_rs, w_sem, in_sem,
):
    rows, width = q_ref.shape
    heads = width // HEAD
    trows = tk_ref.shape[0]
    keys = rows + trows
    half = rows // 2
    pairs = heads // 2
    g, s, t = lax.axis_index("grp"), lax.axis_index("seq"), lax.axis_index("tp")
    u, low = s // GROUP, s % GROUP
    row, col = low // 2, low % 2
    inner = row + u == 1
    outer = row + u != 1
    aside = 1 - 2 * col

    def dev(seq):
        return (g, seq, t)

    near_s, far_s, cross_s = s + 2 - 4 * row, s + 2 - 4 * u, s + GROUP - 2 * GROUP * u
    near, far, cross, ydev = dev(near_s), dev(far_s), dev(cross_s), dev(s + aside)
    near_y, far_y, cross_y = dev(near_s + aside), dev(far_s + aside), dev(cross_s + aside)
    tdev = (g, s, 1 - t)

    barrier = pltpu.get_barrier_semaphore()
    friends = [near, ydev, tdev]
    for friend in friends:
        pl.semaphore_signal(barrier, inc=1, device_id=friend, device_id_type=MESH)

    @pl.when(inner)
    def _():
        pl.semaphore_signal(barrier, inc=1, device_id=far, device_id_type=MESH)

    loads = [
        pltpu.make_async_copy(x, y, in_sem.at[i])
        for i, (x, y) in enumerate(
            ((q_hbm, q_ref), (k_hbm, k_ref), (tk_hbm, tk_ref), (v_hbm, v_ref), (tv_hbm, tv_ref))
        )
    ]
    for load in loads:
        load.start()
    w_copy = pltpu.make_async_copy(w_ref, w, w_sem)
    w_copy.start()

    def remote(src, dst, ss, rs, to):
        return pltpu.make_async_remote_copy(
            src_ref=src, dst_ref=dst, send_sem=ss, recv_sem=rs, device_id=to, device_id_type=MESH
        )

    def mine_on(i):
        return 2 * i + col

    def mine_off(i):
        return 2 * i + 1 - col

    def kv_move(src, slot, kind, i, to):
        return remote(src, held.at[slot - 1, i], kv_ss.at[kind, i], kv_rs.at[slot - 1, i], to)

    def kv_in(i):
        return kv_move(mine.at[mine_on(i)], 1, 0, i, near)

    def kv_off(i):
        return kv_move(mine.at[mine_off(i)], 2, 1, i, ydev)

    def kv_relay(i):
        return kv_move(held.at[1, i], 3, 2, i, near)

    def q_move(src, slot, kind, i, to):
        return remote(src, q_held.at[slot - 1, i], q_ss.at[kind, i], q_rs.at[slot - 1, i], to)

    def q_in(i):
        return q_move(q_mine.at[mine_on(i)], 1, 0, i, near)

    def q_off(i):
        return q_move(q_mine.at[mine_off(i)], 4, 1, i, ydev)

    def q_relay(i):
        return q_move(q_held.at[3, i], 5, 2, i, near)

    def q_far(slot, i):
        if slot == 2:
            return q_move(q_mine.at[mine_on(i)], 2, 0, i, far)
        kind, start = {3: (2, 1), 6: (3, 4), 7: (4, 5)}[slot]
        return q_move(q_held.at[start - 1, i], slot, kind, i, far)

    def o_move(slot, i):
        index, to = {
            1: (0, near), 4: (0, ydev), 5: (0, near_y),
            2: (1, far), 3: (1, cross), 6: (1, far_y), 7: (1, cross_y),
        }[slot]
        h = mine_on(i)
        return remote(
            o_send.at[slot - 1, i], o_recv.at[index, h], o_ss.at[slot - 1, i], o_rs.at[index, h], to
        )

    def h_move(h):
        return remote(h_send.at[h], h_recv.at[h], h_ss.at[h], h_rs.at[h], tdev)

    w_move = remote(w, w_far, wf_ss, wf_rs, tdev)
    tb_in = remote(tb.at[0], tb.at[1], tb_ss.at[0], tb_rs.at[0], near)
    tb_y = remote(tb.at[0], tb.at[2], tb_ss.at[1], tb_rs.at[1], ydev)
    tb_relay = remote(tb.at[2], tb.at[3], tb_ss.at[2], tb_rs.at[2], near)

    freq, part, lead = lanes_ref[0:1, :], lanes_ref[1:2, :], lanes_ref[2:3, :]
    blocks = rows // WIDE
    block = lax.broadcasted_iota(jnp.int32, (blocks, HEAD), 0)
    slab = slab_ref[0] * SLAB_H
    place = jnp.where(part < 0.5, (block // SLAB_H).astype(F32), (slab + block % SLAB_H).astype(F32)) * freq
    across = lax.broadcasted_iota(jnp.int32, (WIDE, HEAD), 0).astype(F32) * freq
    trig = (jnp.cos(place), jnp.cos(across)), (jnp.sin(place), jnp.sin(across))

    def partner(x):
        wide = jnp.broadcast_to(x, (8, HEAD))
        near, far = PARTS[0] // 2, PARTS[1] // 2
        after = jnp.where(part < 0.5, pltpu.roll(wide, HEAD - near, 1), pltpu.roll(wide, HEAD - far, 1))
        before = jnp.where(part < 0.5, pltpu.roll(wide, near, 1), pltpu.roll(wide, far, 1))
        return jnp.where(lead > 0.5, after, before)[0:1]

    scale_q = F32(1.0) / jnp.sqrt(F32(HEAD))
    kg = kg_ref[...]
    qg = qg_ref[...] * scale_q
    for which, (by_block, by_column) in enumerate(trig):
        for gain, index in ((qg, 0), (kg, 2)):
            gain = gain if which == 0 else partner(gain)
            for i in range(blocks):
                full = jnp.where(part < 1.5, by_block[i : i + 1], by_column)
                tabs[index + which, i * WIDE : (i + 1) * WIDE, :] = full * gain
    line = lax.broadcasted_iota(jnp.int32, (trows, trows), 0)
    lane = lax.broadcasted_iota(jnp.int32, (trows, trows), 1)
    mark = jnp.where((line == lane) & (mask_ref[...] != 1), F32(NEGATIVE), F32(0.0))
    tb[0] = jnp.broadcast_to(jnp.sum(mark, axis=1, keepdims=True), (trows, HEAD)).astype(BF16)

    def norm_scale(x32):
        return lax.rsqrt(jnp.mean(x32 * x32, axis=-1, keepdims=True) + 0.05)

    def rotated(x, which):
        x32 = x.astype(F32)
        turned = jnp.dot(x, perm_ref[...], preferred_element_type=F32)
        return ((x32 * tabs[which] + turned * tabs[which + 1]) * norm_scale(x32)).astype(BF16)

    def prepare_q(h):
        q_mine[h] = rotated(q_ref[:, pl.ds(pl.multiple_of(h * HEAD, HEAD), HEAD)], 0)

    def prepare_kv(h):
        cols = pl.ds(pl.multiple_of(h * HEAD, HEAD), HEAD)
        mine[h, 0:rows, :] = rotated(k_ref[:, cols], 2)
        tk = tk_ref[:, cols].astype(F32)
        mine[h, rows:keys, :] = (tk * norm_scale(tk) * kg).astype(BF16)
        mine[h, keys : keys + rows, :] = v_ref[:, cols]
        mine[h, keys + rows : 2 * keys, :] = tv_ref[:, cols]

    def side(slot, i, part):
        where = pl.ds(part * keys, keys)
        return held[slot - 1, i, where, :] if slot else mine[mine_on(i), where, :]

    def score(slot, i, where):
        queries = q_held[slot - 1, i] if slot else q_mine[mine_on(i)]
        top = None
        for n in range(GROUP):
            sc = nt(side(n, i, 0), queries)
            mark = tb[n].astype(F32)
            mark = jnp.concatenate([mark] * (rows // HEAD), axis=1)
            sc = jnp.concatenate([sc[0:rows], sc[rows:keys] + mark], axis=0)
            where[n] = sc
            peak = jnp.max(sc, axis=0, keepdims=True)
            top = peak if top is None else jnp.maximum(top, peak)
        return top

    def weigh(i, where, top):
        total = None
        mixed = None
        for n in range(GROUP):
            p = jnp.exp(where[n] - top)
            amount = jnp.sum(p, axis=0, keepdims=True)
            got = tn(side(n, i, 1), p.astype(BF16))
            total = amount if total is None else total + amount
            mixed = got if mixed is None else mixed + got
        return mixed / total, top + jnp.log(total)

    wides = rows // HEAD

    def pack(to, o, lse):
        high = lse.astype(BF16).astype(F32)
        rest = lse - high
        mid = rest.astype(BF16).astype(F32)
        pieces = [x[:, i * HEAD : (i + 1) * HEAD] for x in (high, mid, rest - mid) for i in range(wides)]
        pieces.append(jnp.zeros((STATS - 3 * wides, HEAD), F32))
        to[rows : rows + STATS, :] = jnp.concatenate(pieces, axis=0).astype(BF16)
        for i in range(wides):
            to[i * HEAD : (i + 1) * HEAD, :] = o[:, i * HEAD : (i + 1) * HEAD].astype(BF16)

    def unpack(index, h):
        o = jnp.concatenate([o_recv[index, h, i * HEAD : (i + 1) * HEAD, :] for i in range(wides)], axis=1)
        stats = o_recv[index, h, rows : rows + STATS, :].astype(F32)
        levels = [
            jnp.concatenate([stats[k * wides + i : k * wides + i + 1] for i in range(wides)], axis=1)
            for k in range(3)
        ]
        return o.astype(F32), levels[0] + levels[1] + levels[2]

    def merge(h):
        @pl.when(jnp.logical_or(outer, h % 2 != col))
        def _():
            remote(
                o_send.at[0, 0], o_recv.at[0, h], o_ss.at[0, 0], o_rs.at[0, h], near
            ).wait_recv()

        remote(o_send.at[0, 0], o_recv.at[1, h], o_ss.at[0, 0], o_rs.at[1, h], near).wait_recv()
        (o, lse), (o_, lse_) = unpack(0, h), unpack(1, h)
        share = 1.0 / (1.0 + jnp.exp(lse_ - lse))
        o_all[...] = (o * share + o_ * (1.0 - share)).astype(BF16)
        h_send[h] = o_all[:, pl.ds(pl.multiple_of((1 - t) * half, half), half)].T
        h_move(h).start()
        cols = pl.ds(pl.multiple_of(h * HEAD, HEAD), HEAD)
        h_mine[:, cols] = o_all[:, pl.ds(pl.multiple_of(t * half, half), half)].T

    loads[0].wait()
    prepare_q(mine_off(0))
    prepare_q(mine_on(0))

    @pl.when(inner)
    def _():
        pl.semaphore_wait(barrier, len(friends) + 1)
        q_far(2, 0).start()

    @pl.when(outer)
    def _():
        pl.semaphore_wait(barrier, len(friends))
        q_in(0).start()
        tb_in.start()

    q_off(0).start()
    tb_y.start()
    for load in loads[1:]:
        load.wait()
    prepare_kv(mine_on(0))

    @pl.when(outer)
    def _():
        kv_in(0).start()

    def queries(i, c):
        prepare_q(mine_off(i))
        q_off(i).start()
        prepare_q(mine_on(i))

        @pl.when(inner)
        def _():
            q_far(2, i).start()

        @pl.when(outer)
        def _():
            q_in(i).start()

        return c

    lax.fori_loop(1, pairs, queries, 0)
    prepare_kv(mine_off(0))
    kv_off(0).start()

    def keep(i, c):
        prepare_kv(mine_off(i))
        kv_off(i).start()
        prepare_kv(mine_on(i))
        return c

    lax.fori_loop(1, pairs, keep, 0)

    @pl.when(outer)
    def _():
        tb_y.wait_recv()
        tb_relay.start()

        def pass_queries(i, c):
            q_off(i).wait_recv()
            q_relay(i).start()
            return c

        lax.fori_loop(0, pairs, pass_queries, 0)

        def pass_keys(i, c):
            @pl.when(i > 0)
            def _():
                kv_in(i).start()

            kv_off(i).wait_recv()
            kv_relay(i).start()
            return c

        lax.fori_loop(0, pairs, pass_keys, 0)

    w_copy.wait()
    w_move.start()

    @pl.when(outer)
    def _():
        def collect(h, c):
            merge(h)
            return c

        lax.fori_loop(0, heads - 2, collect, 0)

    @pl.when(inner)
    def _():
        def onward(i, c):
            q_in(i).wait_recv()
            q_far(3, i).start()
            q_off(i).wait_recv()
            q_far(6, i).start()
            return c

        def onward_last(i, c):
            q_relay(i).wait_recv()
            q_far(7, i).start()
            return c

        lax.fori_loop(0, pairs, onward, 0)
        lax.fori_loop(0, pairs, onward_last, 0)
        tb_in.wait_recv()
        tb_y.wait_recv()
        tb_relay.wait_recv()

        def main(i, c):
            kv_in(i).wait_recv()
            kv_off(i).wait_recv()

            for slot in (2, 3, 6, 7):
                q_far(slot, i).wait_recv()
            kv_relay(i).wait_recv()
            order = (7, 3, 6, 2, 5, 1, 4, 0)
            top = score(order[0], i, scores_a)
            for n, slot in enumerate(order):
                here, there = ((scores_a, scores_b), (scores_b, scores_a))[n % 2]
                after = score(order[n + 1], i, there) if n + 1 < HUB_SLOTS else None
                o, lse = weigh(i, here, top)
                top = after
                if slot:
                    pack(o_send.at[slot - 1, i], o, lse)
                    o_move(slot, i).start()
                else:
                    pack(o_recv.at[0, mine_on(i)], o, lse)

            @pl.when(i > 0)
            def _():
                merge(2 * i - 2)
                merge(2 * i - 1)

            return c

        lax.fori_loop(0, pairs, main, 0)

    step = w.shape[1] // chunks
    spans = [slice(i * step, (i + 1) * step) for i in range(chunks)]
    early = (heads - 2) * HEAD

    def dot(x, y):
        return jnp.dot(x, y, preferred_element_type=F32)

    for span in spans:
        acc[0, :, span] = dot(h_mine[:, :early], w[:early, span])
    w_move.wait_recv()
    for h in range(heads - 2):
        h_move(h).wait_recv()
    theirs = jnp.concatenate([h_recv[h] for h in range(heads - 2)], axis=1)
    for span in spans:
        acc[1, :, span] = dot(theirs, w_far[:early, span])

    merge(heads - 2)
    merge(heads - 1)

    for span in spans:
        acc[0, :, span] += dot(h_mine[:, early:], w[early:, span])
    h_move(heads - 2).wait_recv()
    h_move(heads - 1).wait_recv()
    last = jnp.concatenate([h_recv[heads - 2], h_recv[heads - 1]], axis=1)
    for span in spans:
        theirs = acc[1, :, span] + dot(last, w_far[early:, span])
        mine_too = acc[0, :, span]
        out_ref[:, span] = (mine_too.astype(BF16).astype(F32) + theirs.astype(BF16).astype(F32)).astype(BF16)

    def drain(i, c):
        q_off(i).wait_send()
        kv_off(i).wait_send()

        @pl.when(inner)
        def _():
            for slot in (2, 3, 6, 7):
                q_far(slot, i).wait_send()
            for slot in range(1, HUB_SLOTS):
                o_move(slot, i).wait_send()

        @pl.when(outer)
        def _():
            q_in(i).wait_send()
            kv_in(i).wait_send()
            q_relay(i).wait_send()
            kv_relay(i).wait_send()

        return c

    lax.fori_loop(0, pairs, drain, 0)

    tb_y.wait_send()

    @pl.when(outer)
    def _():
        tb_in.wait_send()
        tb_relay.wait_send()

    def settle(h, c):
        h_move(h).wait_send()
        return c

    lax.fori_loop(0, heads, settle, 0)
    w_move.wait_send()


def hub_scratch(rows, trows, heads, model, w_shape, inputs):
    keys, half, pairs = rows + trows, rows // 2, heads // 2
    dma = pltpu.SemaphoreType.DMA
    return [
        pltpu.VMEM((heads, 2 * keys, HEAD), BF16),
        pltpu.VMEM((3, pairs, 2 * keys, HEAD), BF16),
        pltpu.VMEM((GROUP, trows, HEAD), BF16),
        pltpu.VMEM((heads, rows, HEAD), BF16),
        pltpu.VMEM((HUB_SLOTS - 1, pairs, rows, HEAD), BF16),
        pltpu.VMEM((HUB_SLOTS - 1, pairs, rows + STATS, HEAD), BF16),
        pltpu.VMEM((2, heads, rows + STATS, HEAD), BF16),
        pltpu.VMEM((GROUP, keys, rows), F32),
        pltpu.VMEM((GROUP, keys, rows), F32),
        pltpu.VMEM((HEAD, rows), BF16),
        pltpu.VMEM(w_shape, BF16),
        pltpu.VMEM(w_shape, BF16),
        pltpu.VMEM((half, heads * HEAD), BF16),
        pltpu.VMEM((heads, half, HEAD), BF16),
        pltpu.VMEM((heads, half, HEAD), BF16),
        pltpu.VMEM((2, half, model), F32),
        pltpu.VMEM((4, rows, HEAD), F32),
        *[pltpu.VMEM(x.shape, BF16) for x in inputs],
        dma((3, pairs)), dma((3, pairs)), dma((3,)), dma((3,)),
        dma((5, pairs)), dma((HUB_SLOTS - 1, pairs)), dma((HUB_SLOTS - 1, pairs)), dma((2, heads)),
        dma((heads,)), dma((heads,)), dma, dma, dma, dma((5,)),
    ]


def body(
    n,
    visual_q, visual_key_input, visual_v, text_k, text_v, text_mask, slab_order, q_gain, key_norm_gain, w_out,
):
    rows, width = visual_q.shape
    heads = width // HEAD
    model = w_out.shape[1]
    a = n // GROUP
    trows = -(-text_k.shape[0] // 16) * 16
    pad = trows - text_k.shape[0]
    if pad:
        text_k = jnp.pad(text_k, ((0, pad), (0, 0)))
        text_v = jnp.pad(text_v, ((0, pad), (0, 0)))
        text_mask = jnp.pad(text_mask, (0, pad))
    lanes, perm = lane_constants()
    chunks = 6 if model % (6 * HEAD) == 0 else 1
    keys = rows + trows
    half = rows // 2
    peers = a - 1
    vm = pl.BlockSpec(memory_space=pltpu.VMEM)
    anywhere = pl.BlockSpec(memory_space=pl.ANY)
    dma = pltpu.SemaphoreType.DMA
    operands = (
        slab_order, visual_q, visual_key_input, visual_v, text_k, text_v, text_mask[None], q_gain[None],
        key_norm_gain[None], jnp.asarray(lanes), jnp.asarray(perm, BF16), w_out,
    )
    if n == 2 * GROUP and rows % HEAD == 0 and heads % 2 == 0:
        run = functools.partial(hub_kernel, chunks)
        scratch = hub_scratch(rows, trows, heads, model, w_out.shape, operands[1:6])
    else:
        run = functools.partial(kernel, n, chunks)
        scratch = [
                pltpu.VMEM((GROUP, heads, 2 * keys, HEAD), BF16),
                pltpu.VMEM((GROUP, trows, HEAD), BF16),
                pltpu.VMEM((a, heads, rows, HEAD), BF16),
                pltpu.VMEM((peers, heads, HEAD + 16, rows), BF16),
                pltpu.VMEM((peers, heads, HEAD + 16, rows), BF16),
                pltpu.VMEM((heads, HEAD, rows), F32),
                pltpu.VMEM((heads, 8, rows), F32),
                pltpu.VMEM((HEAD, rows), BF16),
                pltpu.VMEM(w_out.shape, BF16),
                pltpu.VMEM(w_out.shape, BF16),
                pltpu.VMEM((half, width), BF16),
                pltpu.VMEM((heads, half, HEAD), BF16),
                pltpu.VMEM((heads, half, HEAD), BF16),
                pltpu.VMEM((2, half, model), F32),
                pltpu.VMEM((4, rows, HEAD), F32),
                *[pltpu.VMEM(x.shape, BF16) for x in (visual_q, visual_key_input, visual_v, text_k, text_v)],
                dma((3, heads)), dma((3, heads)), dma((3,)), dma((3,)),
                dma((peers, heads)), dma((peers, heads)), dma((peers, heads)), dma((peers, heads)),
                dma((heads,)), dma((heads,)), dma, dma, dma, dma((5,)),
        ]
    return pl.pallas_call(
        run,
        out_shape=pltpu.VMEM((half, model), BF16),
        in_specs=[pl.BlockSpec(memory_space=pltpu.SMEM)] + [anywhere] * 5 + [vm] * 5 + [anywhere],
        out_specs=vm,
        scratch_shapes=scratch,
        compiler_params=pltpu.CompilerParams(
            collective_id=0, has_side_effects=True, vmem_limit_bytes=60 * 1024 * 1024
        ),
    )(*operands)


def solution(mesh):
    rows = P(("grp", "seq"), "tp")
    placed = (rows,) * 5 + (P(("grp", "seq")),) * 2 + (P(), P(), P("tp", None))
    return jax.shard_map(
        functools.partial(body, mesh.shape["seq"]),
        mesh=mesh, in_specs=placed, out_specs=P(("grp", "seq", "tp"), None), check_vma=False,
    )
```

```python
import functools

import jax
import jax.numpy as jnp
import numpy as np
from jax import lax
from jax.experimental import pallas as pl
from jax.experimental.pallas import tpu as pltpu
from jax.sharding import PartitionSpec as P

SLAB_H = 2
WIDE = 32
HEAD = 128
PARTS = (32, 48, 48)
NEGATIVE = -1e30
MESH = pl.DeviceIdType.MESH
F32 = jnp.float32
BF16 = jnp.bfloat16
LEAD_Y, LEAD_Z, LEAD_Q = 2, 2, 2
GROUP = 4
STATS = 8
HUB_SLOTS = 8


def lane_constants():
    lanes = np.zeros((8, HEAD), np.float32)
    perm = np.zeros((HEAD, HEAD), np.float32)
    offset = 0
    for index, size in enumerate(PARTS):
        half = size // 2
        f = np.float32(10000.0) ** (-np.arange(half, dtype=np.float32) / np.float32(half))
        lanes[0, offset : offset + half] = f
        lanes[0, offset + half : offset + size] = f
        lanes[1, offset : offset + size] = index
        lanes[2, offset : offset + half] = 1.0
        for j in range(half):
            perm[offset + half + j, offset + j] = -1.0
            perm[offset + j, offset + half + j] = 1.0
        offset += size
    return lanes, perm


def nt(a, b):
    return lax.dot_general(a, b, (((1,), (1,)), ((), ())), preferred_element_type=F32)


def tn(a, b):
    return lax.dot_general(a, b, (((0,), (0,)), ((), ())), preferred_element_type=F32)


def kernel(
    n, chunks,
    slab_ref, q_hbm, k_hbm, v_hbm, tk_hbm, tv_hbm, mask_ref, qg_ref, kg_ref, lanes_ref, perm_ref, w_ref,
    out_ref,
    kv, tb, qs, o_send, o_recv, o_own, lse_own, o_all, w, w_far, h_mine, h_send, h_recv, acc, tabs,
    q_ref, k_ref, v_ref, tk_ref, tv_ref,
    kv_ss, kv_rs, tb_ss, tb_rs, q_ss, q_rs, o_ss, o_rs, h_ss, h_rs, wf_ss, wf_rs, w_sem, in_sem,
):
    rows, width = q_ref.shape
    heads = width // HEAD
    trows = tk_ref.shape[0]
    keys = rows + trows
    a = n // GROUP
    g, s, t = lax.axis_index("grp"), lax.axis_index("seq"), lax.axis_index("tp")
    u, low = s // GROUP, s % GROUP
    zdev = (g, s + 2 - 4 * (low // 2), t)
    ydev = (g, s + 1 - 2 * (low % 2), t)
    tdev = (g, s, 1 - t)
    fwd = [(g, lax.rem(u + j, a) * GROUP + low, t) for j in range(a)]
    back = [(g, lax.rem(u + a - j, a) * GROUP + low, t) for j in range(a)]

    barrier = pltpu.get_barrier_semaphore()
    friends = [zdev, ydev, tdev] + fwd[1:]
    for dev in friends:
        pl.semaphore_signal(barrier, inc=1, device_id=dev, device_id_type=MESH)

    loads = [
        pltpu.make_async_copy(x, y, in_sem.at[i])
        for i, (x, y) in enumerate(
            ((k_hbm, k_ref), (tk_hbm, tk_ref), (v_hbm, v_ref), (tv_hbm, tv_ref), (q_hbm, q_ref))
        )
    ]
    for load in loads:
        load.start()
    w_copy = pltpu.make_async_copy(w_ref, w, w_sem)
    w_copy.start()

    def remote(src, dst, ss, rs, dev):
        return pltpu.make_async_remote_copy(
            src_ref=src, dst_ref=dst, send_sem=ss, recv_sem=rs, device_id=dev, device_id_type=MESH
        )

    def kv_z(h):
        return remote(kv.at[0, h], kv.at[1, h], kv_ss.at[0, h], kv_rs.at[0, h], zdev)

    def kv_y(h):
        return remote(kv.at[0, h], kv.at[2, h], kv_ss.at[1, h], kv_rs.at[1, h], ydev)

    def kv_relay(h):
        return remote(kv.at[1, h], kv.at[3, h], kv_ss.at[2, h], kv_rs.at[2, h], ydev)

    def q_move(j, h):
        return remote(qs.at[0, h], qs.at[j, h], q_ss.at[j - 1, h], q_rs.at[j - 1, h], fwd[j])

    def o_move(j, h):
        return remote(
            o_send.at[j - 1, h], o_recv.at[j - 1, h], o_ss.at[j - 1, h], o_rs.at[j - 1, h], back[j]
        )

    tb_z = remote(tb.at[0], tb.at[1], tb_ss.at[0], tb_rs.at[0], zdev)
    tb_y = remote(tb.at[0], tb.at[2], tb_ss.at[1], tb_rs.at[1], ydev)
    tb_relay = remote(tb.at[1], tb.at[3], tb_ss.at[2], tb_rs.at[2], ydev)

    freq, part, lead = lanes_ref[0:1, :], lanes_ref[1:2, :], lanes_ref[2:3, :]
    blocks = rows // WIDE
    block = lax.broadcasted_iota(jnp.int32, (blocks, HEAD), 0)
    slab = slab_ref[0] * SLAB_H
    place = jnp.where(part < 0.5, (block // SLAB_H).astype(F32), (slab + block % SLAB_H).astype(F32)) * freq
    across = lax.broadcasted_iota(jnp.int32, (WIDE, HEAD), 0).astype(F32) * freq
    trig = (jnp.cos(place), jnp.cos(across)), (jnp.sin(place), jnp.sin(across))

    def partner(x):
        wide = jnp.broadcast_to(x, (8, HEAD))
        near, far = PARTS[0] // 2, PARTS[1] // 2
        after = jnp.where(part < 0.5, pltpu.roll(wide, HEAD - near, 1), pltpu.roll(wide, HEAD - far, 1))
        before = jnp.where(part < 0.5, pltpu.roll(wide, near, 1), pltpu.roll(wide, far, 1))
        return jnp.where(lead > 0.5, after, before)[0:1]

    def h_move(h):
        return remote(h_send.at[h], h_recv.at[h], h_ss.at[h], h_rs.at[h], tdev)

    w_move = remote(w, w_far, wf_ss, wf_rs, tdev)

    scale_q = F32(1.0) / jnp.sqrt(F32(HEAD))
    kg = kg_ref[...]
    qg = qg_ref[...] * scale_q
    for which, (by_block, by_column) in enumerate(trig):
        for gain, index in ((qg, 0), (kg, 2)):
            gain = gain if which == 0 else partner(gain)
            for i in range(blocks):
                full = jnp.where(part < 1.5, by_block[i : i + 1], by_column)
                tabs[index + which, i * WIDE : (i + 1) * WIDE, :] = full * gain
    row = lax.broadcasted_iota(jnp.int32, (trows, trows), 0)
    col = lax.broadcasted_iota(jnp.int32, (trows, trows), 1)
    mark = jnp.where((row == col) & (mask_ref[...] != 1), F32(NEGATIVE), F32(0.0))
    tb[0] = jnp.broadcast_to(jnp.sum(mark, axis=1, keepdims=True), (trows, HEAD)).astype(BF16)

    def norm_scale(x32):
        return lax.rsqrt(jnp.mean(x32 * x32, axis=-1, keepdims=True) + 0.05)

    def rotated(x, which):
        x32 = x.astype(F32)
        turned = jnp.dot(x, perm_ref[...], preferred_element_type=F32)
        return ((x32 * tabs[which] + turned * tabs[which + 1]) * norm_scale(x32)).astype(BF16)

    def prepare(h):
        cols = pl.ds(pl.multiple_of(h * HEAD, HEAD), HEAD)
        kv[0, h, 0:rows, :] = rotated(k_ref[:, cols], 2)
        tk = tk_ref[:, cols].astype(F32)
        kv[0, h, rows:keys, :] = (tk * norm_scale(tk) * kg).astype(BF16)
        kv[0, h, keys : keys + rows, :] = v_ref[:, cols]
        kv[0, h, keys + rows : 2 * keys, :] = tv_ref[:, cols]
        qs[0, h] = rotated(q_ref[:, cols], 0)

    def send(h, ready):
        for lead, start in ((LEAD_Y, send_y), (LEAD_Z, send_z), (LEAD_Q, send_q)):
            if ready is None:

                @pl.when(h < lead)
                def _(start=start):
                    start(h)
            else:

                @pl.when(h + lead < heads)
                def _(start=start, lead=lead):
                    start(h + lead)

    def send_y(h):
        kv_y(h).start()

    def send_z(h):
        kv_z(h).start()

    def send_q(h):
        for j in range(1, a):
            q_move(j, h).start()

    for load in loads:
        load.wait()
    prepare(0)
    pl.semaphore_wait(barrier, len(friends))
    tb_z.start()
    tb_y.start()
    send(0, None)

    def first(h, c):
        prepare(h)
        send(h, None)
        return c

    lax.fori_loop(1, heads, first, 0)
    tb_z.wait_recv()
    tb_relay.start()
    kv_z(0).wait_recv()
    kv_relay(0).start()
    w_copy.wait()
    w_move.start()
    half = rows // 2

    def attend(j, h):
        queries = qs[j, h]
        scores = []
        top = None
        for slot in range(GROUP):
            sc = nt(kv[slot, h, 0:keys, :], queries)
            mark = tb[slot].astype(F32)
            mark = jnp.concatenate([mark] * (rows // HEAD), axis=1)
            sc = jnp.concatenate([sc[0:rows], sc[rows:keys] + mark], axis=0)
            peak = jnp.max(sc, axis=0, keepdims=True)
            top = peak if top is None else jnp.maximum(top, peak)
            scores.append(sc)
        total = None
        acc = None
        for slot in range(GROUP):
            p = jnp.exp(scores[slot] - top)
            part = jnp.sum(p, axis=0, keepdims=True)
            mixed = tn(kv[slot, h, keys : 2 * keys, :], p.astype(BF16))
            total = part if total is None else total + part
            acc = mixed if acc is None else acc + mixed
        return acc / total, top + jnp.log(total)

    def main(h, c):
        @pl.when(h + 1 < heads)
        def _():
            kv_z(h + 1).wait_recv()
            kv_relay(h + 1).start()

        send(h, True)

        kv_y(h).wait_recv()

        @pl.when(h == 0)
        def _():
            tb_y.wait_recv()
            tb_relay.wait_recv()

        for j in range(1, a):
            q_move(j, h).wait_recv()
        kv_relay(h).wait_recv()
        for j in range(1, a):
            o, lse = attend(j, h)
            high = lse.astype(BF16)
            rest = lse - high.astype(F32)
            mid = rest.astype(BF16)
            tail = (rest - mid.astype(F32)).astype(BF16)
            o_send[j - 1, h, HEAD : HEAD + 16, :] = jnp.concatenate(
                [high.astype(F32), mid.astype(F32), tail.astype(F32), jnp.zeros((13, rows), F32)], axis=0
            ).astype(BF16)
            o_send[j - 1, h, 0:HEAD, :] = o.astype(BF16)
            o_move(j, h).start()
        o, lse = attend(0, h)
        o_own[h] = o
        lse_own[h] = jnp.broadcast_to(lse, (8, rows))

        @pl.when(h > 0)
        def _():
            merge(h - 1)

        return c

    def merge(h):
        lses = [lse_own[h][0:1]]
        parts = [o_own[h]]
        for j in range(1, a):
            o_move(j, h).wait_recv()
            stats = o_recv[j - 1, h, HEAD : HEAD + 16, :].astype(F32)
            lses.append(stats[0:1] + stats[1:2] + stats[2:3])
            parts.append(o_recv[j - 1, h, 0:HEAD, :].astype(F32))
        top = functools.reduce(jnp.maximum, lses)
        shares = [jnp.exp(x - top) for x in lses]
        total = functools.reduce(jnp.add, shares)
        o = functools.reduce(jnp.add, [x * y for x, y in zip(parts, shares)]) / total
        o_all[...] = o.astype(BF16)
        h_send[h] = o_all[:, pl.ds(pl.multiple_of((1 - t) * half, half), half)].T
        h_move(h).start()
        cols = pl.ds(pl.multiple_of(h * HEAD, HEAD), HEAD)
        h_mine[:, cols] = o_all[:, pl.ds(pl.multiple_of(t * half, half), half)].T

    lax.fori_loop(0, heads, main, 0)

    step = w.shape[1] // chunks
    spans = [slice(i * step, (i + 1) * step) for i in range(chunks)]
    early = (heads - 1) * HEAD

    def dot(x, y):
        return jnp.dot(x, y, preferred_element_type=F32)

    for span in spans:
        acc[0, :, span] = dot(h_mine[:, :early], w[:early, span])
    w_move.wait_recv()
    for h in range(heads - 1):
        h_move(h).wait_recv()
    theirs = jnp.concatenate([h_recv[h] for h in range(heads - 1)], axis=1)
    for span in spans:
        acc[1, :, span] = dot(theirs, w_far[:early, span])
    merge(heads - 1)
    for span in spans:
        acc[0, :, span] += dot(h_mine[:, early:], w[early:, span])
    h_move(heads - 1).wait_recv()
    for span in spans:
        far = acc[1, :, span] + dot(h_recv[heads - 1], w_far[early:, span])
        near = acc[0, :, span]
        out_ref[:, span] = (near.astype(BF16).astype(F32) + far.astype(BF16).astype(F32)).astype(BF16)

    def drain(h, c):
        kv_z(h).wait_send()
        kv_y(h).wait_send()
        kv_relay(h).wait_send()
        h_move(h).wait_send()
        for j in range(1, a):
            q_move(j, h).wait_send()
            o_move(j, h).wait_send()
        return c

    lax.fori_loop(0, heads, drain, 0)
    tb_z.wait_send()
    tb_y.wait_send()
    tb_relay.wait_send()
    w_move.wait_send()


def hub_kernel(
    chunks,
    slab_hbm, q_hbm, k_hbm, v_hbm, tk_hbm, tv_hbm, mask_hbm, qg_hbm, kg_hbm, lanes_hbm, perm_hbm, w_ref,
    out_ref,
    mine, held, tb, q_mine, q_held, o_send, o_recv, scores_a, scores_b, o_all, w, w_far, h_mine, h_send, h_recv,
    acc, tabs, q_ref, k_ref, v_ref, tk_ref, tv_ref, slab_ref, mask_ref, qg_ref, kg_ref, lanes_ref, perm_ref,
    kv_ss, kv_rs, tb_ss, tb_rs, q_ss, q_rs, o_ss, o_rs, h_ss, h_rs, wf_ss, wf_rs, w_sem, in_sem,
):
    rows, width = q_ref.shape
    heads = width // HEAD
    trows = tk_ref.shape[0]
    keys = rows + trows
    half = rows // 2
    pairs = heads // 2
    g, s, t = lax.axis_index("grp"), lax.axis_index("seq"), lax.axis_index("tp")
    u, low = s // GROUP, s % GROUP
    row, col = low // 2, low % 2
    inner = row + u == 1
    outer = row + u != 1
    aside = 1 - 2 * col

    def dev(seq):
        return (g, seq, t)

    near_s, far_s, cross_s = s + 2 - 4 * row, s + 2 - 4 * u, s + GROUP - 2 * GROUP * u
    near, far, cross, ydev = dev(near_s), dev(far_s), dev(cross_s), dev(s + aside)
    near_y, far_y, cross_y = dev(near_s + aside), dev(far_s + aside), dev(cross_s + aside)
    tdev = (g, s, 1 - t)

    barrier = pltpu.get_barrier_semaphore()
    friends = [near, ydev, tdev]
    for friend in friends:
        pl.semaphore_signal(barrier, inc=1, device_id=friend, device_id_type=MESH)

    @pl.when(inner)
    def _():
        pl.semaphore_signal(barrier, inc=1, device_id=far, device_id_type=MESH)

    loads = [
        pltpu.make_async_copy(x, y, in_sem.at[i])
        for i, (x, y) in enumerate(
            (
                (q_hbm, q_ref), (lanes_hbm, lanes_ref), (slab_hbm, slab_ref), (qg_hbm, qg_ref), (kg_hbm, kg_ref),
                (perm_hbm, perm_ref), (mask_hbm, mask_ref),
                (k_hbm, k_ref), (tk_hbm, tk_ref), (v_hbm, v_ref), (tv_hbm, tv_ref),
            )
        )
    ]
    for load in loads:
        load.start()
    w_copy = pltpu.make_async_copy(w_ref, w, w_sem)
    w_copy.start()

    def remote(src, dst, ss, rs, to):
        return pltpu.make_async_remote_copy(
            src_ref=src, dst_ref=dst, send_sem=ss, recv_sem=rs, device_id=to, device_id_type=MESH
        )

    def mine_on(i):
        return 2 * i + col

    def mine_off(i):
        return 2 * i + 1 - col

    def kv_move(src, slot, i, to):
        return remote(src, held.at[slot - 1, i], kv_ss, kv_rs.at[i], to)

    def kv_in(i):
        return kv_move(mine.at[mine_on(i)], 1, i, near)

    def kv_off(i):
        return kv_move(mine.at[mine_off(i)], 2, i, ydev)

    def kv_relay(i):
        return kv_move(held.at[1, i], 3, i, near)

    def q_move(src, slot, i, to):
        return remote(src, q_held.at[slot - 1, i], q_ss, q_rs.at[{1: 0, 4: 1, 5: 2}.get(slot, 3), i], to)

    def q_in(i):
        return q_move(q_mine.at[mine_on(i)], 1, i, near)

    def q_off(i):
        return q_move(q_mine.at[mine_off(i)], 4, i, ydev)

    def q_relay(i):
        return q_move(q_held.at[3, i], 5, i, near)

    def q_far(slot, i):
        if slot == 2:
            return q_move(q_mine.at[mine_on(i)], 2, i, far)
        start = {3: 1, 6: 4, 7: 5}[slot]
        return q_move(q_held.at[start - 1, i], slot, i, far)

    def o_move(slot, i):
        index, to = {
            1: (0, near), 4: (0, ydev), 5: (0, near_y),
            2: (1, far), 3: (1, cross), 6: (1, far_y), 7: (1, cross_y),
        }[slot]
        h = mine_on(i)
        return remote(
            o_send.at[slot - 1, i], o_recv.at[index, h], o_ss, o_rs.at[h], to
        )

    def h_move(h):
        return remote(h_send.at[h], h_recv.at[h], h_ss, h_rs.at[h // (heads - 2)], tdev)

    def arrived(ref, sem):
        remote(ref, ref, sem, sem, near).wait_recv()

    def left(ref, sem):
        remote(ref, ref, sem, sem, near).wait_send()

    w_move = remote(w, w_far, wf_ss, wf_rs, tdev)
    tb_in = remote(tb.at[0], tb.at[1], tb_ss, tb_rs, near)
    tb_y = remote(tb.at[0], tb.at[2], tb_ss, tb_rs, ydev)
    tb_relay = remote(tb.at[2], tb.at[3], tb_ss, tb_rs, near)

    for load in loads[1:7]:
        load.wait()
    freq, part, lead = lanes_ref[0:1, :], lanes_ref[1:2, :], lanes_ref[2:3, :]
    blocks = rows // WIDE
    block = lax.broadcasted_iota(jnp.int32, (blocks, HEAD), 0)
    slab = slab_ref[...] * SLAB_H
    place = jnp.where(part < 0.5, (block // SLAB_H).astype(F32), (slab + block % SLAB_H).astype(F32)) * freq
    across = lax.broadcasted_iota(jnp.int32, (WIDE, HEAD), 0).astype(F32) * freq
    trig = (jnp.cos(place), jnp.cos(across)), (jnp.sin(place), jnp.sin(across))

    def partner(x):
        wide = jnp.broadcast_to(x, (8, HEAD))
        near, far = PARTS[0] // 2, PARTS[1] // 2
        after = jnp.where(part < 0.5, pltpu.roll(wide, HEAD - near, 1), pltpu.roll(wide, HEAD - far, 1))
        before = jnp.where(part < 0.5, pltpu.roll(wide, near, 1), pltpu.roll(wide, far, 1))
        return jnp.where(lead > 0.5, after, before)[0:1]

    scale_q = F32(1.0) / jnp.sqrt(F32(HEAD))
    kg = kg_ref[...]
    qg = qg_ref[...] * scale_q
    for which, (by_block, by_column) in enumerate(trig):
        for gain, index in ((qg, 0), (kg, 2)):
            gain = gain if which == 0 else partner(gain)
            for i in range(blocks):
                full = jnp.where(part < 1.5, by_block[i : i + 1], by_column)
                tabs[index + which, i * WIDE : (i + 1) * WIDE, :] = full * gain
    line = lax.broadcasted_iota(jnp.int32, (trows, trows), 0)
    lane = lax.broadcasted_iota(jnp.int32, (trows, trows), 1)
    mark = jnp.where((line == lane) & (mask_ref[...] != 1), F32(NEGATIVE), F32(0.0))
    tb[0] = jnp.broadcast_to(jnp.sum(mark, axis=1, keepdims=True), (trows, HEAD)).astype(BF16)

    def norm_scale(x32):
        return lax.rsqrt(jnp.mean(x32 * x32, axis=-1, keepdims=True) + 0.05)

    def rotated(x, which):
        x32 = x.astype(F32)
        turned = jnp.dot(x, perm_ref[...], preferred_element_type=F32)
        return ((x32 * tabs[which] + turned * tabs[which + 1]) * norm_scale(x32)).astype(BF16)

    def prepare_q(h):
        q_mine[h] = rotated(q_ref[:, pl.ds(pl.multiple_of(h * HEAD, HEAD), HEAD)], 0)

    def prepare_kv(h):
        cols = pl.ds(pl.multiple_of(h * HEAD, HEAD), HEAD)
        mine[h, 0:rows, :] = rotated(k_ref[:, cols], 2)
        tk = tk_ref[:, cols].astype(F32)
        mine[h, rows:keys, :] = (tk * norm_scale(tk) * kg).astype(BF16)
        mine[h, keys : keys + rows, :] = v_ref[:, cols]
        mine[h, keys + rows : 2 * keys, :] = tv_ref[:, cols]

    def side(slot, i, part):
        where = pl.ds(part * keys, keys)
        return held[slot - 1, i, where, :] if slot else mine[mine_on(i), where, :]

    def score(slot, i, where):
        queries = q_held[slot - 1, i] if slot else q_mine[mine_on(i)]
        top = None
        for n in range(GROUP):
            sc = nt(side(n, i, 0), queries)
            mark = tb[n].astype(F32)
            mark = jnp.concatenate([mark] * (rows // HEAD), axis=1)
            sc = jnp.concatenate([sc[0:rows], sc[rows:keys] + mark], axis=0)
            where[n] = sc
            peak = jnp.max(sc, axis=0, keepdims=True)
            top = peak if top is None else jnp.maximum(top, peak)
        return top

    def weigh(i, where, top):
        total = None
        mixed = None
        for n in range(GROUP):
            p = jnp.exp(where[n] - top)
            amount = jnp.sum(p, axis=0, keepdims=True)
            got = tn(side(n, i, 1), p.astype(BF16))
            total = amount if total is None else total + amount
            mixed = got if mixed is None else mixed + got
        return mixed / total, top + jnp.log(total)

    wides = rows // HEAD

    def pack(to, o, lse):
        high = lse.astype(BF16).astype(F32)
        rest = lse - high
        mid = rest.astype(BF16).astype(F32)
        pieces = [x[:, i * HEAD : (i + 1) * HEAD] for x in (high, mid, rest - mid) for i in range(wides)]
        pieces.append(jnp.zeros((STATS - 3 * wides, HEAD), F32))
        to[rows : rows + STATS, :] = jnp.concatenate(pieces, axis=0).astype(BF16)
        for i in range(wides):
            to[i * HEAD : (i + 1) * HEAD, :] = o[:, i * HEAD : (i + 1) * HEAD].astype(BF16)

    def unpack(index, h):
        o = jnp.concatenate([o_recv[index, h, i * HEAD : (i + 1) * HEAD, :] for i in range(wides)], axis=1)
        stats = o_recv[index, h, rows : rows + STATS, :].astype(F32)
        levels = [
            jnp.concatenate([stats[k * wides + i : k * wides + i + 1] for i in range(wides)], axis=1)
            for k in range(3)
        ]
        return o.astype(F32), levels[0] + levels[1] + levels[2]

    def merge(h):
        hub = jnp.logical_and(inner, h % 2 == col)

        @pl.when(hub)
        def _():
            arrived(o_recv.at[1:2, h], o_rs.at[h])

        @pl.when(jnp.logical_not(hub))
        def _():
            arrived(o_recv.at[:, h], o_rs.at[h])

        (o, lse), (o_, lse_) = unpack(0, h), unpack(1, h)
        share = 1.0 / (1.0 + jnp.exp(lse_ - lse))
        o_all[...] = (o * share + o_ * (1.0 - share)).astype(BF16)
        h_send[h] = o_all[:, pl.ds(pl.multiple_of((1 - t) * half, half), half)].T
        h_move(h).start()
        cols = pl.ds(pl.multiple_of(h * HEAD, HEAD), HEAD)
        h_mine[:, cols] = o_all[:, pl.ds(pl.multiple_of(t * half, half), half)].T

    loads[0].wait()
    prepare_q(mine_off(0))
    prepare_q(mine_on(0))

    @pl.when(inner)
    def _():
        pl.semaphore_wait(barrier, len(friends) + 1)
        q_far(2, 0).start()

    @pl.when(outer)
    def _():
        pl.semaphore_wait(barrier, len(friends))
        q_in(0).start()
        tb_in.start()

    q_off(0).start()
    tb_y.start()

    def queries(i, c):
        prepare_q(mine_off(i))
        q_off(i).start()
        prepare_q(mine_on(i))

        @pl.when(inner)
        def _():
            q_far(2, i).start()

        @pl.when(outer)
        def _():
            q_in(i).start()

        return c

    lax.fori_loop(1, pairs, queries, 0)
    for load in loads[7:]:
        load.wait()
    prepare_kv(mine_off(0))
    kv_off(0).start()
    prepare_kv(mine_on(0))

    def keep(i, c):
        prepare_kv(mine_off(i))
        kv_off(i).start()
        prepare_kv(mine_on(i))
        return c

    lax.fori_loop(1, pairs, keep, 0)

    @pl.when(outer)
    def _():
        tb_y.wait_recv()
        tb_relay.start()

        def pass_queries(i, c):
            q_off(i).wait_recv()
            q_relay(i).start()
            return c

        lax.fori_loop(0, pairs, pass_queries, 0)

        def pass_keys(i, c):
            kv_in(i).start()
            kv_off(i).wait_recv()
            kv_relay(i).start()
            return c

        lax.fori_loop(0, pairs, pass_keys, 0)

    w_copy.wait()
    w_move.start()

    @pl.when(outer)
    def _():
        def collect(h, c):
            merge(h)
            return c

        lax.fori_loop(0, heads - 2, collect, 0)

    @pl.when(inner)
    def _():
        def onward(i, c):
            q_in(i).wait_recv()
            q_far(3, i).start()
            q_off(i).wait_recv()
            q_far(6, i).start()
            return c

        def onward_last(i, c):
            q_relay(i).wait_recv()
            q_far(7, i).start()
            return c

        lax.fori_loop(0, pairs, onward, 0)
        lax.fori_loop(0, pairs, onward_last, 0)
        arrived(tb.at[1:GROUP], tb_rs)

        def main(i, c):
            arrived(q_held.at[0:4, i], q_rs.at[3, i])
            arrived(held.at[:, i], kv_rs.at[i])
            order = (7, 3, 6, 2, 5, 1, 4, 0)
            top = score(order[0], i, scores_a)
            for n, slot in enumerate(order):
                here, there = ((scores_a, scores_b), (scores_b, scores_a))[n % 2]
                after = score(order[n + 1], i, there) if n + 1 < HUB_SLOTS else None
                o, lse = weigh(i, here, top)
                top = after
                if slot:
                    pack(o_send.at[slot - 1, i], o, lse)
                    o_move(slot, i).start()
                else:
                    pack(o_recv.at[0, mine_on(i)], o, lse)

            @pl.when(i > 0)
            def _():
                merge(2 * i - 2)
                merge(2 * i - 1)

            return c

        lax.fori_loop(0, pairs, main, 0)

    step = w.shape[1] // chunks
    spans = [slice(i * step, (i + 1) * step) for i in range(chunks)]
    early = (heads - 2) * HEAD

    def dot(x, y):
        return jnp.dot(x, y, preferred_element_type=F32)

    for span in spans:
        acc[0, :, span] = dot(h_mine[:, :early], w[:early, span])
    w_move.wait_recv()
    arrived(h_recv.at[0 : heads - 2], h_rs.at[0])
    theirs = jnp.concatenate([h_recv[h] for h in range(heads - 2)], axis=1)
    for span in spans:
        acc[1, :, span] = dot(theirs, w_far[:early, span])

    merge(heads - 2)
    merge(heads - 1)

    for span in spans:
        acc[0, :, span] += dot(h_mine[:, early:], w[early:, span])
    arrived(h_recv.at[heads - 2 : heads], h_rs.at[1])
    last = jnp.concatenate([h_recv[heads - 2], h_recv[heads - 1]], axis=1)
    for span in spans:
        theirs = acc[1, :, span] + dot(last, w_far[early:, span])
        mine_too = acc[0, :, span]
        out_ref[:, span] = (mine_too.astype(BF16).astype(F32) + theirs.astype(BF16).astype(F32)).astype(BF16)

    @pl.when(inner)
    def _():
        left(q_held.at[0:5], q_ss)
        left(held.at[0:1], kv_ss)
        left(o_send, o_ss)
        left(tb.at[0:1], tb_ss)

    @pl.when(outer)
    def _():
        left(q_held.at[0:3], q_ss)
        left(held, kv_ss)
        left(tb.at[0:3], tb_ss)

    left(h_send, h_ss)
    w_move.wait_send()


def hub_scratch(rows, trows, heads, model, w_shape, inputs):
    keys, half, pairs = rows + trows, rows // 2, heads // 2
    dma = pltpu.SemaphoreType.DMA
    return [
        pltpu.VMEM((heads, 2 * keys, HEAD), BF16),
        pltpu.VMEM((3, pairs, 2 * keys, HEAD), BF16),
        pltpu.VMEM((GROUP, trows, HEAD), BF16),
        pltpu.VMEM((heads, rows, HEAD), BF16),
        pltpu.VMEM((HUB_SLOTS - 1, pairs, rows, HEAD), BF16),
        pltpu.VMEM((HUB_SLOTS - 1, pairs, rows + STATS, HEAD), BF16),
        pltpu.VMEM((2, heads, rows + STATS, HEAD), BF16),
        pltpu.VMEM((GROUP, keys, rows), F32),
        pltpu.VMEM((GROUP, keys, rows), F32),
        pltpu.VMEM((HEAD, rows), BF16),
        pltpu.VMEM(w_shape, BF16),
        pltpu.VMEM(w_shape, BF16),
        pltpu.VMEM((half, heads * HEAD), BF16),
        pltpu.VMEM((heads, half, HEAD), BF16),
        pltpu.VMEM((heads, half, HEAD), BF16),
        pltpu.VMEM((2, half, model), F32),
        pltpu.VMEM((4, rows, HEAD), F32),
        *[pltpu.VMEM(x.shape, x.dtype) for x in inputs],
        dma, dma((pairs,)), dma, dma, dma, dma((4, pairs)), dma, dma((heads,)), dma, dma((2,)), dma, dma, dma,
        dma((11,)),
    ]


def body(
    n,
    visual_q, visual_key_input, visual_v, text_k, text_v, text_mask, slab_order, q_gain, key_norm_gain, w_out,
):
    rows, width = visual_q.shape
    heads = width // HEAD
    model = w_out.shape[1]
    a = n // GROUP
    trows = -(-text_k.shape[0] // 16) * 16
    pad = trows - text_k.shape[0]
    if pad:
        text_k = jnp.pad(text_k, ((0, pad), (0, 0)))
        text_v = jnp.pad(text_v, ((0, pad), (0, 0)))
        text_mask = jnp.pad(text_mask, (0, pad))
    lanes, perm = lane_constants()
    chunks = 6 if model % (6 * HEAD) == 0 else 1
    keys = rows + trows
    half = rows // 2
    peers = a - 1
    vm = pl.BlockSpec(memory_space=pltpu.VMEM)
    anywhere = pl.BlockSpec(memory_space=pl.ANY)
    dma = pltpu.SemaphoreType.DMA
    operands = (
        slab_order, visual_q, visual_key_input, visual_v, text_k, text_v, text_mask[None], q_gain[None],
        key_norm_gain[None], jnp.asarray(lanes), jnp.asarray(perm, BF16), w_out,
    )
    if n == 2 * GROUP and rows % HEAD == 0 and heads % 2 == 0 and heads > 3:
        run = functools.partial(hub_kernel, chunks)
        operands = (slab_order[None],) + operands[1:]
        scratch = hub_scratch(rows, trows, heads, model, w_out.shape, operands[1:6] + operands[:1] + operands[6:11])
        places = [anywhere] * 12
    else:
        run = functools.partial(kernel, n, chunks)
        places = [pl.BlockSpec(memory_space=pltpu.SMEM)] + [anywhere] * 5 + [vm] * 5 + [anywhere]
        scratch = [
                pltpu.VMEM((GROUP, heads, 2 * keys, HEAD), BF16),
                pltpu.VMEM((GROUP, trows, HEAD), BF16),
                pltpu.VMEM((a, heads, rows, HEAD), BF16),
                pltpu.VMEM((peers, heads, HEAD + 16, rows), BF16),
                pltpu.VMEM((peers, heads, HEAD + 16, rows), BF16),
                pltpu.VMEM((heads, HEAD, rows), F32),
                pltpu.VMEM((heads, 8, rows), F32),
                pltpu.VMEM((HEAD, rows), BF16),
                pltpu.VMEM(w_out.shape, BF16),
                pltpu.VMEM(w_out.shape, BF16),
                pltpu.VMEM((half, width), BF16),
                pltpu.VMEM((heads, half, HEAD), BF16),
                pltpu.VMEM((heads, half, HEAD), BF16),
                pltpu.VMEM((2, half, model), F32),
                pltpu.VMEM((4, rows, HEAD), F32),
                *[pltpu.VMEM(x.shape, BF16) for x in (visual_q, visual_key_input, visual_v, text_k, text_v)],
                dma((3, heads)), dma((3, heads)), dma((3,)), dma((3,)),
                dma((peers, heads)), dma((peers, heads)), dma((peers, heads)), dma((peers, heads)),
                dma((heads,)), dma((heads,)), dma, dma, dma, dma((5,)),
        ]
    return pl.pallas_call(
        run,
        out_shape=pltpu.VMEM((half, model), BF16),
        in_specs=places,
        out_specs=vm,
        scratch_shapes=scratch,
        compiler_params=pltpu.CompilerParams(
            collective_id=0, has_side_effects=True, vmem_limit_bytes=60 * 1024 * 1024
        ),
    )(*operands)


def solution(mesh):
    rows = P(("grp", "seq"), "tp")
    placed = (rows,) * 5 + (P(("grp", "seq")),) * 2 + (P(), P(), P("tp", None))
    return jax.shard_map(
        functools.partial(body, mesh.shape["seq"]),
        mesh=mesh, in_specs=placed, out_specs=P(("grp", "seq", "tp"), None), check_vma=False,
    )
```

```python
import functools

import jax
import jax.numpy as jnp
import numpy as np
from jax import lax
from jax.experimental import pallas as pl
from jax.experimental.pallas import tpu as pltpu
from jax.sharding import PartitionSpec as P

SLAB_H = 2
WIDE = 32
HEAD = 128
PARTS = (32, 48, 48)
NEGATIVE = -1e30
MESH = pl.DeviceIdType.MESH
F32 = jnp.float32
BF16 = jnp.bfloat16
LEAD_Y, LEAD_Z, LEAD_Q = 2, 2, 2
GROUP = 4
STATS = 8
HUB_SLOTS = 8


def lane_constants():
    lanes = np.zeros((8, HEAD), np.float32)
    perm = np.zeros((HEAD, HEAD), np.float32)
    offset = 0
    for index, size in enumerate(PARTS):
        half = size // 2
        f = np.float32(10000.0) ** (-np.arange(half, dtype=np.float32) / np.float32(half))
        lanes[0, offset : offset + half] = f
        lanes[0, offset + half : offset + size] = f
        lanes[1, offset : offset + size] = index
        lanes[2, offset : offset + half] = 1.0
        for j in range(half):
            perm[offset + half + j, offset + j] = -1.0
            perm[offset + j, offset + half + j] = 1.0
        offset += size
    return lanes, perm


def nt(a, b):
    return lax.dot_general(a, b, (((1,), (1,)), ((), ())), preferred_element_type=F32)


def tn(a, b):
    return lax.dot_general(a, b, (((0,), (0,)), ((), ())), preferred_element_type=F32)


def kernel(
    n, chunks,
    slab_ref, q_hbm, k_hbm, v_hbm, tk_hbm, tv_hbm, mask_ref, qg_ref, kg_ref, lanes_ref, perm_ref, w_ref,
    out_ref,
    kv, tb, qs, o_send, o_recv, o_own, lse_own, o_all, w, w_far, h_mine, h_send, h_recv, acc, tabs,
    q_ref, k_ref, v_ref, tk_ref, tv_ref,
    kv_ss, kv_rs, tb_ss, tb_rs, q_ss, q_rs, o_ss, o_rs, h_ss, h_rs, wf_ss, wf_rs, w_sem, in_sem,
):
    rows, width = q_ref.shape
    heads = width // HEAD
    trows = tk_ref.shape[0]
    keys = rows + trows
    a = n // GROUP
    g, s, t = lax.axis_index("grp"), lax.axis_index("seq"), lax.axis_index("tp")
    u, low = s // GROUP, s % GROUP
    zdev = (g, s + 2 - 4 * (low // 2), t)
    ydev = (g, s + 1 - 2 * (low % 2), t)
    tdev = (g, s, 1 - t)
    fwd = [(g, lax.rem(u + j, a) * GROUP + low, t) for j in range(a)]
    back = [(g, lax.rem(u + a - j, a) * GROUP + low, t) for j in range(a)]

    barrier = pltpu.get_barrier_semaphore()
    friends = [zdev, ydev, tdev] + fwd[1:]
    for dev in friends:
        pl.semaphore_signal(barrier, inc=1, device_id=dev, device_id_type=MESH)

    loads = [
        pltpu.make_async_copy(x, y, in_sem.at[i])
        for i, (x, y) in enumerate(
            ((k_hbm, k_ref), (tk_hbm, tk_ref), (v_hbm, v_ref), (tv_hbm, tv_ref), (q_hbm, q_ref))
        )
    ]
    for load in loads:
        load.start()
    w_copy = pltpu.make_async_copy(w_ref, w, w_sem)
    w_copy.start()

    def remote(src, dst, ss, rs, dev):
        return pltpu.make_async_remote_copy(
            src_ref=src, dst_ref=dst, send_sem=ss, recv_sem=rs, device_id=dev, device_id_type=MESH
        )

    def kv_z(h):
        return remote(kv.at[0, h], kv.at[1, h], kv_ss.at[0, h], kv_rs.at[0, h], zdev)

    def kv_y(h):
        return remote(kv.at[0, h], kv.at[2, h], kv_ss.at[1, h], kv_rs.at[1, h], ydev)

    def kv_relay(h):
        return remote(kv.at[1, h], kv.at[3, h], kv_ss.at[2, h], kv_rs.at[2, h], ydev)

    def q_move(j, h):
        return remote(qs.at[0, h], qs.at[j, h], q_ss.at[j - 1, h], q_rs.at[j - 1, h], fwd[j])

    def o_move(j, h):
        return remote(
            o_send.at[j - 1, h], o_recv.at[j - 1, h], o_ss.at[j - 1, h], o_rs.at[j - 1, h], back[j]
        )

    tb_z = remote(tb.at[0], tb.at[1], tb_ss.at[0], tb_rs.at[0], zdev)
    tb_y = remote(tb.at[0], tb.at[2], tb_ss.at[1], tb_rs.at[1], ydev)
    tb_relay = remote(tb.at[1], tb.at[3], tb_ss.at[2], tb_rs.at[2], ydev)

    freq, part, lead = lanes_ref[0:1, :], lanes_ref[1:2, :], lanes_ref[2:3, :]
    blocks = rows // WIDE
    block = lax.broadcasted_iota(jnp.int32, (blocks, HEAD), 0)
    slab = slab_ref[0] * SLAB_H
    place = jnp.where(part < 0.5, (block // SLAB_H).astype(F32), (slab + block % SLAB_H).astype(F32)) * freq
    across = lax.broadcasted_iota(jnp.int32, (WIDE, HEAD), 0).astype(F32) * freq
    trig = (jnp.cos(place), jnp.cos(across)), (jnp.sin(place), jnp.sin(across))

    def partner(x):
        wide = jnp.broadcast_to(x, (8, HEAD))
        near, far = PARTS[0] // 2, PARTS[1] // 2
        after = jnp.where(part < 0.5, pltpu.roll(wide, HEAD - near, 1), pltpu.roll(wide, HEAD - far, 1))
        before = jnp.where(part < 0.5, pltpu.roll(wide, near, 1), pltpu.roll(wide, far, 1))
        return jnp.where(lead > 0.5, after, before)[0:1]

    def h_move(h):
        return remote(h_send.at[h], h_recv.at[h], h_ss.at[h], h_rs.at[h], tdev)

    w_move = remote(w, w_far, wf_ss, wf_rs, tdev)

    scale_q = F32(1.0) / jnp.sqrt(F32(HEAD))
    kg = kg_ref[...]
    qg = qg_ref[...] * scale_q
    for which, (by_block, by_column) in enumerate(trig):
        for gain, index in ((qg, 0), (kg, 2)):
            gain = gain if which == 0 else partner(gain)
            for i in range(blocks):
                full = jnp.where(part < 1.5, by_block[i : i + 1], by_column)
                tabs[index + which, i * WIDE : (i + 1) * WIDE, :] = full * gain
    row = lax.broadcasted_iota(jnp.int32, (trows, trows), 0)
    col = lax.broadcasted_iota(jnp.int32, (trows, trows), 1)
    mark = jnp.where((row == col) & (mask_ref[...] != 1), F32(NEGATIVE), F32(0.0))
    tb[0] = jnp.broadcast_to(jnp.sum(mark, axis=1, keepdims=True), (trows, HEAD)).astype(BF16)

    def norm_scale(x32):
        return lax.rsqrt(jnp.mean(x32 * x32, axis=-1, keepdims=True) + 0.05)

    def rotated(x, which):
        x32 = x.astype(F32)
        turned = jnp.dot(x, perm_ref[...], preferred_element_type=F32)
        return ((x32 * tabs[which] + turned * tabs[which + 1]) * norm_scale(x32)).astype(BF16)

    def prepare(h):
        cols = pl.ds(pl.multiple_of(h * HEAD, HEAD), HEAD)
        kv[0, h, 0:rows, :] = rotated(k_ref[:, cols], 2)
        tk = tk_ref[:, cols].astype(F32)
        kv[0, h, rows:keys, :] = (tk * norm_scale(tk) * kg).astype(BF16)
        kv[0, h, keys : keys + rows, :] = v_ref[:, cols]
        kv[0, h, keys + rows : 2 * keys, :] = tv_ref[:, cols]
        qs[0, h] = rotated(q_ref[:, cols], 0)

    def send(h, ready):
        for lead, start in ((LEAD_Y, send_y), (LEAD_Z, send_z), (LEAD_Q, send_q)):
            if ready is None:

                @pl.when(h < lead)
                def _(start=start):
                    start(h)
            else:

                @pl.when(h + lead < heads)
                def _(start=start, lead=lead):
                    start(h + lead)

    def send_y(h):
        kv_y(h).start()

    def send_z(h):
        kv_z(h).start()

    def send_q(h):
        for j in range(1, a):
            q_move(j, h).start()

    for load in loads:
        load.wait()
    prepare(0)
    pl.semaphore_wait(barrier, len(friends))
    tb_z.start()
    tb_y.start()
    send(0, None)

    def first(h, c):
        prepare(h)
        send(h, None)
        return c

    lax.fori_loop(1, heads, first, 0)
    tb_z.wait_recv()
    tb_relay.start()
    kv_z(0).wait_recv()
    kv_relay(0).start()
    w_copy.wait()
    w_move.start()
    half = rows // 2

    def attend(j, h):
        queries = qs[j, h]
        scores = []
        top = None
        for slot in range(GROUP):
            sc = nt(kv[slot, h, 0:keys, :], queries)
            mark = tb[slot].astype(F32)
            mark = jnp.concatenate([mark] * (rows // HEAD), axis=1)
            sc = jnp.concatenate([sc[0:rows], sc[rows:keys] + mark], axis=0)
            peak = jnp.max(sc, axis=0, keepdims=True)
            top = peak if top is None else jnp.maximum(top, peak)
            scores.append(sc)
        total = None
        acc = None
        for slot in range(GROUP):
            p = jnp.exp(scores[slot] - top)
            part = jnp.sum(p, axis=0, keepdims=True)
            mixed = tn(kv[slot, h, keys : 2 * keys, :], p.astype(BF16))
            total = part if total is None else total + part
            acc = mixed if acc is None else acc + mixed
        return acc / total, top + jnp.log(total)

    def main(h, c):
        @pl.when(h + 1 < heads)
        def _():
            kv_z(h + 1).wait_recv()
            kv_relay(h + 1).start()

        send(h, True)

        kv_y(h).wait_recv()

        @pl.when(h == 0)
        def _():
            tb_y.wait_recv()
            tb_relay.wait_recv()

        for j in range(1, a):
            q_move(j, h).wait_recv()
        kv_relay(h).wait_recv()
        for j in range(1, a):
            o, lse = attend(j, h)
            high = lse.astype(BF16)
            rest = lse - high.astype(F32)
            mid = rest.astype(BF16)
            tail = (rest - mid.astype(F32)).astype(BF16)
            o_send[j - 1, h, HEAD : HEAD + 16, :] = jnp.concatenate(
                [high.astype(F32), mid.astype(F32), tail.astype(F32), jnp.zeros((13, rows), F32)], axis=0
            ).astype(BF16)
            o_send[j - 1, h, 0:HEAD, :] = o.astype(BF16)
            o_move(j, h).start()
        o, lse = attend(0, h)
        o_own[h] = o
        lse_own[h] = jnp.broadcast_to(lse, (8, rows))

        @pl.when(h > 0)
        def _():
            merge(h - 1)

        return c

    def merge(h):
        lses = [lse_own[h][0:1]]
        parts = [o_own[h]]
        for j in range(1, a):
            o_move(j, h).wait_recv()
            stats = o_recv[j - 1, h, HEAD : HEAD + 16, :].astype(F32)
            lses.append(stats[0:1] + stats[1:2] + stats[2:3])
            parts.append(o_recv[j - 1, h, 0:HEAD, :].astype(F32))
        top = functools.reduce(jnp.maximum, lses)
        shares = [jnp.exp(x - top) for x in lses]
        total = functools.reduce(jnp.add, shares)
        o = functools.reduce(jnp.add, [x * y for x, y in zip(parts, shares)]) / total
        o_all[...] = o.astype(BF16)
        h_send[h] = o_all[:, pl.ds(pl.multiple_of((1 - t) * half, half), half)].T
        h_move(h).start()
        cols = pl.ds(pl.multiple_of(h * HEAD, HEAD), HEAD)
        h_mine[:, cols] = o_all[:, pl.ds(pl.multiple_of(t * half, half), half)].T

    lax.fori_loop(0, heads, main, 0)

    step = w.shape[1] // chunks
    spans = [slice(i * step, (i + 1) * step) for i in range(chunks)]
    early = (heads - 1) * HEAD

    def dot(x, y):
        return jnp.dot(x, y, preferred_element_type=F32)

    for span in spans:
        acc[0, :, span] = dot(h_mine[:, :early], w[:early, span])
    w_move.wait_recv()
    for h in range(heads - 1):
        h_move(h).wait_recv()
    theirs = jnp.concatenate([h_recv[h] for h in range(heads - 1)], axis=1)
    for span in spans:
        acc[1, :, span] = dot(theirs, w_far[:early, span])
    merge(heads - 1)
    for span in spans:
        acc[0, :, span] += dot(h_mine[:, early:], w[early:, span])
    h_move(heads - 1).wait_recv()
    for span in spans:
        far = acc[1, :, span] + dot(h_recv[heads - 1], w_far[early:, span])
        near = acc[0, :, span]
        out_ref[:, span] = (near.astype(BF16).astype(F32) + far.astype(BF16).astype(F32)).astype(BF16)

    def drain(h, c):
        kv_z(h).wait_send()
        kv_y(h).wait_send()
        kv_relay(h).wait_send()
        h_move(h).wait_send()
        for j in range(1, a):
            q_move(j, h).wait_send()
            o_move(j, h).wait_send()
        return c

    lax.fori_loop(0, heads, drain, 0)
    tb_z.wait_send()
    tb_y.wait_send()
    tb_relay.wait_send()
    w_move.wait_send()


def hub_kernel(
    chunks,
    slab_hbm, q_hbm, k_hbm, v_hbm, tk_hbm, tv_hbm, mask_hbm, qg_hbm, kg_hbm, lanes_hbm, perm_hbm, w_ref,
    out_ref,
    mine, held, tb, q_mine, q_held, o_send, o_recv, scores_a, scores_b, o_all, w, w_far, h_mine, h_send, h_recv,
    acc, tabs, q_ref, k_ref, v_ref, tk_ref, tv_ref, slab_ref, mask_ref, qg_ref, kg_ref, lanes_ref, perm_ref,
    kv_ss, kv_rs, tb_ss, tb_rs, q_ss, q_rs, o_ss, o_rs, h_ss, h_rs, wf_ss, wf_rs, w_sem, in_sem,
):
    rows, width = q_ref.shape
    heads = width // HEAD
    trows = tk_ref.shape[0]
    keys = rows + trows
    half = rows // 2
    pairs = heads // 2
    g, s, t = lax.axis_index("grp"), lax.axis_index("seq"), lax.axis_index("tp")
    u, low = s // GROUP, s % GROUP
    row, col = low // 2, low % 2
    inner = row + u == 1
    outer = row + u != 1
    aside = 1 - 2 * col

    def dev(seq):
        return (g, seq, t)

    near_s, far_s, cross_s = s + 2 - 4 * row, s + 2 - 4 * u, s + GROUP - 2 * GROUP * u
    near, far, cross, ydev = dev(near_s), dev(far_s), dev(cross_s), dev(s + aside)
    near_y, far_y, cross_y = dev(near_s + aside), dev(far_s + aside), dev(cross_s + aside)
    tdev = (g, s, 1 - t)

    barrier = pltpu.get_barrier_semaphore()
    friends = [near, ydev, tdev]
    for friend in friends:
        pl.semaphore_signal(barrier, inc=1, device_id=friend, device_id_type=MESH)

    @pl.when(inner)
    def _():
        pl.semaphore_signal(barrier, inc=1, device_id=far, device_id_type=MESH)

    loads = [
        pltpu.make_async_copy(x, y, in_sem.at[i])
        for i, (x, y) in enumerate(
            (
                (q_hbm, q_ref), (lanes_hbm, lanes_ref), (slab_hbm, slab_ref), (qg_hbm, qg_ref), (kg_hbm, kg_ref),
                (perm_hbm, perm_ref), (mask_hbm, mask_ref),
                (k_hbm, k_ref), (tk_hbm, tk_ref), (v_hbm, v_ref), (tv_hbm, tv_ref),
            )
        )
    ]
    for load in loads:
        load.start()
    w_copy = pltpu.make_async_copy(w_ref, w, w_sem)
    w_copy.start()

    def remote(src, dst, ss, rs, to):
        return pltpu.make_async_remote_copy(
            src_ref=src, dst_ref=dst, send_sem=ss, recv_sem=rs, device_id=to, device_id_type=MESH
        )

    def mine_on(i):
        return 2 * i + col

    def mine_off(i):
        return 2 * i + 1 - col

    def kv_move(src, slot, i, to):
        return remote(src, held.at[slot - 1, i], kv_ss, kv_rs.at[i], to)

    def kv_in(i):
        return kv_move(mine.at[mine_on(i)], 1, i, near)

    def kv_off(i):
        return kv_move(mine.at[mine_off(i)], 2, i, ydev)

    def kv_relay(i):
        return kv_move(held.at[1, i], 3, i, near)

    def q_move(src, slot, i, to):
        return remote(src, q_held.at[slot - 1, i], q_ss, q_rs.at[{1: 0, 4: 1, 5: 2}.get(slot, 3), i], to)

    def q_in(i):
        return q_move(q_mine.at[mine_on(i)], 1, i, near)

    def q_off(i):
        return q_move(q_mine.at[mine_off(i)], 4, i, ydev)

    def q_relay(i):
        return q_move(q_held.at[3, i], 5, i, near)

    def q_far(slot, i):
        if slot == 2:
            return q_move(q_mine.at[mine_on(i)], 2, i, far)
        start = {3: 1, 6: 4, 7: 5}[slot]
        return q_move(q_held.at[start - 1, i], slot, i, far)

    def o_move(slot, i):
        index, to = {
            1: (0, near), 4: (0, ydev), 5: (0, near_y),
            2: (1, far), 3: (1, cross), 6: (1, far_y), 7: (1, cross_y),
        }[slot]
        h = mine_on(i)
        return remote(
            o_send.at[slot - 1, i], o_recv.at[index, h], o_ss, o_rs.at[h], to
        )

    def h_move(h):
        return remote(h_send.at[h], h_recv.at[h], h_ss, h_rs.at[h // (heads - 2)], tdev)

    def arrived(ref, sem):
        remote(ref, ref, sem, sem, near).wait_recv()

    def left(ref, sem):
        remote(ref, ref, sem, sem, near).wait_send()

    w_move = remote(w, w_far, wf_ss, wf_rs, tdev)
    tb_in = remote(tb.at[0], tb.at[1], tb_ss, tb_rs, near)
    tb_y = remote(tb.at[0], tb.at[2], tb_ss, tb_rs, ydev)
    tb_relay = remote(tb.at[2], tb.at[3], tb_ss, tb_rs, near)

    for load in loads[1:7]:
        load.wait()
    freq, part, lead = lanes_ref[0:1, :], lanes_ref[1:2, :], lanes_ref[2:3, :]
    blocks = rows // WIDE
    block = lax.broadcasted_iota(jnp.int32, (blocks, HEAD), 0)
    slab = slab_ref[...] * SLAB_H
    place = jnp.where(part < 0.5, (block // SLAB_H).astype(F32), (slab + block % SLAB_H).astype(F32)) * freq
    across = lax.broadcasted_iota(jnp.int32, (WIDE, HEAD), 0).astype(F32) * freq
    trig = (jnp.cos(place), jnp.cos(across)), (jnp.sin(place), jnp.sin(across))

    def partner(x):
        wide = jnp.broadcast_to(x, (8, HEAD))
        near, far = PARTS[0] // 2, PARTS[1] // 2
        after = jnp.where(part < 0.5, pltpu.roll(wide, HEAD - near, 1), pltpu.roll(wide, HEAD - far, 1))
        before = jnp.where(part < 0.5, pltpu.roll(wide, near, 1), pltpu.roll(wide, far, 1))
        return jnp.where(lead > 0.5, after, before)[0:1]

    scale_q = F32(1.0) / jnp.sqrt(F32(HEAD))
    kg = kg_ref[...]
    qg = qg_ref[...] * scale_q
    for which, (by_block, by_column) in enumerate(trig):
        for gain, index in ((qg, 0), (kg, 2)):
            gain = gain if which == 0 else partner(gain)
            for i in range(blocks):
                full = jnp.where(part < 1.5, by_block[i : i + 1], by_column)
                tabs[index + which, i * WIDE : (i + 1) * WIDE, :] = full * gain
    line = lax.broadcasted_iota(jnp.int32, (trows, trows), 0)
    lane = lax.broadcasted_iota(jnp.int32, (trows, trows), 1)
    mark = jnp.where((line == lane) & (mask_ref[...] != 1), F32(NEGATIVE), F32(0.0))
    tb[0] = jnp.broadcast_to(jnp.sum(mark, axis=1, keepdims=True), (trows, HEAD)).astype(BF16)

    def norm_scale(x32):
        return lax.rsqrt(jnp.mean(x32 * x32, axis=-1, keepdims=True) + 0.05)

    def rotated(x, which):
        x32 = x.astype(F32)
        turned = jnp.dot(x, perm_ref[...], preferred_element_type=F32)
        return ((x32 * tabs[which] + turned * tabs[which + 1]) * norm_scale(x32)).astype(BF16)

    def prepare_q(h):
        q_mine[h] = rotated(q_ref[:, pl.ds(pl.multiple_of(h * HEAD, HEAD), HEAD)], 0)

    def prepare_kv(h):
        cols = pl.ds(pl.multiple_of(h * HEAD, HEAD), HEAD)
        mine[h, 0:rows, :] = rotated(k_ref[:, cols], 2)
        tk = tk_ref[:, cols].astype(F32)
        mine[h, rows:keys, :] = (tk * norm_scale(tk) * kg).astype(BF16)
        mine[h, keys : keys + rows, :] = v_ref[:, cols]
        mine[h, keys + rows : 2 * keys, :] = tv_ref[:, cols]

    def side(slot, i, part):
        where = pl.ds(part * keys, keys)
        return held[slot - 1, i, where, :] if slot else mine[mine_on(i), where, :]

    def score(slot, i, where):
        queries = q_held[slot - 1, i] if slot else q_mine[mine_on(i)]
        top = None
        for n in range(GROUP):
            sc = nt(side(n, i, 0), queries)
            mark = tb[n].astype(F32)
            mark = jnp.concatenate([mark] * (rows // HEAD), axis=1)
            sc = jnp.concatenate([sc[0:rows], sc[rows:keys] + mark], axis=0)
            where[n] = sc
            peak = jnp.max(sc, axis=0, keepdims=True)
            top = peak if top is None else jnp.maximum(top, peak)
        return top

    def weigh(i, where, top):
        total = None
        mixed = None
        for n in range(GROUP):
            p = jnp.exp(where[n] - top)
            amount = jnp.sum(p, axis=0, keepdims=True)
            got = tn(side(n, i, 1), p.astype(BF16))
            total = amount if total is None else total + amount
            mixed = got if mixed is None else mixed + got
        return mixed / total, top + jnp.log(total)

    wides = rows // HEAD

    def pack(to, o, lse):
        high = lse.astype(BF16).astype(F32)
        rest = lse - high
        mid = rest.astype(BF16).astype(F32)
        pieces = [x[:, i * HEAD : (i + 1) * HEAD] for x in (high, mid, rest - mid) for i in range(wides)]
        pieces.append(jnp.zeros((STATS - 3 * wides, HEAD), F32))
        to[rows : rows + STATS, :] = jnp.concatenate(pieces, axis=0).astype(BF16)
        for i in range(wides):
            to[i * HEAD : (i + 1) * HEAD, :] = o[:, i * HEAD : (i + 1) * HEAD].astype(BF16)

    def unpack(index, h):
        o = jnp.concatenate([o_recv[index, h, i * HEAD : (i + 1) * HEAD, :] for i in range(wides)], axis=1)
        stats = o_recv[index, h, rows : rows + STATS, :].astype(F32)
        levels = [
            jnp.concatenate([stats[k * wides + i : k * wides + i + 1] for i in range(wides)], axis=1)
            for k in range(3)
        ]
        return o.astype(F32), levels[0] + levels[1] + levels[2]

    def merge(h):
        hub = jnp.logical_and(inner, h % 2 == col)

        @pl.when(hub)
        def _():
            arrived(o_recv.at[1:2, h], o_rs.at[h])

        @pl.when(jnp.logical_not(hub))
        def _():
            arrived(o_recv.at[:, h], o_rs.at[h])

        (o, lse), (o_, lse_) = unpack(0, h), unpack(1, h)
        share = 1.0 / (1.0 + jnp.exp(lse_ - lse))
        o_all[...] = (o * share + o_ * (1.0 - share)).astype(BF16)
        h_send[h] = o_all[:, pl.ds(pl.multiple_of((1 - t) * half, half), half)].T
        h_move(h).start()
        cols = pl.ds(pl.multiple_of(h * HEAD, HEAD), HEAD)
        h_mine[:, cols] = o_all[:, pl.ds(pl.multiple_of(t * half, half), half)].T

    loads[0].wait()
    prepare_q(mine_off(0))
    prepare_q(mine_on(0))

    @pl.when(inner)
    def _():
        pl.semaphore_wait(barrier, len(friends) + 1)
        q_far(2, 0).start()

    @pl.when(outer)
    def _():
        pl.semaphore_wait(barrier, len(friends))
        q_in(0).start()
        tb_in.start()

    q_off(0).start()
    tb_y.start()

    def queries(i, c):
        prepare_q(mine_off(i))
        q_off(i).start()
        prepare_q(mine_on(i))

        @pl.when(inner)
        def _():
            q_far(2, i).start()

        @pl.when(outer)
        def _():
            q_in(i).start()

        return c

    lax.fori_loop(1, pairs, queries, 0)
    for load in loads[7:]:
        load.wait()
    prepare_kv(mine_off(0))
    kv_off(0).start()
    prepare_kv(mine_on(0))

    def keep(i, c):
        prepare_kv(mine_off(i))
        kv_off(i).start()
        prepare_kv(mine_on(i))
        return c

    lax.fori_loop(1, pairs, keep, 0)

    @pl.when(outer)
    def _():
        tb_y.wait_recv()
        tb_relay.start()

        def pass_queries(i, c):
            q_off(i).wait_recv()
            q_relay(i).start()
            return c

        lax.fori_loop(0, pairs, pass_queries, 0)

        def pass_keys(i, c):
            kv_in(i).start()
            kv_off(i).wait_recv()
            kv_relay(i).start()
            return c

        lax.fori_loop(0, pairs, pass_keys, 0)

    w_copy.wait()
    w_move.start()

    @pl.when(outer)
    def _():
        def collect(h, c):
            merge(h)
            return c

        lax.fori_loop(0, heads - 2, collect, 0)

    @pl.when(inner)
    def _():
        def onward(i, c):
            q_in(i).wait_recv()
            q_far(3, i).start()
            q_off(i).wait_recv()
            q_far(6, i).start()
            return c

        def onward_last(i, c):
            q_relay(i).wait_recv()
            q_far(7, i).start()
            return c

        lax.fori_loop(0, pairs, onward, 0)
        lax.fori_loop(0, pairs, onward_last, 0)
        arrived(tb.at[1:GROUP], tb_rs)

        def main(i, c):
            arrived(q_held.at[0:4, i], q_rs.at[3, i])
            arrived(held.at[:, i], kv_rs.at[i])
            order = (7, 5, 3, 1, 6, 2, 4, 0)
            top = score(order[0], i, scores_a)
            for n, slot in enumerate(order):
                here, there = ((scores_a, scores_b), (scores_b, scores_a))[n % 2]
                after = score(order[n + 1], i, there) if n + 1 < HUB_SLOTS else None
                o, lse = weigh(i, here, top)
                top = after
                if slot:
                    pack(o_send.at[slot - 1, i], o, lse)
                    o_move(slot, i).start()
                else:
                    pack(o_recv.at[0, mine_on(i)], o, lse)

            @pl.when(i > 0)
            def _():
                merge(2 * i - 2)
                merge(2 * i - 1)

            return c

        lax.fori_loop(0, pairs, main, 0)

    step = w.shape[1] // chunks
    spans = [slice(i * step, (i + 1) * step) for i in range(chunks)]
    early = (heads - 2) * HEAD

    def dot(x, y):
        return jnp.dot(x, y, preferred_element_type=F32)

    for span in spans:
        acc[0, :, span] = dot(h_mine[:, :early], w[:early, span])
    w_move.wait_recv()
    arrived(h_recv.at[0 : heads - 2], h_rs.at[0])
    theirs = jnp.concatenate([h_recv[h] for h in range(heads - 2)], axis=1)
    for span in spans:
        acc[1, :, span] = dot(theirs, w_far[:early, span])

    merge(heads - 2)
    merge(heads - 1)

    for span in spans:
        acc[0, :, span] += dot(h_mine[:, early:], w[early:, span])
    arrived(h_recv.at[heads - 2 : heads], h_rs.at[1])
    last = jnp.concatenate([h_recv[heads - 2], h_recv[heads - 1]], axis=1)
    for span in spans:
        theirs = acc[1, :, span] + dot(last, w_far[early:, span])
        mine_too = acc[0, :, span]
        out_ref[:, span] = (mine_too.astype(BF16).astype(F32) + theirs.astype(BF16).astype(F32)).astype(BF16)

    @pl.when(inner)
    def _():
        left(q_held.at[0:5], q_ss)
        left(held.at[0:1], kv_ss)
        left(o_send, o_ss)
        left(tb.at[0:1], tb_ss)

    @pl.when(outer)
    def _():
        left(q_held.at[0:3], q_ss)
        left(held, kv_ss)
        left(tb.at[0:3], tb_ss)

    left(h_send, h_ss)
    w_move.wait_send()


def hub_scratch(rows, trows, heads, model, w_shape, inputs):
    keys, half, pairs = rows + trows, rows // 2, heads // 2
    dma = pltpu.SemaphoreType.DMA
    return [
        pltpu.VMEM((heads, 2 * keys, HEAD), BF16),
        pltpu.VMEM((3, pairs, 2 * keys, HEAD), BF16),
        pltpu.VMEM((GROUP, trows, HEAD), BF16),
        pltpu.VMEM((heads, rows, HEAD), BF16),
        pltpu.VMEM((HUB_SLOTS - 1, pairs, rows, HEAD), BF16),
        pltpu.VMEM((HUB_SLOTS - 1, pairs, rows + STATS, HEAD), BF16),
        pltpu.VMEM((2, heads, rows + STATS, HEAD), BF16),
        pltpu.VMEM((GROUP, keys, rows), F32),
        pltpu.VMEM((GROUP, keys, rows), F32),
        pltpu.VMEM((HEAD, rows), BF16),
        pltpu.VMEM(w_shape, BF16),
        pltpu.VMEM(w_shape, BF16),
        pltpu.VMEM((half, heads * HEAD), BF16),
        pltpu.VMEM((heads, half, HEAD), BF16),
        pltpu.VMEM((heads, half, HEAD), BF16),
        pltpu.VMEM((2, half, model), F32),
        pltpu.VMEM((4, rows, HEAD), F32),
        *[pltpu.VMEM(x.shape, x.dtype) for x in inputs],
        dma, dma((pairs,)), dma, dma, dma, dma((4, pairs)), dma, dma((heads,)), dma, dma((2,)), dma, dma, dma,
        dma((11,)),
    ]


def body(
    n,
    visual_q, visual_key_input, visual_v, text_k, text_v, text_mask, slab_order, q_gain, key_norm_gain, w_out,
):
    rows, width = visual_q.shape
    heads = width // HEAD
    model = w_out.shape[1]
    a = n // GROUP
    trows = -(-text_k.shape[0] // 16) * 16
    pad = trows - text_k.shape[0]
    if pad:
        text_k = jnp.pad(text_k, ((0, pad), (0, 0)))
        text_v = jnp.pad(text_v, ((0, pad), (0, 0)))
        text_mask = jnp.pad(text_mask, (0, pad))
    lanes, perm = lane_constants()
    chunks = 6 if model % (6 * HEAD) == 0 else 1
    keys = rows + trows
    half = rows // 2
    peers = a - 1
    vm = pl.BlockSpec(memory_space=pltpu.VMEM)
    anywhere = pl.BlockSpec(memory_space=pl.ANY)
    dma = pltpu.SemaphoreType.DMA
    operands = (
        slab_order, visual_q, visual_key_input, visual_v, text_k, text_v, text_mask[None], q_gain[None],
        key_norm_gain[None], jnp.asarray(lanes), jnp.asarray(perm, BF16), w_out,
    )
    if n == 2 * GROUP and rows % HEAD == 0 and heads % 2 == 0 and heads > 3:
        run = functools.partial(hub_kernel, chunks)
        operands = (slab_order[None],) + operands[1:]
        scratch = hub_scratch(rows, trows, heads, model, w_out.shape, operands[1:6] + operands[:1] + operands[6:11])
        places = [anywhere] * 12
    else:
        run = functools.partial(kernel, n, chunks)
        places = [pl.BlockSpec(memory_space=pltpu.SMEM)] + [anywhere] * 5 + [vm] * 5 + [anywhere]
        scratch = [
                pltpu.VMEM((GROUP, heads, 2 * keys, HEAD), BF16),
                pltpu.VMEM((GROUP, trows, HEAD), BF16),
                pltpu.VMEM((a, heads, rows, HEAD), BF16),
                pltpu.VMEM((peers, heads, HEAD + 16, rows), BF16),
                pltpu.VMEM((peers, heads, HEAD + 16, rows), BF16),
                pltpu.VMEM((heads, HEAD, rows), F32),
                pltpu.VMEM((heads, 8, rows), F32),
                pltpu.VMEM((HEAD, rows), BF16),
                pltpu.VMEM(w_out.shape, BF16),
                pltpu.VMEM(w_out.shape, BF16),
                pltpu.VMEM((half, width), BF16),
                pltpu.VMEM((heads, half, HEAD), BF16),
                pltpu.VMEM((heads, half, HEAD), BF16),
                pltpu.VMEM((2, half, model), F32),
                pltpu.VMEM((4, rows, HEAD), F32),
                *[pltpu.VMEM(x.shape, BF16) for x in (visual_q, visual_key_input, visual_v, text_k, text_v)],
                dma((3, heads)), dma((3, heads)), dma((3,)), dma((3,)),
                dma((peers, heads)), dma((peers, heads)), dma((peers, heads)), dma((peers, heads)),
                dma((heads,)), dma((heads,)), dma, dma, dma, dma((5,)),
        ]
    return pl.pallas_call(
        run,
        out_shape=pltpu.VMEM((half, model), BF16),
        in_specs=places,
        out_specs=vm,
        scratch_shapes=scratch,
        compiler_params=pltpu.CompilerParams(
            collective_id=0, has_side_effects=True, vmem_limit_bytes=60 * 1024 * 1024
        ),
    )(*operands)


def solution(mesh):
    rows = P(("grp", "seq"), "tp")
    placed = (rows,) * 5 + (P(("grp", "seq")),) * 2 + (P(), P(), P("tp", None))
    return jax.shard_map(
        functools.partial(body, mesh.shape["seq"]),
        mesh=mesh, in_specs=placed, out_specs=P(("grp", "seq", "tp"), None), check_vma=False,
    )
```

```python
import functools

import jax
import jax.numpy as jnp
import numpy as np
from jax import lax
from jax.experimental import pallas as pl
from jax.experimental.pallas import tpu as pltpu
from jax.sharding import PartitionSpec as P

SLAB_H = 2
WIDE = 32
HEAD = 128
PARTS = (32, 48, 48)
NEGATIVE = -1e30
MESH = pl.DeviceIdType.MESH
F32 = jnp.float32
BF16 = jnp.bfloat16
LEAD_Y, LEAD_Z, LEAD_Q = 2, 2, 2
GROUP = 4
STATS = 8
HUB_SLOTS = 8


def lane_constants():
    lanes = np.zeros((8, HEAD), np.float32)
    perm = np.zeros((HEAD, HEAD), np.float32)
    offset = 0
    for index, size in enumerate(PARTS):
        half = size // 2
        f = np.float32(10000.0) ** (-np.arange(half, dtype=np.float32) / np.float32(half))
        lanes[0, offset : offset + half] = f
        lanes[0, offset + half : offset + size] = f
        lanes[1, offset : offset + size] = index
        lanes[2, offset : offset + half] = 1.0
        for j in range(half):
            perm[offset + half + j, offset + j] = -1.0
            perm[offset + j, offset + half + j] = 1.0
        offset += size
    return lanes, perm


def nt(a, b):
    return lax.dot_general(a, b, (((1,), (1,)), ((), ())), preferred_element_type=F32)


def tn(a, b):
    return lax.dot_general(a, b, (((0,), (0,)), ((), ())), preferred_element_type=F32)


def kernel(
    n, chunks,
    slab_ref, q_hbm, k_hbm, v_hbm, tk_hbm, tv_hbm, mask_ref, qg_ref, kg_ref, lanes_ref, perm_ref, w_ref,
    out_ref,
    kv, tb, qs, o_send, o_recv, o_own, lse_own, o_all, w, w_far, h_mine, h_send, h_recv, acc, tabs,
    q_ref, k_ref, v_ref, tk_ref, tv_ref,
    kv_ss, kv_rs, tb_ss, tb_rs, q_ss, q_rs, o_ss, o_rs, h_ss, h_rs, wf_ss, wf_rs, w_sem, in_sem,
):
    rows, width = q_ref.shape
    heads = width // HEAD
    trows = tk_ref.shape[0]
    keys = rows + trows
    a = n // GROUP
    g, s, t = lax.axis_index("grp"), lax.axis_index("seq"), lax.axis_index("tp")
    u, low = s // GROUP, s % GROUP
    zdev = (g, s + 2 - 4 * (low // 2), t)
    ydev = (g, s + 1 - 2 * (low % 2), t)
    tdev = (g, s, 1 - t)
    fwd = [(g, lax.rem(u + j, a) * GROUP + low, t) for j in range(a)]
    back = [(g, lax.rem(u + a - j, a) * GROUP + low, t) for j in range(a)]

    barrier = pltpu.get_barrier_semaphore()
    friends = [zdev, ydev, tdev] + fwd[1:]
    for dev in friends:
        pl.semaphore_signal(barrier, inc=1, device_id=dev, device_id_type=MESH)

    loads = [
        pltpu.make_async_copy(x, y, in_sem.at[i])
        for i, (x, y) in enumerate(
            ((k_hbm, k_ref), (tk_hbm, tk_ref), (v_hbm, v_ref), (tv_hbm, tv_ref), (q_hbm, q_ref))
        )
    ]
    for load in loads:
        load.start()
    w_copy = pltpu.make_async_copy(w_ref, w, w_sem)
    w_copy.start()

    def remote(src, dst, ss, rs, dev):
        return pltpu.make_async_remote_copy(
            src_ref=src, dst_ref=dst, send_sem=ss, recv_sem=rs, device_id=dev, device_id_type=MESH
        )

    def kv_z(h):
        return remote(kv.at[0, h], kv.at[1, h], kv_ss.at[0, h], kv_rs.at[0, h], zdev)

    def kv_y(h):
        return remote(kv.at[0, h], kv.at[2, h], kv_ss.at[1, h], kv_rs.at[1, h], ydev)

    def kv_relay(h):
        return remote(kv.at[1, h], kv.at[3, h], kv_ss.at[2, h], kv_rs.at[2, h], ydev)

    def q_move(j, h):
        return remote(qs.at[0, h], qs.at[j, h], q_ss.at[j - 1, h], q_rs.at[j - 1, h], fwd[j])

    def o_move(j, h):
        return remote(
            o_send.at[j - 1, h], o_recv.at[j - 1, h], o_ss.at[j - 1, h], o_rs.at[j - 1, h], back[j]
        )

    tb_z = remote(tb.at[0], tb.at[1], tb_ss.at[0], tb_rs.at[0], zdev)
    tb_y = remote(tb.at[0], tb.at[2], tb_ss.at[1], tb_rs.at[1], ydev)
    tb_relay = remote(tb.at[1], tb.at[3], tb_ss.at[2], tb_rs.at[2], ydev)

    freq, part, lead = lanes_ref[0:1, :], lanes_ref[1:2, :], lanes_ref[2:3, :]
    blocks = rows // WIDE
    block = lax.broadcasted_iota(jnp.int32, (blocks, HEAD), 0)
    slab = slab_ref[0] * SLAB_H
    place = jnp.where(part < 0.5, (block // SLAB_H).astype(F32), (slab + block % SLAB_H).astype(F32)) * freq
    across = lax.broadcasted_iota(jnp.int32, (WIDE, HEAD), 0).astype(F32) * freq
    trig = (jnp.cos(place), jnp.cos(across)), (jnp.sin(place), jnp.sin(across))

    def partner(x):
        wide = jnp.broadcast_to(x, (8, HEAD))
        near, far = PARTS[0] // 2, PARTS[1] // 2
        after = jnp.where(part < 0.5, pltpu.roll(wide, HEAD - near, 1), pltpu.roll(wide, HEAD - far, 1))
        before = jnp.where(part < 0.5, pltpu.roll(wide, near, 1), pltpu.roll(wide, far, 1))
        return jnp.where(lead > 0.5, after, before)[0:1]

    def h_move(h):
        return remote(h_send.at[h], h_recv.at[h], h_ss.at[h], h_rs.at[h], tdev)

    w_move = remote(w, w_far, wf_ss, wf_rs, tdev)

    scale_q = F32(1.0) / jnp.sqrt(F32(HEAD))
    kg = kg_ref[...]
    qg = qg_ref[...] * scale_q
    for which, (by_block, by_column) in enumerate(trig):
        for gain, index in ((qg, 0), (kg, 2)):
            gain = gain if which == 0 else partner(gain)
            for i in range(blocks):
                full = jnp.where(part < 1.5, by_block[i : i + 1], by_column)
                tabs[index + which, i * WIDE : (i + 1) * WIDE, :] = full * gain
    row = lax.broadcasted_iota(jnp.int32, (trows, trows), 0)
    col = lax.broadcasted_iota(jnp.int32, (trows, trows), 1)
    mark = jnp.where((row == col) & (mask_ref[...] != 1), F32(NEGATIVE), F32(0.0))
    tb[0] = jnp.broadcast_to(jnp.sum(mark, axis=1, keepdims=True), (trows, HEAD)).astype(BF16)

    def norm_scale(x32):
        return lax.rsqrt(jnp.mean(x32 * x32, axis=-1, keepdims=True) + 0.05)

    def rotated(x, which):
        x32 = x.astype(F32)
        turned = jnp.dot(x, perm_ref[...], preferred_element_type=F32)
        return ((x32 * tabs[which] + turned * tabs[which + 1]) * norm_scale(x32)).astype(BF16)

    def prepare(h):
        cols = pl.ds(pl.multiple_of(h * HEAD, HEAD), HEAD)
        kv[0, h, 0:rows, :] = rotated(k_ref[:, cols], 2)
        tk = tk_ref[:, cols].astype(F32)
        kv[0, h, rows:keys, :] = (tk * norm_scale(tk) * kg).astype(BF16)
        kv[0, h, keys : keys + rows, :] = v_ref[:, cols]
        kv[0, h, keys + rows : 2 * keys, :] = tv_ref[:, cols]
        qs[0, h] = rotated(q_ref[:, cols], 0)

    def send(h, ready):
        for lead, start in ((LEAD_Y, send_y), (LEAD_Z, send_z), (LEAD_Q, send_q)):
            if ready is None:

                @pl.when(h < lead)
                def _(start=start):
                    start(h)
            else:

                @pl.when(h + lead < heads)
                def _(start=start, lead=lead):
                    start(h + lead)

    def send_y(h):
        kv_y(h).start()

    def send_z(h):
        kv_z(h).start()

    def send_q(h):
        for j in range(1, a):
            q_move(j, h).start()

    for load in loads:
        load.wait()
    prepare(0)
    pl.semaphore_wait(barrier, len(friends))
    tb_z.start()
    tb_y.start()
    send(0, None)

    def first(h, c):
        prepare(h)
        send(h, None)
        return c

    lax.fori_loop(1, heads, first, 0)
    tb_z.wait_recv()
    tb_relay.start()
    kv_z(0).wait_recv()
    kv_relay(0).start()
    w_copy.wait()
    w_move.start()
    half = rows // 2

    def attend(j, h):
        queries = qs[j, h]
        scores = []
        top = None
        for slot in range(GROUP):
            sc = nt(kv[slot, h, 0:keys, :], queries)
            mark = tb[slot].astype(F32)
            mark = jnp.concatenate([mark] * (rows // HEAD), axis=1)
            sc = jnp.concatenate([sc[0:rows], sc[rows:keys] + mark], axis=0)
            peak = jnp.max(sc, axis=0, keepdims=True)
            top = peak if top is None else jnp.maximum(top, peak)
            scores.append(sc)
        total = None
        acc = None
        for slot in range(GROUP):
            p = jnp.exp(scores[slot] - top)
            part = jnp.sum(p, axis=0, keepdims=True)
            mixed = tn(kv[slot, h, keys : 2 * keys, :], p.astype(BF16))
            total = part if total is None else total + part
            acc = mixed if acc is None else acc + mixed
        return acc / total, top + jnp.log(total)

    def main(h, c):
        @pl.when(h + 1 < heads)
        def _():
            kv_z(h + 1).wait_recv()
            kv_relay(h + 1).start()

        send(h, True)

        kv_y(h).wait_recv()

        @pl.when(h == 0)
        def _():
            tb_y.wait_recv()
            tb_relay.wait_recv()

        for j in range(1, a):
            q_move(j, h).wait_recv()
        kv_relay(h).wait_recv()
        for j in range(1, a):
            o, lse = attend(j, h)
            high = lse.astype(BF16)
            rest = lse - high.astype(F32)
            mid = rest.astype(BF16)
            tail = (rest - mid.astype(F32)).astype(BF16)
            o_send[j - 1, h, HEAD : HEAD + 16, :] = jnp.concatenate(
                [high.astype(F32), mid.astype(F32), tail.astype(F32), jnp.zeros((13, rows), F32)], axis=0
            ).astype(BF16)
            o_send[j - 1, h, 0:HEAD, :] = o.astype(BF16)
            o_move(j, h).start()
        o, lse = attend(0, h)
        o_own[h] = o
        lse_own[h] = jnp.broadcast_to(lse, (8, rows))

        @pl.when(h > 0)
        def _():
            merge(h - 1)

        return c

    def merge(h):
        lses = [lse_own[h][0:1]]
        parts = [o_own[h]]
        for j in range(1, a):
            o_move(j, h).wait_recv()
            stats = o_recv[j - 1, h, HEAD : HEAD + 16, :].astype(F32)
            lses.append(stats[0:1] + stats[1:2] + stats[2:3])
            parts.append(o_recv[j - 1, h, 0:HEAD, :].astype(F32))
        top = functools.reduce(jnp.maximum, lses)
        shares = [jnp.exp(x - top) for x in lses]
        total = functools.reduce(jnp.add, shares)
        o = functools.reduce(jnp.add, [x * y for x, y in zip(parts, shares)]) / total
        o_all[...] = o.astype(BF16)
        h_send[h] = o_all[:, pl.ds(pl.multiple_of((1 - t) * half, half), half)].T
        h_move(h).start()
        cols = pl.ds(pl.multiple_of(h * HEAD, HEAD), HEAD)
        h_mine[:, cols] = o_all[:, pl.ds(pl.multiple_of(t * half, half), half)].T

    lax.fori_loop(0, heads, main, 0)

    step = w.shape[1] // chunks
    spans = [slice(i * step, (i + 1) * step) for i in range(chunks)]
    early = (heads - 1) * HEAD

    def dot(x, y):
        return jnp.dot(x, y, preferred_element_type=F32)

    for span in spans:
        acc[0, :, span] = dot(h_mine[:, :early], w[:early, span])
    w_move.wait_recv()
    for h in range(heads - 1):
        h_move(h).wait_recv()
    theirs = jnp.concatenate([h_recv[h] for h in range(heads - 1)], axis=1)
    for span in spans:
        acc[1, :, span] = dot(theirs, w_far[:early, span])
    merge(heads - 1)
    for span in spans:
        acc[0, :, span] += dot(h_mine[:, early:], w[early:, span])
    h_move(heads - 1).wait_recv()
    for span in spans:
        far = acc[1, :, span] + dot(h_recv[heads - 1], w_far[early:, span])
        near = acc[0, :, span]
        out_ref[:, span] = (near.astype(BF16).astype(F32) + far.astype(BF16).astype(F32)).astype(BF16)

    def drain(h, c):
        kv_z(h).wait_send()
        kv_y(h).wait_send()
        kv_relay(h).wait_send()
        h_move(h).wait_send()
        for j in range(1, a):
            q_move(j, h).wait_send()
            o_move(j, h).wait_send()
        return c

    lax.fori_loop(0, heads, drain, 0)
    tb_z.wait_send()
    tb_y.wait_send()
    tb_relay.wait_send()
    w_move.wait_send()


def hub_kernel(
    chunks,
    slab_hbm, q_hbm, k_hbm, v_hbm, tk_hbm, tv_hbm, mask_hbm, qg_hbm, kg_hbm, lanes_hbm, perm_hbm, w_ref,
    out_ref,
    mine, held, tb, q_mine, q_held, o_send, o_recv, scores_a, scores_b, o_all, w, w_far, h_mine, h_send, h_recv,
    acc, tabs, q_ref, k_ref, v_ref, tk_ref, tv_ref, slab_ref, mask_ref, qg_ref, kg_ref, lanes_ref, perm_ref,
    kv_ss, kv_rs, tb_ss, tb_rs, q_ss, q_rs, o_ss, o_rs, h_ss, h_rs, wf_ss, wf_rs, w_sem, in_sem,
):
    rows, width = q_ref.shape
    heads = width // HEAD
    trows = tk_ref.shape[0]
    keys = rows + trows
    half = rows // 2
    pairs = heads // 2
    g, s, t = lax.axis_index("grp"), lax.axis_index("seq"), lax.axis_index("tp")
    u, low = s // GROUP, s % GROUP
    row, col = low // 2, low % 2
    inner = row + u == 1
    outer = row + u != 1
    aside = 1 - 2 * col

    def dev(seq):
        return (g, seq, t)

    near_s, far_s, cross_s = s + 2 - 4 * row, s + 2 - 4 * u, s + GROUP - 2 * GROUP * u
    near, far, cross, ydev = dev(near_s), dev(far_s), dev(cross_s), dev(s + aside)
    near_y, far_y, cross_y = dev(near_s + aside), dev(far_s + aside), dev(cross_s + aside)
    tdev = (g, s, 1 - t)

    barrier = pltpu.get_barrier_semaphore()
    friends = [near, ydev, tdev]
    for friend in friends:
        pl.semaphore_signal(barrier, inc=1, device_id=friend, device_id_type=MESH)

    @pl.when(inner)
    def _():
        pl.semaphore_signal(barrier, inc=1, device_id=far, device_id_type=MESH)

    loads = [
        pltpu.make_async_copy(x, y, in_sem.at[i])
        for i, (x, y) in enumerate(
            (
                (q_hbm, q_ref), (lanes_hbm, lanes_ref), (slab_hbm, slab_ref), (qg_hbm, qg_ref), (kg_hbm, kg_ref),
                (perm_hbm, perm_ref), (mask_hbm, mask_ref),
                (k_hbm, k_ref), (tk_hbm, tk_ref), (v_hbm, v_ref), (tv_hbm, tv_ref),
            )
        )
    ]
    for load in loads:
        load.start()
    w_copy = pltpu.make_async_copy(w_ref, w, w_sem)
    w_copy.start()

    def remote(src, dst, ss, rs, to):
        return pltpu.make_async_remote_copy(
            src_ref=src, dst_ref=dst, send_sem=ss, recv_sem=rs, device_id=to, device_id_type=MESH
        )

    def mine_on(i):
        return 2 * i + col

    def mine_off(i):
        return 2 * i + 1 - col

    def kv_move(src, slot, i, to):
        return remote(src, held.at[slot - 1, i], kv_ss, kv_rs.at[i], to)

    def kv_in(i):
        return kv_move(mine.at[mine_on(i)], 1, i, near)

    def kv_off(i):
        return kv_move(mine.at[mine_off(i)], 2, i, ydev)

    def kv_relay(i):
        return kv_move(held.at[1, i], 3, i, near)

    def q_move(src, slot, i, to):
        return remote(src, q_held.at[slot - 1, i], q_ss, q_rs.at[{1: 0, 4: 1, 5: 2}.get(slot, 3), i], to)

    def q_in(i):
        return q_move(q_mine.at[mine_on(i)], 1, i, near)

    def q_off(i):
        return q_move(q_mine.at[mine_off(i)], 4, i, ydev)

    def q_relay(i):
        return q_move(q_held.at[3, i], 5, i, near)

    def q_far(slot, i):
        if slot == 2:
            return q_move(q_mine.at[mine_on(i)], 2, i, far)
        start = {3: 1, 6: 4, 7: 5}[slot]
        return q_move(q_held.at[start - 1, i], slot, i, far)

    def o_move(slot, i):
        index, to = {
            1: (0, near), 4: (0, ydev), 5: (0, near_y),
            2: (1, far), 3: (1, cross), 6: (1, far_y), 7: (1, cross_y),
        }[slot]
        h = mine_on(i)
        return remote(
            o_send.at[slot - 1, i], o_recv.at[index, h], o_ss, o_rs.at[h], to
        )

    def h_move(h):
        return remote(h_send.at[h], h_recv.at[h], h_ss, h_rs.at[h // (heads - 2)], tdev)

    def arrived(ref, sem):
        remote(ref, ref, sem, sem, near).wait_recv()

    def left(ref, sem):
        remote(ref, ref, sem, sem, near).wait_send()

    w_move = remote(w, w_far, wf_ss, wf_rs, tdev)
    tb_in = remote(tb.at[0], tb.at[1], tb_ss, tb_rs, near)
    tb_y = remote(tb.at[0], tb.at[2], tb_ss, tb_rs, ydev)
    tb_relay = remote(tb.at[2], tb.at[3], tb_ss, tb_rs, near)

    for load in loads[1:7]:
        load.wait()
    freq, part, lead = lanes_ref[0:1, :], lanes_ref[1:2, :], lanes_ref[2:3, :]
    blocks = rows // WIDE
    block = lax.broadcasted_iota(jnp.int32, (blocks, HEAD), 0)
    slab = slab_ref[...] * SLAB_H
    place = jnp.where(part < 0.5, (block // SLAB_H).astype(F32), (slab + block % SLAB_H).astype(F32)) * freq
    across = lax.broadcasted_iota(jnp.int32, (WIDE, HEAD), 0).astype(F32) * freq
    trig = (jnp.cos(place), jnp.cos(across)), (jnp.sin(place), jnp.sin(across))

    def partner(x):
        wide = jnp.broadcast_to(x, (8, HEAD))
        near, far = PARTS[0] // 2, PARTS[1] // 2
        after = jnp.where(part < 0.5, pltpu.roll(wide, HEAD - near, 1), pltpu.roll(wide, HEAD - far, 1))
        before = jnp.where(part < 0.5, pltpu.roll(wide, near, 1), pltpu.roll(wide, far, 1))
        return jnp.where(lead > 0.5, after, before)[0:1]

    scale_q = F32(1.0) / jnp.sqrt(F32(HEAD))
    kg = kg_ref[...]
    qg = qg_ref[...] * scale_q
    for which, (by_block, by_column) in enumerate(trig):
        for gain, index in ((qg, 0), (kg, 2)):
            gain = gain if which == 0 else partner(gain)
            for i in range(blocks):
                full = jnp.where(part < 1.5, by_block[i : i + 1], by_column)
                tabs[index + which, i * WIDE : (i + 1) * WIDE, :] = full * gain
    line = lax.broadcasted_iota(jnp.int32, (trows, trows), 0)
    lane = lax.broadcasted_iota(jnp.int32, (trows, trows), 1)
    mark = jnp.where((line == lane) & (mask_ref[...] != 1), F32(NEGATIVE), F32(0.0))
    tb[0] = jnp.broadcast_to(jnp.sum(mark, axis=1, keepdims=True), (trows, HEAD)).astype(BF16)

    def norm_scale(x32):
        return lax.rsqrt(jnp.mean(x32 * x32, axis=-1, keepdims=True) + 0.05)

    def rotated(x, which):
        x32 = x.astype(F32)
        turned = jnp.dot(x, perm_ref[...], preferred_element_type=F32)
        return ((x32 * tabs[which] + turned * tabs[which + 1]) * norm_scale(x32)).astype(BF16)

    def prepare_q(h):
        q_mine[h] = rotated(q_ref[:, pl.ds(pl.multiple_of(h * HEAD, HEAD), HEAD)], 0)

    def prepare_kv(h):
        cols = pl.ds(pl.multiple_of(h * HEAD, HEAD), HEAD)
        mine[h, 0:rows, :] = rotated(k_ref[:, cols], 2)
        tk = tk_ref[:, cols].astype(F32)
        mine[h, rows:keys, :] = (tk * norm_scale(tk) * kg).astype(BF16)
        mine[h, keys : keys + rows, :] = v_ref[:, cols]
        mine[h, keys + rows : 2 * keys, :] = tv_ref[:, cols]

    def side(slot, i, part):
        where = pl.ds(part * keys, keys)
        return held[slot - 1, i, where, :] if slot else mine[mine_on(i), where, :]

    def score(slot, i, where):
        queries = q_held[slot - 1, i] if slot else q_mine[mine_on(i)]
        top = None
        for n in range(GROUP):
            sc = nt(side(n, i, 0), queries)
            mark = tb[n].astype(F32)
            mark = jnp.concatenate([mark] * (rows // HEAD), axis=1)
            sc = jnp.concatenate([sc[0:rows], sc[rows:keys] + mark], axis=0)
            where[n] = sc
            peak = jnp.max(sc, axis=0, keepdims=True)
            top = peak if top is None else jnp.maximum(top, peak)
        return top

    def weigh(i, where, top):
        total = None
        mixed = None
        for n in range(GROUP):
            p = jnp.exp(where[n] - top)
            amount = jnp.sum(p, axis=0, keepdims=True)
            got = tn(side(n, i, 1), p.astype(BF16))
            total = amount if total is None else total + amount
            mixed = got if mixed is None else mixed + got
        return mixed / total, top + jnp.log(total)

    wides = rows // HEAD

    def pack(to, o, lse):
        high = lse.astype(BF16).astype(F32)
        rest = lse - high
        mid = rest.astype(BF16).astype(F32)
        pieces = [x[:, i * HEAD : (i + 1) * HEAD] for x in (high, mid, rest - mid) for i in range(wides)]
        pieces.append(jnp.zeros((STATS - 3 * wides, HEAD), F32))
        to[rows : rows + STATS, :] = jnp.concatenate(pieces, axis=0).astype(BF16)
        for i in range(wides):
            to[i * HEAD : (i + 1) * HEAD, :] = o[:, i * HEAD : (i + 1) * HEAD].astype(BF16)

    def unpack(index, h):
        o = jnp.concatenate([o_recv[index, h, i * HEAD : (i + 1) * HEAD, :] for i in range(wides)], axis=1)
        stats = o_recv[index, h, rows : rows + STATS, :].astype(F32)
        levels = [
            jnp.concatenate([stats[k * wides + i : k * wides + i + 1] for i in range(wides)], axis=1)
            for k in range(3)
        ]
        return o.astype(F32), levels[0] + levels[1] + levels[2]

    def merge(h):
        hub = jnp.logical_and(inner, h % 2 == col)

        @pl.when(hub)
        def _():
            arrived(o_recv.at[1:2, h], o_rs.at[h])

        @pl.when(jnp.logical_not(hub))
        def _():
            arrived(o_recv.at[:, h], o_rs.at[h])

        (o, lse), (o_, lse_) = unpack(0, h), unpack(1, h)
        share = 1.0 / (1.0 + jnp.exp(lse_ - lse))
        o_all[...] = (o * share + o_ * (1.0 - share)).astype(BF16)
        h_send[h] = o_all[:, pl.ds(pl.multiple_of((1 - t) * half, half), half)].T
        h_move(h).start()
        cols = pl.ds(pl.multiple_of(h * HEAD, HEAD), HEAD)
        h_mine[:, cols] = o_all[:, pl.ds(pl.multiple_of(t * half, half), half)].T

    loads[0].wait()
    prepare_q(mine_off(0))
    prepare_q(mine_on(0))

    @pl.when(inner)
    def _():
        pl.semaphore_wait(barrier, len(friends) + 1)
        q_far(2, 0).start()

    @pl.when(outer)
    def _():
        pl.semaphore_wait(barrier, len(friends))
        q_in(0).start()
        tb_in.start()

    q_off(0).start()
    tb_y.start()

    def queries(i, c):
        prepare_q(mine_off(i))
        q_off(i).start()
        prepare_q(mine_on(i))

        @pl.when(inner)
        def _():
            q_far(2, i).start()

        @pl.when(outer)
        def _():
            q_in(i).start()

        return c

    lax.fori_loop(1, pairs, queries, 0)
    for load in loads[7:]:
        load.wait()
    prepare_kv(mine_off(0))
    kv_off(0).start()
    prepare_kv(mine_on(0))

    def keep(i, c):
        prepare_kv(mine_off(i))
        kv_off(i).start()
        prepare_kv(mine_on(i))
        return c

    lax.fori_loop(1, pairs, keep, 0)

    @pl.when(outer)
    def _():
        tb_y.wait_recv()
        tb_relay.start()

        def pass_queries(i, c):
            q_off(i).wait_recv()
            q_relay(i).start()
            return c

        def pass_keys(i, c):
            kv_in(i).start()
            kv_off(i).wait_recv()
            kv_relay(i).start()
            return c

        lax.fori_loop(0, 1, pass_queries, 0)
        pass_keys(0, 0)
        lax.fori_loop(1, pairs, pass_queries, 0)
        lax.fori_loop(1, pairs, pass_keys, 0)

    w_copy.wait()
    w_move.start()
    half = rows // 2

    def attend(j, h):
        queries = qs[j, h]
        scores = []
        top = None
        for slot in range(GROUP):
            sc = nt(kv[slot, h, 0:keys, :], queries)
            mark = tb[slot].astype(F32)
            mark = jnp.concatenate([mark] * (rows // HEAD), axis=1)
            sc = jnp.concatenate([sc[0:rows], sc[rows:keys] + mark], axis=0)
            peak = jnp.max(sc, axis=0, keepdims=True)
            top = peak if top is None else jnp.maximum(top, peak)
            scores.append(sc)
        total = None
        acc = None
        for slot in range(GROUP):
            p = jnp.exp(scores[slot] - top)
            part = jnp.sum(p, axis=0, keepdims=True)
            mixed = tn(kv[slot, h, keys : 2 * keys, :], p.astype(BF16))
            total = part if total is None else total + part
            acc = mixed if acc is None else acc + mixed
        return acc / total, top + jnp.log(total)

    def main(h, c):
        @pl.when(h + 1 < heads)
        def _():
            kv_z(h + 1).wait_recv()
            kv_relay(h + 1).start()

        send(h, True)

        kv_y(h).wait_recv()

        @pl.when(h == 0)
        def _():
            tb_y.wait_recv()
            tb_relay.wait_recv()

        for j in range(1, a):
            q_move(j, h).wait_recv()
        kv_relay(h).wait_recv()
        for j in range(1, a):
            o, lse = attend(j, h)
            high = lse.astype(BF16)
            rest = lse - high.astype(F32)
            mid = rest.astype(BF16)
            tail = (rest - mid.astype(F32)).astype(BF16)
            o_send[j - 1, h, HEAD : HEAD + 16, :] = jnp.concatenate(
                [high.astype(F32), mid.astype(F32), tail.astype(F32), jnp.zeros((13, rows), F32)], axis=0
            ).astype(BF16)
            o_send[j - 1, h, 0:HEAD, :] = o.astype(BF16)
            o_move(j, h).start()
        o, lse = attend(0, h)
        o_own[h] = o
        lse_own[h] = jnp.broadcast_to(lse, (8, rows))

        @pl.when(h > 0)
        def _():
            merge(h - 1)

        return c

    def merge(h):
        lses = [lse_own[h][0:1]]
        parts = [o_own[h]]
        for j in range(1, a):
            o_move(j, h).wait_recv()
            stats = o_recv[j - 1, h, HEAD : HEAD + 16, :].astype(F32)
            lses.append(stats[0:1] + stats[1:2] + stats[2:3])
            parts.append(o_recv[j - 1, h, 0:HEAD, :].astype(F32))
        top = functools.reduce(jnp.maximum, lses)
        shares = [jnp.exp(x - top) for x in lses]
        total = functools.reduce(jnp.add, shares)
        o = functools.reduce(jnp.add, [x * y for x, y in zip(parts, shares)]) / total
        o_all[...] = o.astype(BF16)
        h_send[h] = o_all[:, pl.ds(pl.multiple_of((1 - t) * half, half), half)].T
        h_move(h).start()
        cols = pl.ds(pl.multiple_of(h * HEAD, HEAD), HEAD)
        h_mine[:, cols] = o_all[:, pl.ds(pl.multiple_of(t * half, half), half)].T

    lax.fori_loop(0, heads, main, 0)

    step = w.shape[1] // chunks
    spans = [slice(i * step, (i + 1) * step) for i in range(chunks)]
    early = (heads - 1) * HEAD

    def dot(x, y):
        return jnp.dot(x, y, preferred_element_type=F32)

    for span in spans:
        acc[0, :, span] = dot(h_mine[:, :early], w[:early, span])
    w_move.wait_recv()
    for h in range(heads - 1):
        h_move(h).wait_recv()
    theirs = jnp.concatenate([h_recv[h] for h in range(heads - 1)], axis=1)
    for span in spans:
        acc[1, :, span] = dot(theirs, w_far[:early, span])
    merge(heads - 1)
    for span in spans:
        acc[0, :, span] += dot(h_mine[:, early:], w[early:, span])
    h_move(heads - 1).wait_recv()
    for span in spans:
        far = acc[1, :, span] + dot(h_recv[heads - 1], w_far[early:, span])
        near = acc[0, :, span]
        out_ref[:, span] = (near.astype(BF16).astype(F32) + far.astype(BF16).astype(F32)).astype(BF16)

    def drain(h, c):
        kv_z(h).wait_send()
        kv_y(h).wait_send()
        kv_relay(h).wait_send()
        h_move(h).wait_send()
        for j in range(1, a):
            q_move(j, h).wait_send()
            o_move(j, h).wait_send()
        return c

    lax.fori_loop(0, heads, drain, 0)
    tb_z.wait_send()
    tb_y.wait_send()
    tb_relay.wait_send()
    w_move.wait_send()


def hub_kernel(
    chunks,
    slab_hbm, q_hbm, k_hbm, v_hbm, tk_hbm, tv_hbm, mask_hbm, qg_hbm, kg_hbm, lanes_hbm, perm_hbm, w_ref,
    out_ref,
    mine, held, tb, q_mine, q_held, o_send, o_recv, scores_a, scores_b, o_all, w, w_far, h_mine, h_send, h_recv,
    acc, tabs, q_ref, k_ref, v_ref, tk_ref, tv_ref, slab_ref, mask_ref, qg_ref, kg_ref, lanes_ref, perm_ref,
    kv_ss, kv_rs, tb_ss, tb_rs, q_ss, q_rs, o_ss, o_rs, h_ss, h_rs, wf_ss, wf_rs, w_sem, in_sem,
):
    rows, width = q_ref.shape
    heads = width // HEAD
    trows = tk_ref.shape[0]
    keys = rows + trows
    half = rows // 2
    pairs = heads // 2
    g, s, t = lax.axis_index("grp"), lax.axis_index("seq"), lax.axis_index("tp")
    u, low = s // GROUP, s % GROUP
    row, col = low // 2, low % 2
    inner = row + u == 1
    outer = row + u != 1
    aside = 1 - 2 * col

    def dev(seq):
        return (g, seq, t)

    near_s, far_s, cross_s = s + 2 - 4 * row, s + 2 - 4 * u, s + GROUP - 2 * GROUP * u
    near, far, cross, ydev = dev(near_s), dev(far_s), dev(cross_s), dev(s + aside)
    near_y, far_y, cross_y = dev(near_s + aside), dev(far_s + aside), dev(cross_s + aside)
    tdev = (g, s, 1 - t)

    barrier = pltpu.get_barrier_semaphore()
    friends = [near, ydev, tdev]
    for friend in friends:
        pl.semaphore_signal(barrier, inc=1, device_id=friend, device_id_type=MESH)

    @pl.when(inner)
    def _():
        pl.semaphore_signal(barrier, inc=1, device_id=far, device_id_type=MESH)

    loads = [
        pltpu.make_async_copy(x, y, in_sem.at[i])
        for i, (x, y) in enumerate(
            (
                (q_hbm, q_ref), (lanes_hbm, lanes_ref), (slab_hbm, slab_ref), (qg_hbm, qg_ref), (kg_hbm, kg_ref),
                (perm_hbm, perm_ref), (mask_hbm, mask_ref),
                (k_hbm, k_ref), (tk_hbm, tk_ref), (v_hbm, v_ref), (tv_hbm, tv_ref),
            )
        )
    ]
    for load in loads:
        load.start()
    w_copy = pltpu.make_async_copy(w_ref, w, w_sem)
    w_copy.start()

    def remote(src, dst, ss, rs, to):
        return pltpu.make_async_remote_copy(
            src_ref=src, dst_ref=dst, send_sem=ss, recv_sem=rs, device_id=to, device_id_type=MESH
        )

    def mine_on(i):
        return 2 * i + col

    def mine_off(i):
        return 2 * i + 1 - col

    def kv_move(src, slot, i, to):
        return remote(src, held.at[slot - 1, i], kv_ss, kv_rs.at[i], to)

    def kv_in(i):
        return kv_move(mine.at[mine_on(i)], 1, i, near)

    def kv_off(i):
        return kv_move(mine.at[mine_off(i)], 2, i, ydev)

    def kv_relay(i):
        return kv_move(held.at[1, i], 3, i, near)

    def q_move(src, slot, i, to):
        return remote(src, q_held.at[slot - 1, i], q_ss, q_rs.at[{1: 0, 4: 1, 5: 2}.get(slot, 3), i], to)

    def q_in(i):
        return q_move(q_mine.at[mine_on(i)], 1, i, near)

    def q_off(i):
        return q_move(q_mine.at[mine_off(i)], 4, i, ydev)

    def q_relay(i):
        return q_move(q_held.at[3, i], 5, i, near)

    def q_far(slot, i):
        if slot == 2:
            return q_move(q_mine.at[mine_on(i)], 2, i, far)
        start = {3: 1, 6: 4, 7: 5}[slot]
        return q_move(q_held.at[start - 1, i], slot, i, far)

    def o_move(slot, i):
        index, to = {
            1: (0, near), 4: (0, ydev), 5: (0, near_y),
            2: (1, far), 3: (1, cross), 6: (1, far_y), 7: (1, cross_y),
        }[slot]
        h = mine_on(i)
        return remote(
            o_send.at[slot - 1, i], o_recv.at[index, h], o_ss, o_rs.at[h], to
        )

    def h_move(h):
        return remote(h_send.at[h], h_recv.at[h], h_ss, h_rs.at[h // (heads - 2)], tdev)

    def arrived(ref, sem):
        remote(ref, ref, sem, sem, near).wait_recv()

    def left(ref, sem):
        remote(ref, ref, sem, sem, near).wait_send()

    w_move = remote(w, w_far, wf_ss, wf_rs, tdev)
    tb_in = remote(tb.at[0], tb.at[1], tb_ss, tb_rs, near)
    tb_y = remote(tb.at[0], tb.at[2], tb_ss, tb_rs, ydev)
    tb_relay = remote(tb.at[2], tb.at[3], tb_ss, tb_rs, near)

    for load in loads[1:7]:
        load.wait()
    freq, part, lead = lanes_ref[0:1, :], lanes_ref[1:2, :], lanes_ref[2:3, :]
    blocks = rows // WIDE
    block = lax.broadcasted_iota(jnp.int32, (blocks, HEAD), 0)
    slab = slab_ref[...] * SLAB_H
    place = jnp.where(part < 0.5, (block // SLAB_H).astype(F32), (slab + block % SLAB_H).astype(F32)) * freq
    across = lax.broadcasted_iota(jnp.int32, (WIDE, HEAD), 0).astype(F32) * freq
    trig = (jnp.cos(place), jnp.cos(across)), (jnp.sin(place), jnp.sin(across))

    def partner(x):
        wide = jnp.broadcast_to(x, (8, HEAD))
        near, far = PARTS[0] // 2, PARTS[1] // 2
        after = jnp.where(part < 0.5, pltpu.roll(wide, HEAD - near, 1), pltpu.roll(wide, HEAD - far, 1))
        before = jnp.where(part < 0.5, pltpu.roll(wide, near, 1), pltpu.roll(wide, far, 1))
        return jnp.where(lead > 0.5, after, before)[0:1]

    scale_q = F32(1.0) / jnp.sqrt(F32(HEAD))
    kg = kg_ref[...]
    qg = qg_ref[...] * scale_q
    for which, (by_block, by_column) in enumerate(trig):
        for gain, index in ((qg, 0), (kg, 2)):
            gain = gain if which == 0 else partner(gain)
            for i in range(blocks):
                full = jnp.where(part < 1.5, by_block[i : i + 1], by_column)
                tabs[index + which, i * WIDE : (i + 1) * WIDE, :] = full * gain
    line = lax.broadcasted_iota(jnp.int32, (trows, trows), 0)
    lane = lax.broadcasted_iota(jnp.int32, (trows, trows), 1)
    mark = jnp.where((line == lane) & (mask_ref[...] != 1), F32(NEGATIVE), F32(0.0))
    tb[0] = jnp.broadcast_to(jnp.sum(mark, axis=1, keepdims=True), (trows, HEAD)).astype(BF16)

    def norm_scale(x32):
        return lax.rsqrt(jnp.mean(x32 * x32, axis=-1, keepdims=True) + 0.05)

    def rotated(x, which):
        x32 = x.astype(F32)
        turned = jnp.dot(x, perm_ref[...], preferred_element_type=F32)
        return ((x32 * tabs[which] + turned * tabs[which + 1]) * norm_scale(x32)).astype(BF16)

    def prepare_q(h):
        q_mine[h] = rotated(q_ref[:, pl.ds(pl.multiple_of(h * HEAD, HEAD), HEAD)], 0)

    def prepare_kv(h):
        cols = pl.ds(pl.multiple_of(h * HEAD, HEAD), HEAD)
        mine[h, 0:rows, :] = rotated(k_ref[:, cols], 2)
        tk = tk_ref[:, cols].astype(F32)
        mine[h, rows:keys, :] = (tk * norm_scale(tk) * kg).astype(BF16)
        mine[h, keys : keys + rows, :] = v_ref[:, cols]
        mine[h, keys + rows : 2 * keys, :] = tv_ref[:, cols]

    def side(slot, i, part):
        where = pl.ds(part * keys, keys)
        return held[slot - 1, i, where, :] if slot else mine[mine_on(i), where, :]

    def score(slot, i, where):
        queries = q_held[slot - 1, i] if slot else q_mine[mine_on(i)]
        top = None
        for n in range(GROUP):
            sc = nt(side(n, i, 0), queries)
            mark = tb[n].astype(F32)
            mark = jnp.concatenate([mark] * (rows // HEAD), axis=1)
            sc = jnp.concatenate([sc[0:rows], sc[rows:keys] + mark], axis=0)
            where[n] = sc
            peak = jnp.max(sc, axis=0, keepdims=True)
            top = peak if top is None else jnp.maximum(top, peak)
        return top

    def weigh(i, where, top):
        total = None
        mixed = None
        for n in range(GROUP):
            p = jnp.exp(where[n] - top)
            amount = jnp.sum(p, axis=0, keepdims=True)
            got = tn(side(n, i, 1), p.astype(BF16))
            total = amount if total is None else total + amount
            mixed = got if mixed is None else mixed + got
        return mixed / total, top + jnp.log(total)

    wides = rows // HEAD

    def pack(to, o, lse):
        high = lse.astype(BF16).astype(F32)
        rest = lse - high
        mid = rest.astype(BF16).astype(F32)
        pieces = [x[:, i * HEAD : (i + 1) * HEAD] for x in (high, mid, rest - mid) for i in range(wides)]
        pieces.append(jnp.zeros((STATS - 3 * wides, HEAD), F32))
        to[rows : rows + STATS, :] = jnp.concatenate(pieces, axis=0).astype(BF16)
        for i in range(wides):
            to[i * HEAD : (i + 1) * HEAD, :] = o[:, i * HEAD : (i + 1) * HEAD].astype(BF16)

    def unpack(index, h):
        o = jnp.concatenate([o_recv[index, h, i * HEAD : (i + 1) * HEAD, :] for i in range(wides)], axis=1)
        stats = o_recv[index, h, rows : rows + STATS, :].astype(F32)
        levels = [
            jnp.concatenate([stats[k * wides + i : k * wides + i + 1] for i in range(wides)], axis=1)
            for k in range(3)
        ]
        return o.astype(F32), levels[0] + levels[1] + levels[2]

    def merge(h):
        hub = jnp.logical_and(inner, h % 2 == col)

        @pl.when(hub)
        def _():
            arrived(o_recv.at[1:2, h], o_rs.at[h])

        @pl.when(jnp.logical_not(hub))
        def _():
            arrived(o_recv.at[:, h], o_rs.at[h])

        (o, lse), (o_, lse_) = unpack(0, h), unpack(1, h)
        share = 1.0 / (1.0 + jnp.exp(lse_ - lse))
        o_all[...] = (o * share + o_ * (1.0 - share)).astype(BF16)
        h_send[h] = o_all[:, pl.ds(pl.multiple_of((1 - t) * half, half), half)].T
        h_move(h).start()
        cols = pl.ds(pl.multiple_of(h * HEAD, HEAD), HEAD)
        h_mine[:, cols] = o_all[:, pl.ds(pl.multiple_of(t * half, half), half)].T

    loads[0].wait()
    prepare_q(mine_off(0))
    prepare_q(mine_on(0))

    @pl.when(inner)
    def _():
        pl.semaphore_wait(barrier, len(friends) + 1)
        q_far(2, 0).start()

    @pl.when(outer)
    def _():
        pl.semaphore_wait(barrier, len(friends))
        q_in(0).start()
        tb_in.start()

    q_off(0).start()
    tb_y.start()

    def queries(i, c):
        prepare_q(mine_off(i))
        q_off(i).start()
        prepare_q(mine_on(i))

        @pl.when(inner)
        def _():
            q_far(2, i).start()

        @pl.when(outer)
        def _():
            q_in(i).start()

        return c

    lax.fori_loop(1, pairs, queries, 0)
    for load in loads[7:]:
        load.wait()
    prepare_kv(mine_off(0))
    kv_off(0).start()
    prepare_kv(mine_on(0))

    def keep(i, c):
        prepare_kv(mine_off(i))
        kv_off(i).start()
        prepare_kv(mine_on(i))
        return c

    lax.fori_loop(1, pairs, keep, 0)

    @pl.when(outer)
    def _():
        tb_y.wait_recv()
        tb_relay.start()

        def pass_queries(i, c):
            q_off(i).wait_recv()
            q_relay(i).start()
            return c

        lax.fori_loop(0, pairs, pass_queries, 0)

        def pass_keys(i, c):
            kv_in(i).start()
            kv_off(i).wait_recv()
            kv_relay(i).start()
            return c

        lax.fori_loop(0, pairs, pass_keys, 0)

    w_copy.wait()
    w_move.start()

    @pl.when(inner)
    def _():
        def onward(i):
            q_in(i).wait_recv()
            q_far(3, i).start()
            q_off(i).wait_recv()
            q_far(6, i).start()

        def onward_last(i):
            q_relay(i).wait_recv()
            q_far(7, i).start()

        onward(0)
        onward(1)

        def trail(i, c):
            onward_last(i)

            @pl.when(i + 2 < pairs)
            def _():
                onward(i + 2)

            return c

        lax.fori_loop(0, pairs, trail, 0)
        arrived(tb.at[1:GROUP], tb_rs)

        def main(i, c):
            arrived(q_held.at[0:4, i], q_rs.at[3, i])
            arrived(held.at[:, i], kv_rs.at[i])
            order = (7, 5, 3, 1, 6, 2, 4, 0)
            top = score(order[0], i, scores_a)
            for n, slot in enumerate(order):
                here, there = ((scores_a, scores_b), (scores_b, scores_a))[n % 2]
                after = score(order[n + 1], i, there) if n + 1 < HUB_SLOTS else None
                o, lse = weigh(i, here, top)
                top = after
                if slot:
                    pack(o_send.at[slot - 1, i], o, lse)
                    o_move(slot, i).start()
                else:
                    pack(o_recv.at[0, mine_on(i)], o, lse)

            return c

        lax.fori_loop(0, pairs, main, 0)

    def collect(h, c):
        merge(h)
        return c

    lax.fori_loop(0, heads - 2, collect, 0)

    step = w.shape[1] // chunks
    spans = [slice(i * step, (i + 1) * step) for i in range(chunks)]
    early = (heads - 2) * HEAD

    def dot(x, y):
        return jnp.dot(x, y, preferred_element_type=F32)

    for span in spans:
        acc[0, :, span] = dot(h_mine[:, :early], w[:early, span])
    w_move.wait_recv()
    arrived(h_recv.at[0 : heads - 2], h_rs.at[0])
    theirs = jnp.concatenate([h_recv[h] for h in range(heads - 2)], axis=1)
    for span in spans:
        acc[1, :, span] = dot(theirs, w_far[:early, span])

    merge(heads - 2)
    merge(heads - 1)

    for span in spans:
        acc[0, :, span] += dot(h_mine[:, early:], w[early:, span])
    arrived(h_recv.at[heads - 2 : heads], h_rs.at[1])
    last = jnp.concatenate([h_recv[heads - 2], h_recv[heads - 1]], axis=1)
    for span in spans:
        theirs = acc[1, :, span] + dot(last, w_far[early:, span])
        mine_too = acc[0, :, span]
        out_ref[:, span] = (mine_too.astype(BF16).astype(F32) + theirs.astype(BF16).astype(F32)).astype(BF16)

    @pl.when(inner)
    def _():
        left(q_held.at[0:5], q_ss)
        left(held.at[0:1], kv_ss)
        left(o_send, o_ss)
        left(tb.at[0:1], tb_ss)

    @pl.when(outer)
    def _():
        left(q_held.at[0:3], q_ss)
        left(held, kv_ss)
        left(tb.at[0:3], tb_ss)

    left(h_send, h_ss)
    w_move.wait_send()


def hub_scratch(rows, trows, heads, model, w_shape, inputs):
    keys, half, pairs = rows + trows, rows // 2, heads // 2
    dma = pltpu.SemaphoreType.DMA
    return [
        pltpu.VMEM((heads, 2 * keys, HEAD), BF16),
        pltpu.VMEM((3, pairs, 2 * keys, HEAD), BF16),
        pltpu.VMEM((GROUP, trows, HEAD), BF16),
        pltpu.VMEM((heads, rows, HEAD), BF16),
        pltpu.VMEM((HUB_SLOTS - 1, pairs, rows, HEAD), BF16),
        pltpu.VMEM((HUB_SLOTS - 1, pairs, rows + STATS, HEAD), BF16),
        pltpu.VMEM((2, heads, rows + STATS, HEAD), BF16),
        pltpu.VMEM((GROUP, keys, rows), F32),
        pltpu.VMEM((GROUP, keys, rows), F32),
        pltpu.VMEM((HEAD, rows), BF16),
        pltpu.VMEM(w_shape, BF16),
        pltpu.VMEM(w_shape, BF16),
        pltpu.VMEM((half, heads * HEAD), BF16),
        pltpu.VMEM((heads, half, HEAD), BF16),
        pltpu.VMEM((heads, half, HEAD), BF16),
        pltpu.VMEM((2, half, model), F32),
        pltpu.VMEM((4, rows, HEAD), F32),
        *[pltpu.VMEM(x.shape, x.dtype) for x in inputs],
        dma, dma((pairs,)), dma, dma, dma, dma((4, pairs)), dma, dma((heads,)), dma, dma((2,)), dma, dma, dma,
        dma((11,)),
    ]


def body(
    n,
    visual_q, visual_key_input, visual_v, text_k, text_v, text_mask, slab_order, q_gain, key_norm_gain, w_out,
):
    rows, width = visual_q.shape
    heads = width // HEAD
    model = w_out.shape[1]
    a = n // GROUP
    trows = -(-text_k.shape[0] // 16) * 16
    pad = trows - text_k.shape[0]
    if pad:
        text_k = jnp.pad(text_k, ((0, pad), (0, 0)))
        text_v = jnp.pad(text_v, ((0, pad), (0, 0)))
        text_mask = jnp.pad(text_mask, (0, pad))
    lanes, perm = lane_constants()
    chunks = 6 if model % (6 * HEAD) == 0 else 1
    keys = rows + trows
    half = rows // 2
    peers = a - 1
    vm = pl.BlockSpec(memory_space=pltpu.VMEM)
    anywhere = pl.BlockSpec(memory_space=pl.ANY)
    dma = pltpu.SemaphoreType.DMA
    operands = (
        slab_order, visual_q, visual_key_input, visual_v, text_k, text_v, text_mask[None], q_gain[None],
        key_norm_gain[None], jnp.asarray(lanes), jnp.asarray(perm, BF16), w_out,
    )
    if n == 2 * GROUP and rows % HEAD == 0 and heads % 2 == 0 and heads > 3:
        run = functools.partial(hub_kernel, chunks)
        operands = (slab_order[None],) + operands[1:]
        scratch = hub_scratch(rows, trows, heads, model, w_out.shape, operands[1:6] + operands[:1] + operands[6:11])
        places = [anywhere] * 12
    else:
        run = functools.partial(kernel, n, chunks)
        places = [pl.BlockSpec(memory_space=pltpu.SMEM)] + [anywhere] * 5 + [vm] * 5 + [anywhere]
        scratch = [
                pltpu.VMEM((GROUP, heads, 2 * keys, HEAD), BF16),
                pltpu.VMEM((GROUP, trows, HEAD), BF16),
                pltpu.VMEM((a, heads, rows, HEAD), BF16),
                pltpu.VMEM((peers, heads, HEAD + 16, rows), BF16),
                pltpu.VMEM((peers, heads, HEAD + 16, rows), BF16),
                pltpu.VMEM((heads, HEAD, rows), F32),
                pltpu.VMEM((heads, 8, rows), F32),
                pltpu.VMEM((HEAD, rows), BF16),
                pltpu.VMEM(w_out.shape, BF16),
                pltpu.VMEM(w_out.shape, BF16),
                pltpu.VMEM((half, width), BF16),
                pltpu.VMEM((heads, half, HEAD), BF16),
                pltpu.VMEM((heads, half, HEAD), BF16),
                pltpu.VMEM((2, half, model), F32),
                pltpu.VMEM((4, rows, HEAD), F32),
                *[pltpu.VMEM(x.shape, BF16) for x in (visual_q, visual_key_input, visual_v, text_k, text_v)],
                dma((3, heads)), dma((3, heads)), dma((3,)), dma((3,)),
                dma((peers, heads)), dma((peers, heads)), dma((peers, heads)), dma((peers, heads)),
                dma((heads,)), dma((heads,)), dma, dma, dma, dma((5,)),
        ]
    return pl.pallas_call(
        run,
        out_shape=pltpu.VMEM((half, model), BF16),
        in_specs=places,
        out_specs=vm,
        scratch_shapes=scratch,
        compiler_params=pltpu.CompilerParams(
            collective_id=0, has_side_effects=True, vmem_limit_bytes=60 * 1024 * 1024
        ),
    )(*operands)


def solution(mesh):
    rows = P(("grp", "seq"), "tp")
    placed = (rows,) * 5 + (P(("grp", "seq")),) * 2 + (P(), P(), P("tp", None))
    return jax.shard_map(
        functools.partial(body, mesh.shape["seq"]),
        mesh=mesh, in_specs=placed, out_specs=P(("grp", "seq", "tp"), None), check_vma=False,
    )
```

```python
import functools

import jax
import jax.numpy as jnp
import numpy as np
from jax import lax
from jax.experimental import pallas as pl
from jax.experimental.pallas import tpu as pltpu
from jax.sharding import PartitionSpec as P

SLAB_H = 2
WIDE = 32
HEAD = 128
PARTS = (32, 48, 48)
NEGATIVE = -1e30
MESH = pl.DeviceIdType.MESH
F32 = jnp.float32
BF16 = jnp.bfloat16
LEAD_Y, LEAD_Z, LEAD_Q = 2, 2, 2
GROUP = 4
STATS = 8
HUB_SLOTS = 8


def lane_constants():
    lanes = np.zeros((8, HEAD), np.float32)
    perm = np.zeros((HEAD, HEAD), np.float32)
    offset = 0
    for index, size in enumerate(PARTS):
        half = size // 2
        f = np.float32(10000.0) ** (-np.arange(half, dtype=np.float32) / np.float32(half))
        lanes[0, offset : offset + half] = f
        lanes[0, offset + half : offset + size] = f
        lanes[1, offset : offset + size] = index
        lanes[2, offset : offset + half] = 1.0
        for j in range(half):
            perm[offset + half + j, offset + j] = -1.0
            perm[offset + j, offset + half + j] = 1.0
        offset += size
    return lanes, perm


def nt(a, b):
    return lax.dot_general(a, b, (((1,), (1,)), ((), ())), preferred_element_type=F32)


def tn(a, b):
    return lax.dot_general(a, b, (((0,), (0,)), ((), ())), preferred_element_type=F32)


def kernel(
    n, chunks,
    slab_ref, q_hbm, k_hbm, v_hbm, tk_hbm, tv_hbm, mask_ref, qg_ref, kg_ref, lanes_ref, perm_ref, w_ref,
    out_ref,
    kv, tb, qs, o_send, o_recv, o_own, lse_own, o_all, w, w_far, h_mine, h_send, h_recv, acc, tabs,
    q_ref, k_ref, v_ref, tk_ref, tv_ref,
    kv_ss, kv_rs, tb_ss, tb_rs, q_ss, q_rs, o_ss, o_rs, h_ss, h_rs, wf_ss, wf_rs, w_sem, in_sem,
):
    rows, width = q_ref.shape
    heads = width // HEAD
    trows = tk_ref.shape[0]
    keys = rows + trows
    a = n // GROUP
    g, s, t = lax.axis_index("grp"), lax.axis_index("seq"), lax.axis_index("tp")
    u, low = s // GROUP, s % GROUP
    zdev = (g, s + 2 - 4 * (low // 2), t)
    ydev = (g, s + 1 - 2 * (low % 2), t)
    tdev = (g, s, 1 - t)
    fwd = [(g, lax.rem(u + j, a) * GROUP + low, t) for j in range(a)]
    back = [(g, lax.rem(u + a - j, a) * GROUP + low, t) for j in range(a)]

    barrier = pltpu.get_barrier_semaphore()
    friends = [zdev, ydev, tdev] + fwd[1:]
    for dev in friends:
        pl.semaphore_signal(barrier, inc=1, device_id=dev, device_id_type=MESH)

    loads = [
        pltpu.make_async_copy(x, y, in_sem.at[i])
        for i, (x, y) in enumerate(
            ((k_hbm, k_ref), (tk_hbm, tk_ref), (v_hbm, v_ref), (tv_hbm, tv_ref), (q_hbm, q_ref))
        )
    ]
    for load in loads:
        load.start()
    w_copy = pltpu.make_async_copy(w_ref, w, w_sem)
    w_copy.start()

    def remote(src, dst, ss, rs, dev):
        return pltpu.make_async_remote_copy(
            src_ref=src, dst_ref=dst, send_sem=ss, recv_sem=rs, device_id=dev, device_id_type=MESH
        )

    def kv_z(h):
        return remote(kv.at[0, h], kv.at[1, h], kv_ss.at[0, h], kv_rs.at[0, h], zdev)

    def kv_y(h):
        return remote(kv.at[0, h], kv.at[2, h], kv_ss.at[1, h], kv_rs.at[1, h], ydev)

    def kv_relay(h):
        return remote(kv.at[1, h], kv.at[3, h], kv_ss.at[2, h], kv_rs.at[2, h], ydev)

    def q_move(j, h):
        return remote(qs.at[0, h], qs.at[j, h], q_ss.at[j - 1, h], q_rs.at[j - 1, h], fwd[j])

    def o_move(j, h):
        return remote(
            o_send.at[j - 1, h], o_recv.at[j - 1, h], o_ss.at[j - 1, h], o_rs.at[j - 1, h], back[j]
        )

    tb_z = remote(tb.at[0], tb.at[1], tb_ss.at[0], tb_rs.at[0], zdev)
    tb_y = remote(tb.at[0], tb.at[2], tb_ss.at[1], tb_rs.at[1], ydev)
    tb_relay = remote(tb.at[1], tb.at[3], tb_ss.at[2], tb_rs.at[2], ydev)

    freq, part, lead = lanes_ref[0:1, :], lanes_ref[1:2, :], lanes_ref[2:3, :]
    blocks = rows // WIDE
    block = lax.broadcasted_iota(jnp.int32, (blocks, HEAD), 0)
    slab = slab_ref[0] * SLAB_H
    place = jnp.where(part < 0.5, (block // SLAB_H).astype(F32), (slab + block % SLAB_H).astype(F32)) * freq
    across = lax.broadcasted_iota(jnp.int32, (WIDE, HEAD), 0).astype(F32) * freq
    trig = (jnp.cos(place), jnp.cos(across)), (jnp.sin(place), jnp.sin(across))

    def partner(x):
        wide = jnp.broadcast_to(x, (8, HEAD))
        near, far = PARTS[0] // 2, PARTS[1] // 2
        after = jnp.where(part < 0.5, pltpu.roll(wide, HEAD - near, 1), pltpu.roll(wide, HEAD - far, 1))
        before = jnp.where(part < 0.5, pltpu.roll(wide, near, 1), pltpu.roll(wide, far, 1))
        return jnp.where(lead > 0.5, after, before)[0:1]

    def h_move(h):
        return remote(h_send.at[h], h_recv.at[h], h_ss.at[h], h_rs.at[h], tdev)

    w_move = remote(w, w_far, wf_ss, wf_rs, tdev)

    scale_q = F32(1.0) / jnp.sqrt(F32(HEAD))
    kg = kg_ref[...]
    qg = qg_ref[...] * scale_q
    for which, (by_block, by_column) in enumerate(trig):
        for gain, index in ((qg, 0), (kg, 2)):
            gain = gain if which == 0 else partner(gain)
            for i in range(blocks):
                full = jnp.where(part < 1.5, by_block[i : i + 1], by_column)
                tabs[index + which, i * WIDE : (i + 1) * WIDE, :] = full * gain
    row = lax.broadcasted_iota(jnp.int32, (trows, trows), 0)
    col = lax.broadcasted_iota(jnp.int32, (trows, trows), 1)
    mark = jnp.where((row == col) & (mask_ref[...] != 1), F32(NEGATIVE), F32(0.0))
    tb[0] = jnp.broadcast_to(jnp.sum(mark, axis=1, keepdims=True), (trows, HEAD)).astype(BF16)

    def norm_scale(x32):
        return lax.rsqrt(jnp.mean(x32 * x32, axis=-1, keepdims=True) + 0.05)

    def rotated(x, which):
        x32 = x.astype(F32)
        turned = jnp.dot(x, perm_ref[...], preferred_element_type=F32)
        return ((x32 * tabs[which] + turned * tabs[which + 1]) * norm_scale(x32)).astype(BF16)

    def prepare(h):
        cols = pl.ds(pl.multiple_of(h * HEAD, HEAD), HEAD)
        kv[0, h, 0:rows, :] = rotated(k_ref[:, cols], 2)
        tk = tk_ref[:, cols].astype(F32)
        kv[0, h, rows:keys, :] = (tk * norm_scale(tk) * kg).astype(BF16)
        kv[0, h, keys : keys + rows, :] = v_ref[:, cols]
        kv[0, h, keys + rows : 2 * keys, :] = tv_ref[:, cols]
        qs[0, h] = rotated(q_ref[:, cols], 0)

    def send(h, ready):
        for lead, start in ((LEAD_Y, send_y), (LEAD_Z, send_z), (LEAD_Q, send_q)):
            if ready is None:

                @pl.when(h < lead)
                def _(start=start):
                    start(h)
            else:

                @pl.when(h + lead < heads)
                def _(start=start, lead=lead):
                    start(h + lead)

    def send_y(h):
        kv_y(h).start()

    def send_z(h):
        kv_z(h).start()

    def send_q(h):
        for j in range(1, a):
            q_move(j, h).start()

    for load in loads:
        load.wait()
    prepare(0)
    pl.semaphore_wait(barrier, len(friends))
    tb_z.start()
    tb_y.start()
    send(0, None)

    def first(h, c):
        prepare(h)
        send(h, None)
        return c

    lax.fori_loop(1, heads, first, 0)
    tb_z.wait_recv()
    tb_relay.start()
    kv_z(0).wait_recv()
    kv_relay(0).start()
    w_copy.wait()
    w_move.start()
    half = rows // 2

    def attend(j, h):
        queries = qs[j, h]
        scores = []
        top = None
        for slot in range(GROUP):
            sc = nt(kv[slot, h, 0:keys, :], queries)
            mark = tb[slot].astype(F32)
            mark = jnp.concatenate([mark] * (rows // HEAD), axis=1)
            sc = jnp.concatenate([sc[0:rows], sc[rows:keys] + mark], axis=0)
            peak = jnp.max(sc, axis=0, keepdims=True)
            top = peak if top is None else jnp.maximum(top, peak)
            scores.append(sc)
        total = None
        acc = None
        for slot in range(GROUP):
            p = jnp.exp(scores[slot] - top)
            part = jnp.sum(p, axis=0, keepdims=True)
            mixed = tn(kv[slot, h, keys : 2 * keys, :], p.astype(BF16))
            total = part if total is None else total + part
            acc = mixed if acc is None else acc + mixed
        return acc / total, top + jnp.log(total)

    def main(h, c):
        @pl.when(h + 1 < heads)
        def _():
            kv_z(h + 1).wait_recv()
            kv_relay(h + 1).start()

        send(h, True)

        kv_y(h).wait_recv()

        @pl.when(h == 0)
        def _():
            tb_y.wait_recv()
            tb_relay.wait_recv()

        for j in range(1, a):
            q_move(j, h).wait_recv()
        kv_relay(h).wait_recv()
        for j in range(1, a):
            o, lse = attend(j, h)
            high = lse.astype(BF16)
            rest = lse - high.astype(F32)
            mid = rest.astype(BF16)
            tail = (rest - mid.astype(F32)).astype(BF16)
            o_send[j - 1, h, HEAD : HEAD + 16, :] = jnp.concatenate(
                [high.astype(F32), mid.astype(F32), tail.astype(F32), jnp.zeros((13, rows), F32)], axis=0
            ).astype(BF16)
            o_send[j - 1, h, 0:HEAD, :] = o.astype(BF16)
            o_move(j, h).start()
        o, lse = attend(0, h)
        o_own[h] = o
        lse_own[h] = jnp.broadcast_to(lse, (8, rows))

        @pl.when(h > 0)
        def _():
            merge(h - 1)

        return c

    def merge(h):
        lses = [lse_own[h][0:1]]
        parts = [o_own[h]]
        for j in range(1, a):
            o_move(j, h).wait_recv()
            stats = o_recv[j - 1, h, HEAD : HEAD + 16, :].astype(F32)
            lses.append(stats[0:1] + stats[1:2] + stats[2:3])
            parts.append(o_recv[j - 1, h, 0:HEAD, :].astype(F32))
        top = functools.reduce(jnp.maximum, lses)
        shares = [jnp.exp(x - top) for x in lses]
        total = functools.reduce(jnp.add, shares)
        o = functools.reduce(jnp.add, [x * y for x, y in zip(parts, shares)]) / total
        o_all[...] = o.astype(BF16)
        h_send[h] = o_all[:, pl.ds(pl.multiple_of((1 - t) * half, half), half)].T
        h_move(h).start()
        cols = pl.ds(pl.multiple_of(h * HEAD, HEAD), HEAD)
        h_mine[:, cols] = o_all[:, pl.ds(pl.multiple_of(t * half, half), half)].T

    lax.fori_loop(0, heads, main, 0)

    step = w.shape[1] // chunks
    spans = [slice(i * step, (i + 1) * step) for i in range(chunks)]
    early = (heads - 1) * HEAD

    def dot(x, y):
        return jnp.dot(x, y, preferred_element_type=F32)

    for span in spans:
        acc[0, :, span] = dot(h_mine[:, :early], w[:early, span])
    w_move.wait_recv()
    for h in range(heads - 1):
        h_move(h).wait_recv()
    theirs = jnp.concatenate([h_recv[h] for h in range(heads - 1)], axis=1)
    for span in spans:
        acc[1, :, span] = dot(theirs, w_far[:early, span])
    merge(heads - 1)
    for span in spans:
        acc[0, :, span] += dot(h_mine[:, early:], w[early:, span])
    h_move(heads - 1).wait_recv()
    for span in spans:
        far = acc[1, :, span] + dot(h_recv[heads - 1], w_far[early:, span])
        near = acc[0, :, span]
        out_ref[:, span] = (near.astype(BF16).astype(F32) + far.astype(BF16).astype(F32)).astype(BF16)

    def drain(h, c):
        kv_z(h).wait_send()
        kv_y(h).wait_send()
        kv_relay(h).wait_send()
        h_move(h).wait_send()
        for j in range(1, a):
            q_move(j, h).wait_send()
            o_move(j, h).wait_send()
        return c

    lax.fori_loop(0, heads, drain, 0)
    tb_z.wait_send()
    tb_y.wait_send()
    tb_relay.wait_send()
    w_move.wait_send()


def hub_kernel(
    chunks,
    slab_hbm, q_hbm, k_hbm, v_hbm, tk_hbm, tv_hbm, mask_hbm, qg_hbm, kg_hbm, lanes_hbm, perm_hbm, w_ref,
    out_ref,
    mine, held, tb, q_mine, q_held, o_send, o_recv, scores_a, scores_b, o_all, w, w_far, h_mine, h_send, h_recv,
    acc, tabs, q_ref, k_ref, v_ref, tk_ref, tv_ref, slab_ref, mask_ref, qg_ref, kg_ref, lanes_ref, perm_ref,
    kv_ss, kv_rs, tb_ss, tb_rs, q_ss, q_rs, o_ss, o_rs, h_ss, h_rs, wf_ss, wf_rs, w_sem, in_sem,
):
    rows, width = q_ref.shape
    heads = width // HEAD
    trows = tk_ref.shape[0]
    keys = rows + trows
    half = rows // 2
    pairs = heads // 2
    g, s, t = lax.axis_index("grp"), lax.axis_index("seq"), lax.axis_index("tp")
    u, low = s // GROUP, s % GROUP
    row, col = low // 2, low % 2
    inner = row + u == 1
    outer = row + u != 1
    aside = 1 - 2 * col

    def dev(seq):
        return (g, seq, t)

    near_s, far_s, cross_s = s + 2 - 4 * row, s + 2 - 4 * u, s + GROUP - 2 * GROUP * u
    near, far, cross, ydev = dev(near_s), dev(far_s), dev(cross_s), dev(s + aside)
    near_y, far_y, cross_y = dev(near_s + aside), dev(far_s + aside), dev(cross_s + aside)
    tdev = (g, s, 1 - t)

    barrier = pltpu.get_barrier_semaphore()
    friends = [near, ydev, tdev]
    for friend in friends:
        pl.semaphore_signal(barrier, inc=1, device_id=friend, device_id_type=MESH)

    @pl.when(inner)
    def _():
        pl.semaphore_signal(barrier, inc=1, device_id=far, device_id_type=MESH)

    loads = [
        pltpu.make_async_copy(x, y, in_sem.at[i])
        for i, (x, y) in enumerate(
            (
                (q_hbm, q_ref), (lanes_hbm, lanes_ref), (slab_hbm, slab_ref), (qg_hbm, qg_ref), (kg_hbm, kg_ref),
                (perm_hbm, perm_ref), (mask_hbm, mask_ref),
                (k_hbm, k_ref), (tk_hbm, tk_ref), (v_hbm, v_ref), (tv_hbm, tv_ref),
            )
        )
    ]
    for load in loads:
        load.start()
    w_copy = pltpu.make_async_copy(w_ref, w, w_sem)
    w_copy.start()

    def remote(src, dst, ss, rs, to):
        return pltpu.make_async_remote_copy(
            src_ref=src, dst_ref=dst, send_sem=ss, recv_sem=rs, device_id=to, device_id_type=MESH
        )

    def mine_on(i):
        return 2 * i + col

    def mine_off(i):
        return 2 * i + 1 - col

    def kv_move(src, slot, i, to):
        return remote(src, held.at[slot - 1, i], kv_ss, kv_rs.at[i], to)

    def kv_in(i):
        return kv_move(mine.at[mine_on(i)], 1, i, near)

    def kv_off(i):
        return kv_move(mine.at[mine_off(i)], 2, i, ydev)

    def kv_relay(i):
        return kv_move(held.at[1, i], 3, i, near)

    def q_move(src, slot, i, to):
        return remote(src, q_held.at[slot - 1, i], q_ss, q_rs.at[{1: 0, 4: 1, 5: 2}.get(slot, 3), i], to)

    def q_in(i):
        return q_move(q_mine.at[mine_on(i)], 1, i, near)

    def q_off(i):
        return q_move(q_mine.at[mine_off(i)], 4, i, ydev)

    def q_relay(i):
        return q_move(q_held.at[3, i], 5, i, near)

    def q_far(slot, i):
        if slot == 2:
            return q_move(q_mine.at[mine_on(i)], 2, i, far)
        start = {3: 1, 6: 4, 7: 5}[slot]
        return q_move(q_held.at[start - 1, i], slot, i, far)

    def o_move(slot, i):
        index, to = {
            1: (0, near), 4: (0, ydev), 5: (0, near_y),
            2: (1, far), 3: (1, cross), 6: (1, far_y), 7: (1, cross_y),
        }[slot]
        h = mine_on(i)
        return remote(
            o_send.at[slot - 1, i], o_recv.at[index, h], o_ss, o_rs.at[h], to
        )

    def h_move(h):
        return remote(h_send.at[h], h_recv.at[h], h_ss, h_rs.at[h // (heads - 2)], tdev)

    def arrived(ref, sem):
        remote(ref, ref, sem, sem, near).wait_recv()

    def left(ref, sem):
        remote(ref, ref, sem, sem, near).wait_send()

    w_move = remote(w, w_far, wf_ss, wf_rs, tdev)
    tb_in = remote(tb.at[0], tb.at[1], tb_ss, tb_rs, near)
    tb_y = remote(tb.at[0], tb.at[2], tb_ss, tb_rs, ydev)
    tb_relay = remote(tb.at[2], tb.at[3], tb_ss, tb_rs, near)

    for load in loads[1:7]:
        load.wait()
    freq, part, lead = lanes_ref[0:1, :], lanes_ref[1:2, :], lanes_ref[2:3, :]
    blocks = rows // WIDE
    block = lax.broadcasted_iota(jnp.int32, (blocks, HEAD), 0)
    slab = slab_ref[...] * SLAB_H
    place = jnp.where(part < 0.5, (block // SLAB_H).astype(F32), (slab + block % SLAB_H).astype(F32)) * freq
    across = lax.broadcasted_iota(jnp.int32, (WIDE, HEAD), 0).astype(F32) * freq
    trig = (jnp.cos(place), jnp.cos(across)), (jnp.sin(place), jnp.sin(across))

    def partner(x):
        wide = jnp.broadcast_to(x, (8, HEAD))
        near, far = PARTS[0] // 2, PARTS[1] // 2
        after = jnp.where(part < 0.5, pltpu.roll(wide, HEAD - near, 1), pltpu.roll(wide, HEAD - far, 1))
        before = jnp.where(part < 0.5, pltpu.roll(wide, near, 1), pltpu.roll(wide, far, 1))
        return jnp.where(lead > 0.5, after, before)[0:1]

    scale_q = F32(1.0) / jnp.sqrt(F32(HEAD))
    kg = kg_ref[...]
    qg = qg_ref[...] * scale_q
    for which, (by_block, by_column) in enumerate(trig):
        for gain, index in ((qg, 0), (kg, 2)):
            gain = gain if which == 0 else partner(gain)
            for i in range(blocks):
                full = jnp.where(part < 1.5, by_block[i : i + 1], by_column)
                tabs[index + which, i * WIDE : (i + 1) * WIDE, :] = full * gain
    line = lax.broadcasted_iota(jnp.int32, (trows, trows), 0)
    lane = lax.broadcasted_iota(jnp.int32, (trows, trows), 1)
    mark = jnp.where((line == lane) & (mask_ref[...] != 1), F32(NEGATIVE), F32(0.0))
    tb[0] = jnp.broadcast_to(jnp.sum(mark, axis=1, keepdims=True), (trows, HEAD)).astype(BF16)

    def norm_scale(x32):
        return lax.rsqrt(jnp.mean(x32 * x32, axis=-1, keepdims=True) + 0.05)

    def rotated(x, which):
        x32 = x.astype(F32)
        turned = jnp.dot(x, perm_ref[...], preferred_element_type=F32)
        return ((x32 * tabs[which] + turned * tabs[which + 1]) * norm_scale(x32)).astype(BF16)

    def prepare_q(h):
        q_mine[h] = rotated(q_ref[:, pl.ds(pl.multiple_of(h * HEAD, HEAD), HEAD)], 0)

    def prepare_kv(h):
        cols = pl.ds(pl.multiple_of(h * HEAD, HEAD), HEAD)
        mine[h, 0:rows, :] = rotated(k_ref[:, cols], 2)
        tk = tk_ref[:, cols].astype(F32)
        mine[h, rows:keys, :] = (tk * norm_scale(tk) * kg).astype(BF16)
        mine[h, keys : keys + rows, :] = v_ref[:, cols]
        mine[h, keys + rows : 2 * keys, :] = tv_ref[:, cols]

    def side(slot, i, part):
        where = pl.ds(part * keys, keys)
        return held[slot - 1, i, where, :] if slot else mine[mine_on(i), where, :]

    def score(slot, i, where):
        queries = q_held[slot - 1, i] if slot else q_mine[mine_on(i)]
        top = None
        for n in range(GROUP):
            sc = nt(side(n, i, 0), queries)
            mark = tb[n].astype(F32)
            mark = jnp.concatenate([mark] * (rows // HEAD), axis=1)
            sc = jnp.concatenate([sc[0:rows], sc[rows:keys] + mark], axis=0)
            where[n] = sc
            peak = jnp.max(sc, axis=0, keepdims=True)
            top = peak if top is None else jnp.maximum(top, peak)
        return top

    def weigh(i, where, top):
        total = None
        mixed = None
        for n in range(GROUP):
            p = jnp.exp(where[n] - top)
            amount = jnp.sum(p, axis=0, keepdims=True)
            got = tn(side(n, i, 1), p.astype(BF16))
            total = amount if total is None else total + amount
            mixed = got if mixed is None else mixed + got
        return mixed / total, top + jnp.log(total)

    wides = rows // HEAD

    def pack(to, o, lse):
        high = lse.astype(BF16).astype(F32)
        rest = lse - high
        mid = rest.astype(BF16).astype(F32)
        pieces = [x[:, i * HEAD : (i + 1) * HEAD] for x in (high, mid, rest - mid) for i in range(wides)]
        pieces.append(jnp.zeros((STATS - 3 * wides, HEAD), F32))
        to[rows : rows + STATS, :] = jnp.concatenate(pieces, axis=0).astype(BF16)
        for i in range(wides):
            to[i * HEAD : (i + 1) * HEAD, :] = o[:, i * HEAD : (i + 1) * HEAD].astype(BF16)

    def unpack(index, h):
        o = jnp.concatenate([o_recv[index, h, i * HEAD : (i + 1) * HEAD, :] for i in range(wides)], axis=1)
        stats = o_recv[index, h, rows : rows + STATS, :].astype(F32)
        levels = [
            jnp.concatenate([stats[k * wides + i : k * wides + i + 1] for i in range(wides)], axis=1)
            for k in range(3)
        ]
        return o.astype(F32), levels[0] + levels[1] + levels[2]

    def merge(h):
        hub = jnp.logical_and(inner, h % 2 == col)

        @pl.when(hub)
        def _():
            arrived(o_recv.at[1:2, h], o_rs.at[h])

        @pl.when(jnp.logical_not(hub))
        def _():
            arrived(o_recv.at[:, h], o_rs.at[h])

        (o, lse), (o_, lse_) = unpack(0, h), unpack(1, h)
        share = 1.0 / (1.0 + jnp.exp(lse_ - lse))
        o_all[...] = (o * share + o_ * (1.0 - share)).astype(BF16)
        h_send[h] = o_all[:, pl.ds(pl.multiple_of((1 - t) * half, half), half)].T
        h_move(h).start()
        cols = pl.ds(pl.multiple_of(h * HEAD, HEAD), HEAD)
        h_mine[:, cols] = o_all[:, pl.ds(pl.multiple_of(t * half, half), half)].T

    loads[0].wait()
    prepare_q(mine_off(0))
    prepare_q(mine_on(0))

    @pl.when(inner)
    def _():
        pl.semaphore_wait(barrier, len(friends) + 1)
        q_far(2, 0).start()

    @pl.when(outer)
    def _():
        pl.semaphore_wait(barrier, len(friends))
        q_in(0).start()
        tb_in.start()

    q_off(0).start()
    tb_y.start()

    def queries(i, c):
        prepare_q(mine_off(i))
        q_off(i).start()
        prepare_q(mine_on(i))

        @pl.when(inner)
        def _():
            q_far(2, i).start()

        @pl.when(outer)
        def _():
            q_in(i).start()

        return c

    lax.fori_loop(1, pairs, queries, 0)
    for load in loads[7:]:
        load.wait()
    prepare_kv(mine_off(0))
    kv_off(0).start()
    prepare_kv(mine_on(0))

    def keep(i, c):
        prepare_kv(mine_off(i))
        kv_off(i).start()
        prepare_kv(mine_on(i))
        return c

    lax.fori_loop(1, pairs, keep, 0)

    @pl.when(outer)
    def _():
        tb_y.wait_recv()
        tb_relay.start()

        def pass_queries(i, c):
            q_off(i).wait_recv()
            q_relay(i).start()
            return c

        def pass_keys(i, c):
            kv_in(i).start()
            kv_off(i).wait_recv()
            kv_relay(i).start()
            return c

        lax.fori_loop(0, 1, pass_queries, 0)
        pass_keys(0, 0)
        lax.fori_loop(1, pairs, pass_queries, 0)
        lax.fori_loop(1, pairs, pass_keys, 0)

    w_copy.wait()
    w_move.start()
    half = rows // 2

    def attend(j, h):
        queries = qs[j, h]
        scores = []
        top = None
        for slot in range(GROUP):
            sc = nt(kv[slot, h, 0:keys, :], queries)
            mark = tb[slot].astype(F32)
            mark = jnp.concatenate([mark] * (rows // HEAD), axis=1)
            sc = jnp.concatenate([sc[0:rows], sc[rows:keys] + mark], axis=0)
            peak = jnp.max(sc, axis=0, keepdims=True)
            top = peak if top is None else jnp.maximum(top, peak)
            scores.append(sc)
        total = None
        acc = None
        for slot in range(GROUP):
            p = jnp.exp(scores[slot] - top)
            part = jnp.sum(p, axis=0, keepdims=True)
            mixed = tn(kv[slot, h, keys : 2 * keys, :], p.astype(BF16))
            total = part if total is None else total + part
            acc = mixed if acc is None else acc + mixed
        return acc / total, top + jnp.log(total)

    def main(h, c):
        @pl.when(h + 1 < heads)
        def _():
            kv_z(h + 1).wait_recv()
            kv_relay(h + 1).start()

        send(h, True)

        kv_y(h).wait_recv()

        @pl.when(h == 0)
        def _():
            tb_y.wait_recv()
            tb_relay.wait_recv()

        for j in range(1, a):
            q_move(j, h).wait_recv()
        kv_relay(h).wait_recv()
        for j in range(1, a):
            o, lse = attend(j, h)
            high = lse.astype(BF16)
            rest = lse - high.astype(F32)
            mid = rest.astype(BF16)
            tail = (rest - mid.astype(F32)).astype(BF16)
            o_send[j - 1, h, HEAD : HEAD + 16, :] = jnp.concatenate(
                [high.astype(F32), mid.astype(F32), tail.astype(F32), jnp.zeros((13, rows), F32)], axis=0
            ).astype(BF16)
            o_send[j - 1, h, 0:HEAD, :] = o.astype(BF16)
            o_move(j, h).start()
        o, lse = attend(0, h)
        o_own[h] = o
        lse_own[h] = jnp.broadcast_to(lse, (8, rows))

        @pl.when(h > 0)
        def _():
            merge(h - 1)

        return c

    def merge(h):
        lses = [lse_own[h][0:1]]
        parts = [o_own[h]]
        for j in range(1, a):
            o_move(j, h).wait_recv()
            stats = o_recv[j - 1, h, HEAD : HEAD + 16, :].astype(F32)
            lses.append(stats[0:1] + stats[1:2] + stats[2:3])
            parts.append(o_recv[j - 1, h, 0:HEAD, :].astype(F32))
        top = functools.reduce(jnp.maximum, lses)
        shares = [jnp.exp(x - top) for x in lses]
        total = functools.reduce(jnp.add, shares)
        o = functools.reduce(jnp.add, [x * y for x, y in zip(parts, shares)]) / total
        o_all[...] = o.astype(BF16)
        h_send[h] = o_all[:, pl.ds(pl.multiple_of((1 - t) * half, half), half)].T
        h_move(h).start()
        cols = pl.ds(pl.multiple_of(h * HEAD, HEAD), HEAD)
        h_mine[:, cols] = o_all[:, pl.ds(pl.multiple_of(t * half, half), half)].T

    lax.fori_loop(0, heads, main, 0)

    step = w.shape[1] // chunks
    spans = [slice(i * step, (i + 1) * step) for i in range(chunks)]
    early = (heads - 1) * HEAD

    def dot(x, y):
        return jnp.dot(x, y, preferred_element_type=F32)

    for span in spans:
        acc[0, :, span] = dot(h_mine[:, :early], w[:early, span])
    w_move.wait_recv()
    for h in range(heads - 1):
        h_move(h).wait_recv()
    theirs = jnp.concatenate([h_recv[h] for h in range(heads - 1)], axis=1)
    for span in spans:
        acc[1, :, span] = dot(theirs, w_far[:early, span])
    merge(heads - 1)
    for span in spans:
        acc[0, :, span] += dot(h_mine[:, early:], w[early:, span])
    h_move(heads - 1).wait_recv()
    for span in spans:
        far = acc[1, :, span] + dot(h_recv[heads - 1], w_far[early:, span])
        near = acc[0, :, span]
        out_ref[:, span] = (near.astype(BF16).astype(F32) + far.astype(BF16).astype(F32)).astype(BF16)

    def drain(h, c):
        kv_z(h).wait_send()
        kv_y(h).wait_send()
        kv_relay(h).wait_send()
        h_move(h).wait_send()
        for j in range(1, a):
            q_move(j, h).wait_send()
            o_move(j, h).wait_send()
        return c

    lax.fori_loop(0, heads, drain, 0)
    tb_z.wait_send()
    tb_y.wait_send()
    tb_relay.wait_send()
    w_move.wait_send()


def hub_kernel(
    chunks,
    slab_hbm, q_hbm, k_hbm, v_hbm, tk_hbm, tv_hbm, mask_hbm, qg_hbm, kg_hbm, lanes_hbm, perm_hbm, w_ref,
    out_ref,
    mine, held, tb, q_mine, q_held, o_send, o_recv, scores_a, scores_b, o_all, w, w_far, h_mine, h_send, h_recv,
    acc, tabs, q_ref, k_ref, v_ref, tk_ref, tv_ref, slab_ref, mask_ref, qg_ref, kg_ref, lanes_ref, perm_ref,
    kv_ss, kv_rs, tb_ss, tb_rs, q_ss, q_rs, o_ss, o_rs, h_ss, h_rs, wf_ss, wf_rs, w_sem, in_sem,
):
    rows, width = q_ref.shape
    heads = width // HEAD
    trows = tk_ref.shape[0]
    keys = rows + trows
    half = rows // 2
    pairs = heads // 2
    g, s, t = lax.axis_index("grp"), lax.axis_index("seq"), lax.axis_index("tp")
    u, low = s // GROUP, s % GROUP
    row, col = low // 2, low % 2
    inner = row + u == 1
    outer = row + u != 1
    aside = 1 - 2 * col

    def dev(seq):
        return (g, seq, t)

    near_s, far_s, cross_s = s + 2 - 4 * row, s + 2 - 4 * u, s + GROUP - 2 * GROUP * u
    near, far, cross, ydev = dev(near_s), dev(far_s), dev(cross_s), dev(s + aside)
    near_y, far_y, cross_y = dev(near_s + aside), dev(far_s + aside), dev(cross_s + aside)
    tdev = (g, s, 1 - t)

    barrier = pltpu.get_barrier_semaphore()
    friends = [near, ydev, tdev]
    for friend in friends:
        pl.semaphore_signal(barrier, inc=1, device_id=friend, device_id_type=MESH)

    @pl.when(inner)
    def _():
        pl.semaphore_signal(barrier, inc=1, device_id=far, device_id_type=MESH)

    loads = [
        pltpu.make_async_copy(x, y, in_sem.at[i])
        for i, (x, y) in enumerate(
            (
                (q_hbm, q_ref), (lanes_hbm, lanes_ref), (slab_hbm, slab_ref), (qg_hbm, qg_ref), (kg_hbm, kg_ref),
                (perm_hbm, perm_ref), (mask_hbm, mask_ref),
                (k_hbm, k_ref), (tk_hbm, tk_ref), (v_hbm, v_ref), (tv_hbm, tv_ref),
            )
        )
    ]
    for load in loads:
        load.start()
    w_copy = pltpu.make_async_copy(w_ref, w, w_sem)
    w_copy.start()

    def remote(src, dst, ss, rs, to):
        return pltpu.make_async_remote_copy(
            src_ref=src, dst_ref=dst, send_sem=ss, recv_sem=rs, device_id=to, device_id_type=MESH
        )

    def mine_on(i):
        return 2 * i + col

    def mine_off(i):
        return 2 * i + 1 - col

    def kv_move(src, slot, i, to):
        return remote(src, held.at[slot - 1, i], kv_ss, kv_rs.at[i], to)

    def kv_in(i):
        return kv_move(mine.at[mine_on(i)], 1, i, near)

    def kv_off(i):
        return kv_move(mine.at[mine_off(i)], 2, i, ydev)

    def kv_relay(i):
        return kv_move(held.at[1, i], 3, i, near)

    def q_move(src, slot, i, to):
        return remote(src, q_held.at[slot - 1, i], q_ss, q_rs.at[{1: 0, 4: 1, 5: 2}.get(slot, 3), i], to)

    def q_in(i):
        return q_move(q_mine.at[mine_on(i)], 1, i, near)

    def q_off(i):
        return q_move(q_mine.at[mine_off(i)], 4, i, ydev)

    def q_relay(i):
        return q_move(q_held.at[3, i], 5, i, near)

    def q_far(slot, i):
        if slot == 2:
            return q_move(q_mine.at[mine_on(i)], 2, i, far)
        start = {3: 1, 6: 4, 7: 5}[slot]
        return q_move(q_held.at[start - 1, i], slot, i, far)

    def o_move(slot, i):
        index, to = {
            1: (0, near), 4: (0, ydev), 5: (0, near_y),
            2: (1, far), 3: (1, cross), 6: (1, far_y), 7: (1, cross_y),
        }[slot]
        h = mine_on(i)
        return remote(
            o_send.at[slot - 1, i], o_recv.at[index, h], o_ss, o_rs.at[h], to
        )

    def h_move(h):
        return remote(h_send.at[h], h_recv.at[h], h_ss, h_rs.at[h // (heads - 2)], tdev)

    def arrived(ref, sem):
        remote(ref, ref, sem, sem, near).wait_recv()

    def left(ref, sem):
        remote(ref, ref, sem, sem, near).wait_send()

    w_move = remote(w, w_far, wf_ss, wf_rs, tdev)
    tb_in = remote(tb.at[0], tb.at[1], tb_ss, tb_rs, near)
    tb_y = remote(tb.at[0], tb.at[2], tb_ss, tb_rs, ydev)
    tb_relay = remote(tb.at[2], tb.at[3], tb_ss, tb_rs, near)

    for load in loads[1:7]:
        load.wait()
    freq, part, lead = lanes_ref[0:1, :], lanes_ref[1:2, :], lanes_ref[2:3, :]
    blocks = rows // WIDE
    block = lax.broadcasted_iota(jnp.int32, (blocks, HEAD), 0)
    slab = slab_ref[...] * SLAB_H
    place = jnp.where(part < 0.5, (block // SLAB_H).astype(F32), (slab + block % SLAB_H).astype(F32)) * freq
    across = lax.broadcasted_iota(jnp.int32, (WIDE, HEAD), 0).astype(F32) * freq
    trig = (jnp.cos(place), jnp.cos(across)), (jnp.sin(place), jnp.sin(across))

    def partner(x):
        wide = jnp.broadcast_to(x, (8, HEAD))
        near, far = PARTS[0] // 2, PARTS[1] // 2
        after = jnp.where(part < 0.5, pltpu.roll(wide, HEAD - near, 1), pltpu.roll(wide, HEAD - far, 1))
        before = jnp.where(part < 0.5, pltpu.roll(wide, near, 1), pltpu.roll(wide, far, 1))
        return jnp.where(lead > 0.5, after, before)[0:1]

    scale_q = F32(1.0) / jnp.sqrt(F32(HEAD))
    kg = kg_ref[...]
    qg = qg_ref[...] * scale_q
    for which, (by_block, by_column) in enumerate(trig):
        for gain, index in ((qg, 0), (kg, 2)):
            gain = gain if which == 0 else partner(gain)
            for i in range(blocks):
                full = jnp.where(part < 1.5, by_block[i : i + 1], by_column)
                tabs[index + which, i * WIDE : (i + 1) * WIDE, :] = full * gain
    line = lax.broadcasted_iota(jnp.int32, (trows, trows), 0)
    lane = lax.broadcasted_iota(jnp.int32, (trows, trows), 1)
    mark = jnp.where((line == lane) & (mask_ref[...] != 1), F32(NEGATIVE), F32(0.0))
    tb[0] = jnp.broadcast_to(jnp.sum(mark, axis=1, keepdims=True), (trows, HEAD)).astype(BF16)

    def norm_scale(x32):
        return lax.rsqrt(jnp.mean(x32 * x32, axis=-1, keepdims=True) + 0.05)

    def rotated(x, which):
        x32 = x.astype(F32)
        turned = jnp.dot(x, perm_ref[...], preferred_element_type=F32)
        return ((x32 * tabs[which] + turned * tabs[which + 1]) * norm_scale(x32)).astype(BF16)

    def prepare_q(h):
        q_mine[h] = rotated(q_ref[:, pl.ds(pl.multiple_of(h * HEAD, HEAD), HEAD)], 0)

    def prepare_kv(h):
        cols = pl.ds(pl.multiple_of(h * HEAD, HEAD), HEAD)
        mine[h, 0:rows, :] = rotated(k_ref[:, cols], 2)
        tk = tk_ref[:, cols].astype(F32)
        mine[h, rows:keys, :] = (tk * norm_scale(tk) * kg).astype(BF16)
        mine[h, keys : keys + rows, :] = v_ref[:, cols]
        mine[h, keys + rows : 2 * keys, :] = tv_ref[:, cols]

    def side(slot, i, part):
        where = pl.ds(part * keys, keys)
        return held[slot - 1, i, where, :] if slot else mine[mine_on(i), where, :]

    def score(slot, i, where):
        queries = q_held[slot - 1, i] if slot else q_mine[mine_on(i)]
        top = None
        for n in range(GROUP):
            sc = nt(side(n, i, 0), queries)
            mark = tb[n].astype(F32)
            mark = jnp.concatenate([mark] * (rows // HEAD), axis=1)
            sc = jnp.concatenate([sc[0:rows], sc[rows:keys] + mark], axis=0)
            where[n] = sc
            peak = jnp.max(sc, axis=0, keepdims=True)
            top = peak if top is None else jnp.maximum(top, peak)
        return top

    def weigh(i, where, top):
        total = None
        mixed = None
        for n in range(GROUP):
            p = jnp.exp(where[n] - top)
            amount = jnp.sum(p, axis=0, keepdims=True)
            got = tn(side(n, i, 1), p.astype(BF16))
            total = amount if total is None else total + amount
            mixed = got if mixed is None else mixed + got
        return mixed / total, top + jnp.log(total)

    wides = rows // HEAD

    def pack(to, o, lse):
        high = lse.astype(BF16).astype(F32)
        rest = lse - high
        mid = rest.astype(BF16).astype(F32)
        pieces = [x[:, i * HEAD : (i + 1) * HEAD] for x in (high, mid, rest - mid) for i in range(wides)]
        pieces.append(jnp.zeros((STATS - 3 * wides, HEAD), F32))
        to[rows : rows + STATS, :] = jnp.concatenate(pieces, axis=0).astype(BF16)
        for i in range(wides):
            to[i * HEAD : (i + 1) * HEAD, :] = o[:, i * HEAD : (i + 1) * HEAD].astype(BF16)

    def unpack(index, h):
        o = jnp.concatenate([o_recv[index, h, i * HEAD : (i + 1) * HEAD, :] for i in range(wides)], axis=1)
        stats = o_recv[index, h, rows : rows + STATS, :].astype(F32)
        levels = [
            jnp.concatenate([stats[k * wides + i : k * wides + i + 1] for i in range(wides)], axis=1)
            for k in range(3)
        ]
        return o.astype(F32), levels[0] + levels[1] + levels[2]

    def merge(h):
        hub = jnp.logical_and(inner, h % 2 == col)

        @pl.when(hub)
        def _():
            arrived(o_recv.at[1:2, h], o_rs.at[h])

        @pl.when(jnp.logical_not(hub))
        def _():
            arrived(o_recv.at[:, h], o_rs.at[h])

        (o, lse), (o_, lse_) = unpack(0, h), unpack(1, h)
        share = 1.0 / (1.0 + jnp.exp(lse_ - lse))
        o_all[...] = (o * share + o_ * (1.0 - share)).astype(BF16)
        h_send[h] = o_all[:, pl.ds(pl.multiple_of((1 - t) * half, half), half)].T
        h_move(h).start()
        cols = pl.ds(pl.multiple_of(h * HEAD, HEAD), HEAD)
        h_mine[:, cols] = o_all[:, pl.ds(pl.multiple_of(t * half, half), half)].T

    loads[0].wait()
    prepare_q(mine_off(0))
    prepare_q(mine_on(0))

    @pl.when(inner)
    def _():
        pl.semaphore_wait(barrier, len(friends) + 1)
        q_far(2, 0).start()

    @pl.when(outer)
    def _():
        pl.semaphore_wait(barrier, len(friends))
        q_in(0).start()
        tb_in.start()

    q_off(0).start()
    tb_y.start()

    def queries(i, c):
        prepare_q(mine_off(i))
        q_off(i).start()
        prepare_q(mine_on(i))

        @pl.when(inner)
        def _():
            q_far(2, i).start()

        @pl.when(outer)
        def _():
            q_in(i).start()

        return c

    lax.fori_loop(1, pairs, queries, 0)
    for load in loads[7:]:
        load.wait()
    prepare_kv(mine_off(0))
    kv_off(0).start()
    prepare_kv(mine_on(0))

    def keep(i, c):
        prepare_kv(mine_off(i))
        kv_off(i).start()
        prepare_kv(mine_on(i))
        return c

    lax.fori_loop(1, pairs, keep, 0)

    @pl.when(outer)
    def _():
        tb_y.wait_recv()
        tb_relay.start()

        def pass_queries(i, c):
            q_off(i).wait_recv()
            q_relay(i).start()
            return c

        lax.fori_loop(0, pairs, pass_queries, 0)

        def pass_keys(i, c):
            kv_in(i).start()
            kv_off(i).wait_recv()
            kv_relay(i).start()
            return c

        lax.fori_loop(0, pairs, pass_keys, 0)

    w_copy.wait()
    w_move.start()

    @pl.when(inner)
    def _():
        def onward(i):
            q_in(i).wait_recv()
            q_far(3, i).start()
            q_off(i).wait_recv()
            q_far(6, i).start()

        def onward_last(i):
            q_relay(i).wait_recv()
            q_far(7, i).start()

        onward(0)
        onward(1)

        def trail(i, c):
            onward_last(i)

            @pl.when(i + 2 < pairs)
            def _():
                onward(i + 2)

            return c

        lax.fori_loop(0, pairs, trail, 0)
        arrived(tb.at[1:GROUP], tb_rs)

        def serve(i, order):
            top = score(order[0], i, scores_a)
            for n, slot in enumerate(order):
                here, there = ((scores_a, scores_b), (scores_b, scores_a))[n % 2]
                after = score(order[n + 1], i, there) if n + 1 < HUB_SLOTS else None
                o, lse = weigh(i, here, top)
                top = after
                if slot:
                    pack(o_send.at[slot - 1, i], o, lse)
                    o_move(slot, i).start()
                else:
                    pack(o_recv.at[0, mine_on(i)], o, lse)

        def main(i, c):
            arrived(q_held.at[0:4, i], q_rs.at[3, i])
            arrived(held.at[:, i], kv_rs.at[i])
            @pl.when(t == 0)
            def _():
                serve(i, (7, 3, 5, 6, 2, 1, 4, 0))

            @pl.when(t == 1)
            def _():
                serve(i, (5, 7, 1, 3, 4, 6, 2, 0))

            return c

        lax.fori_loop(0, pairs, main, 0)

    def collect(h, c):
        merge(h)
        return c

    lax.fori_loop(0, heads - 2, collect, 0)

    step = w.shape[1] // chunks
    spans = [slice(i * step, (i + 1) * step) for i in range(chunks)]
    early = (heads - 2) * HEAD

    def dot(x, y):
        return jnp.dot(x, y, preferred_element_type=F32)

    for span in spans:
        acc[0, :, span] = dot(h_mine[:, :early], w[:early, span])
    w_move.wait_recv()
    arrived(h_recv.at[0 : heads - 2], h_rs.at[0])
    theirs = jnp.concatenate([h_recv[h] for h in range(heads - 2)], axis=1)
    for span in spans:
        acc[1, :, span] = dot(theirs, w_far[:early, span])

    merge(heads - 2)
    merge(heads - 1)

    for span in spans:
        acc[0, :, span] += dot(h_mine[:, early:], w[early:, span])
    arrived(h_recv.at[heads - 2 : heads], h_rs.at[1])
    last = jnp.concatenate([h_recv[heads - 2], h_recv[heads - 1]], axis=1)
    for span in spans:
        theirs = acc[1, :, span] + dot(last, w_far[early:, span])
        mine_too = acc[0, :, span]
        out_ref[:, span] = (mine_too.astype(BF16).astype(F32) + theirs.astype(BF16).astype(F32)).astype(BF16)

    @pl.when(inner)
    def _():
        left(q_held.at[0:5], q_ss)
        left(held.at[0:1], kv_ss)
        left(o_send, o_ss)
        left(tb.at[0:1], tb_ss)

    @pl.when(outer)
    def _():
        left(q_held.at[0:3], q_ss)
        left(held, kv_ss)
        left(tb.at[0:3], tb_ss)

    left(h_send, h_ss)
    w_move.wait_send()


def hub_scratch(rows, trows, heads, model, w_shape, inputs):
    keys, half, pairs = rows + trows, rows // 2, heads // 2
    dma = pltpu.SemaphoreType.DMA
    return [
        pltpu.VMEM((heads, 2 * keys, HEAD), BF16),
        pltpu.VMEM((3, pairs, 2 * keys, HEAD), BF16),
        pltpu.VMEM((GROUP, trows, HEAD), BF16),
        pltpu.VMEM((heads, rows, HEAD), BF16),
        pltpu.VMEM((HUB_SLOTS - 1, pairs, rows, HEAD), BF16),
        pltpu.VMEM((HUB_SLOTS - 1, pairs, rows + STATS, HEAD), BF16),
        pltpu.VMEM((2, heads, rows + STATS, HEAD), BF16),
        pltpu.VMEM((GROUP, keys, rows), F32),
        pltpu.VMEM((GROUP, keys, rows), F32),
        pltpu.VMEM((HEAD, rows), BF16),
        pltpu.VMEM(w_shape, BF16),
        pltpu.VMEM(w_shape, BF16),
        pltpu.VMEM((half, heads * HEAD), BF16),
        pltpu.VMEM((heads, half, HEAD), BF16),
        pltpu.VMEM((heads, half, HEAD), BF16),
        pltpu.VMEM((2, half, model), F32),
        pltpu.VMEM((4, rows, HEAD), F32),
        *[pltpu.VMEM(x.shape, x.dtype) for x in inputs],
        dma, dma((pairs,)), dma, dma, dma, dma((4, pairs)), dma, dma((heads,)), dma, dma((2,)), dma, dma, dma,
        dma((11,)),
    ]


def body(
    n,
    visual_q, visual_key_input, visual_v, text_k, text_v, text_mask, slab_order, q_gain, key_norm_gain, w_out,
):
    rows, width = visual_q.shape
    heads = width // HEAD
    model = w_out.shape[1]
    a = n // GROUP
    trows = -(-text_k.shape[0] // 16) * 16
    pad = trows - text_k.shape[0]
    if pad:
        text_k = jnp.pad(text_k, ((0, pad), (0, 0)))
        text_v = jnp.pad(text_v, ((0, pad), (0, 0)))
        text_mask = jnp.pad(text_mask, (0, pad))
    lanes, perm = lane_constants()
    chunks = 6 if model % (6 * HEAD) == 0 else 1
    keys = rows + trows
    half = rows // 2
    peers = a - 1
    vm = pl.BlockSpec(memory_space=pltpu.VMEM)
    anywhere = pl.BlockSpec(memory_space=pl.ANY)
    dma = pltpu.SemaphoreType.DMA
    operands = (
        slab_order, visual_q, visual_key_input, visual_v, text_k, text_v, text_mask[None], q_gain[None],
        key_norm_gain[None], jnp.asarray(lanes), jnp.asarray(perm, BF16), w_out,
    )
    if n == 2 * GROUP and rows % HEAD == 0 and heads % 2 == 0 and heads > 3:
        run = functools.partial(hub_kernel, chunks)
        operands = (slab_order[None],) + operands[1:]
        scratch = hub_scratch(rows, trows, heads, model, w_out.shape, operands[1:6] + operands[:1] + operands[6:11])
        places = [anywhere] * 12
    else:
        run = functools.partial(kernel, n, chunks)
        places = [pl.BlockSpec(memory_space=pltpu.SMEM)] + [anywhere] * 5 + [vm] * 5 + [anywhere]
        scratch = [
                pltpu.VMEM((GROUP, heads, 2 * keys, HEAD), BF16),
                pltpu.VMEM((GROUP, trows, HEAD), BF16),
                pltpu.VMEM((a, heads, rows, HEAD), BF16),
                pltpu.VMEM((peers, heads, HEAD + 16, rows), BF16),
                pltpu.VMEM((peers, heads, HEAD + 16, rows), BF16),
                pltpu.VMEM((heads, HEAD, rows), F32),
                pltpu.VMEM((heads, 8, rows), F32),
                pltpu.VMEM((HEAD, rows), BF16),
                pltpu.VMEM(w_out.shape, BF16),
                pltpu.VMEM(w_out.shape, BF16),
                pltpu.VMEM((half, width), BF16),
                pltpu.VMEM((heads, half, HEAD), BF16),
                pltpu.VMEM((heads, half, HEAD), BF16),
                pltpu.VMEM((2, half, model), F32),
                pltpu.VMEM((4, rows, HEAD), F32),
                *[pltpu.VMEM(x.shape, BF16) for x in (visual_q, visual_key_input, visual_v, text_k, text_v)],
                dma((3, heads)), dma((3, heads)), dma((3,)), dma((3,)),
                dma((peers, heads)), dma((peers, heads)), dma((peers, heads)), dma((peers, heads)),
                dma((heads,)), dma((heads,)), dma, dma, dma, dma((5,)),
        ]
    return pl.pallas_call(
        run,
        out_shape=pltpu.VMEM((half, model), BF16),
        in_specs=places,
        out_specs=vm,
        scratch_shapes=scratch,
        compiler_params=pltpu.CompilerParams(
            collective_id=0, has_side_effects=True, vmem_limit_bytes=60 * 1024 * 1024
        ),
    )(*operands)


def solution(mesh):
    rows = P(("grp", "seq"), "tp")
    placed = (rows,) * 5 + (P(("grp", "seq")),) * 2 + (P(), P(), P("tp", None))
    return jax.shard_map(
        functools.partial(body, mesh.shape["seq"]),
        mesh=mesh, in_specs=placed, out_specs=P(("grp", "seq", "tp"), None), check_vma=False,
    )
```
